32 devices in a mesh: data: 1 (over z), cp: 4 (over y), tp: 8 (over x, core).
Axes of the slice: x: 4, y: 4, z: 1, core: 2. Of those that a mesh axis runs over, the one named last changes fastest.
The devices are a block of a 4x4x8 slice.
Arguments:
- act_in: bfloat16 [2, 2048, 1536], P(None, ('data', 'cp', 'tp'))
- route_ids: int32 [2, 2048, 2], P(None, ('data', 'cp', 'tp'))
- route_gates: float32 [2, 2048, 2], P(None, ('data', 'cp', 'tp'))
- w_query: bfloat16 [1536, 24, 64], P(None, 'tp')
- w_key: bfloat16 [1536, 8, 64], P(None, 'tp')
- w_value: bfloat16 [1536, 8, 64], P(None, 'tp')
- w_out: bfloat16 [24, 64, 1536], P('tp')
- w_gate: bfloat16 [32, 1536, 512], P(('cp', 'tp'))
- w_up: bfloat16 [32, 1536, 512], P(('cp', 'tp'))
- w_down: bfloat16 [32, 512, 1536], P(('cp', 'tp'))
Outputs:
- output: bfloat16 [2, 2048, 1536], P(None, ('data', 'cp', 'tp'))
All inputs are finite; a program needn't handle non-finite values.
Results may differ from the reference program's by a relative error of at most 0.00477921.
Values are sent between devices in bfloat16 or wider.
A program may use at most 768 MiB of HBM per device.

```python
import math
import jax
import jax.numpy as jnp
from jax import lax

HIDDEN = 1536
EXPERT_FF = 512
Q_HEADS = 24
KV_HEADS = 8
HEAD_DIM = 64
CP_SIZE = 4
TP_SIZE = 8
TOKENS_DEV = 64
MICRO_BATCHES = 2

EXPERTS = CP_SIZE * TP_SIZE
SEQ_LEN = TOKENS_DEV * EXPERTS
PIECE_LEN = SEQ_LEN // (2 * CP_SIZE)
CAPACITY = (4 * TOKENS_DEV) // EXPERTS
EXPERT_ROWS = CAPACITY * EXPERTS
GROUP_SIZE = Q_HEADS // KV_HEADS
SCORE_SHARP = math.sqrt(0.75 * math.log(SEQ_LEN))


def draw_routing(base_key):
    half_cap = CAPACITY // 2

    def one_source(src_key):
        k_perm, k_delta, k_tok, k_swap = jax.random.split(src_key, 4)
        expert_perm = jax.random.permutation(k_perm, EXPERTS)
        deltas = jax.random.randint(k_delta, (EXPERTS // 2,), 0, half_cap + 1).at[0].set(half_cap)
        pair_counts = jnp.stack([half_cap + deltas, half_cap - deltas], axis=1).reshape(EXPERTS)
        counts = jnp.zeros((EXPERTS,), jnp.int32).at[expert_perm].set(pair_counts)
        count_ends = jnp.cumsum(counts)
        labels = jnp.sum((jnp.arange(2 * TOKENS_DEV)[:, None] >= count_ends[None, :]).astype(jnp.int32), axis=1)
        id_pairs = jnp.stack([labels[:TOKENS_DEV], labels[TOKENS_DEV:]], axis=1)
        id_pairs = id_pairs[jax.random.permutation(k_tok, TOKENS_DEV)]
        swap_flag = jax.random.randint(k_swap, (TOKENS_DEV, 1), 0, 2)
        return jnp.where(swap_flag == 1, id_pairs[:, ::-1], id_pairs).astype(jnp.int32)

    return jax.vmap(one_source)(jax.random.split(base_key, EXPERTS)).reshape(SEQ_LEN, 2)


def normal_weight(weight_key, arr_shape, w_scale):
    return (jax.random.normal(weight_key, arr_shape, jnp.float32) * w_scale).astype(jnp.bfloat16)


def expert_stack(weight_key, arr_shape, w_scale):
    return lax.map(lambda one_key: normal_weight(one_key, arr_shape, w_scale), jax.random.split(weight_key, EXPERTS))


def setup_inputs(seed: int = 0, part: int = 0) -> dict:
    part_key = jax.random.fold_in(jax.random.key(seed), part)
    k_act, k_route, k_gate = jax.random.split(part_key, 3)
    shared = jax.random.split(jax.random.key(seed + 1), 7)
    act_in = jax.random.normal(k_act, (MICRO_BATCHES, SEQ_LEN, HIDDEN), jnp.float32).astype(jnp.bfloat16)
    route_ids = jax.vmap(draw_routing)(jax.random.split(k_route, MICRO_BATCHES))
    route_gates = jax.random.uniform(k_gate, (MICRO_BATCHES, SEQ_LEN, 2), jnp.float32, 0.3, 0.7)
    return {
        'act_in': act_in,
        'route_ids': route_ids,
        'route_gates': route_gates,
        'w_query': normal_weight(shared[0], (HIDDEN, Q_HEADS, HEAD_DIM), SCORE_SHARP / math.sqrt(HIDDEN)),
        'w_key': normal_weight(shared[1], (HIDDEN, KV_HEADS, HEAD_DIM), 1.0 / math.sqrt(HIDDEN)),
        'w_value': normal_weight(shared[2], (HIDDEN, KV_HEADS, HEAD_DIM), 1.0 / math.sqrt(HIDDEN)),
        'w_out': normal_weight(shared[3], (Q_HEADS, HEAD_DIM, HIDDEN), 1.0 / math.sqrt(Q_HEADS * HEAD_DIM)),
        'w_gate': expert_stack(shared[4], (HIDDEN, EXPERT_FF), 1.0 / math.sqrt(HIDDEN)),
        'w_up': expert_stack(shared[5], (HIDDEN, EXPERT_FF), 1.0 / math.sqrt(HIDDEN)),
        'w_down': expert_stack(shared[6], (EXPERT_FF, HIDDEN), 1.0 / math.sqrt(EXPERT_FF)),
    }


def token_positions():
    row_ix = jnp.arange(SEQ_LEN)
    owner_ix = row_ix // (2 * PIECE_LEN)
    inner_ix = row_ix % (2 * PIECE_LEN)
    return jnp.where(inner_ix < PIECE_LEN, owner_ix * PIECE_LEN + inner_ix, (2 * CP_SIZE - 1 - owner_ix) * PIECE_LEN + inner_ix - PIECE_LEN)


def attention_block(seq_in, w_query, w_key, w_value, w_out):
    query_rows = jnp.dot(seq_in, w_query.reshape(HIDDEN, Q_HEADS * HEAD_DIM), preferred_element_type=jnp.float32).astype(jnp.bfloat16)
    key_rows = jnp.dot(seq_in, w_key.reshape(HIDDEN, KV_HEADS * HEAD_DIM), preferred_element_type=jnp.float32).astype(jnp.bfloat16)
    value_rows = jnp.dot(seq_in, w_value.reshape(HIDDEN, KV_HEADS * HEAD_DIM), preferred_element_type=jnp.float32).astype(jnp.bfloat16)
    key_rows = key_rows.astype(jnp.float32).reshape(SEQ_LEN, KV_HEADS, HEAD_DIM)
    value_rows = value_rows.astype(jnp.float32).reshape(SEQ_LEN, KV_HEADS, HEAD_DIM)
    positions = token_positions()
    query_blocks = query_rows.reshape(EXPERTS, TOKENS_DEV, KV_HEADS, GROUP_SIZE, HEAD_DIM)
    pos_blocks = positions.reshape(EXPERTS, TOKENS_DEV)

    def one_block(block_args):
        q_block, q_pos = block_args
        scores = jnp.einsum('qhgd,khd->hgqk', q_block.astype(jnp.float32), key_rows) * HEAD_DIM ** -0.5
        scores = jnp.where(positions[None, :] <= q_pos[:, None], scores, -jnp.inf)
        row_peak = jnp.max(scores, axis=-1, keepdims=True)
        exp_scores = jnp.exp(scores - row_peak)
        row_sum = jnp.sum(exp_scores, axis=-1)
        weighted = jnp.einsum('hgqk,khd->qhgd', exp_scores.astype(jnp.bfloat16).astype(jnp.float32), value_rows)
        weighted = weighted / jnp.transpose(row_sum, (2, 0, 1))[..., None]
        return weighted.astype(jnp.bfloat16).reshape(TOKENS_DEV, Q_HEADS * HEAD_DIM)

    attn_rows = lax.map(one_block, (query_blocks, pos_blocks)).reshape(SEQ_LEN, Q_HEADS * HEAD_DIM)
    attn_sum = jnp.dot(attn_rows, w_out.reshape(Q_HEADS * HEAD_DIM, HIDDEN), preferred_element_type=jnp.float32)
    return (seq_in.astype(jnp.float32) + attn_sum).astype(jnp.bfloat16)


def expert_block(mid_rows, seq_ids, seq_gates, w_gate, w_up, w_down):
    choice_expert = seq_ids.reshape(2 * SEQ_LEN)
    choice_token = jnp.arange(2 * SEQ_LEN) // 2
    sort_ix = jnp.argsort(choice_expert, stable=True)
    counts = jnp.sum((choice_expert[None, :] == jnp.arange(EXPERTS)[:, None]).astype(jnp.int32), axis=1)
    starts = jnp.cumsum(counts) - counts
    sorted_token = jnp.concatenate([choice_token[sort_ix], jnp.zeros((EXPERT_ROWS,), choice_token.dtype)])

    def one_expert(expert_id):
        token_ids = lax.dynamic_slice(sorted_token, (starts[expert_id],), (EXPERT_ROWS,))
        expert_in = mid_rows[token_ids]
        gate_act = jnp.dot(expert_in, w_gate[expert_id], preferred_element_type=jnp.float32)
        up_act = jnp.dot(expert_in, w_up[expert_id], preferred_element_type=jnp.float32)
        mixed_act = (jax.nn.silu(gate_act) * up_act).astype(jnp.bfloat16)
        return jnp.dot(mixed_act, w_down[expert_id], preferred_element_type=jnp.float32).astype(jnp.bfloat16)

    expert_out = lax.map(one_expert, jnp.arange(EXPERTS)).reshape(EXPERTS * EXPERT_ROWS, HIDDEN)
    sorted_expert = choice_expert[sort_ix]
    slot_rank = jnp.arange(2 * SEQ_LEN) - starts[sorted_expert]
    z_sorted = expert_out[sorted_expert * EXPERT_ROWS + slot_rank]
    z_choice = z_sorted[jnp.argsort(sort_ix)].reshape(SEQ_LEN, 2, HIDDEN)
    mixed_sum = jnp.sum(seq_gates[:, :, None] * z_choice.astype(jnp.float32), axis=1)
    return (mid_rows.astype(jnp.float32) + mixed_sum).astype(jnp.bfloat16)


def reference(act_in, route_ids, route_gates, w_query, w_key, w_value, w_out, w_gate, w_up, w_down):
    def one_sequence(seq_args):
        seq_in, seq_ids, seq_gates = seq_args
        mid_rows = attention_block(seq_in, w_query, w_key, w_value, w_out)
        return expert_block(mid_rows, seq_ids, seq_gates, w_gate, w_up, w_down)

    return lax.map(one_sequence, (act_in, route_ids, route_gates))
```

```python
import functools

import jax
import jax.numpy as jnp
from jax import lax
from jax.experimental import pallas as pl
from jax.experimental.pallas import tpu as pltpu
from jax.sharding import PartitionSpec as P

MESH = pl.DeviceIdType.MESH
F32 = jnp.float32
BF16 = jnp.bfloat16
NT = (((1,), (1,)), ((), ()))


def mm(a, b):
    return jnp.dot(a, b, preferred_element_type=F32)


def mm_nt(a, b):
    return lax.dot_general(a, b, NT, preferred_element_type=F32)


def layer_kernel(dims, x_hbm, ids_ref, gates_ref, wq_hbm, wk_hbm, wv_hbm, wo_hbm, wg_hbm, wu_hbm, wd_hbm, y_ref,
                 xf, wqkv, kv, qs, sbuf, mx, lsum, acc, osend, orecv, wof, onehot, onehot_t, gcol, hbuf,
                 dsend, drecv, rsend, rrecv, wg, wu, wd,
                 loc_sem, xs_sem, xr_sem, ws_sem, wr_sem, ks_sem, kr_sem, os_sem, or_sem,
                 ds_sem, dr_sem, rs_sem, rr_sem):
    cps, tps, seqs, n, hid, hd, qh, cap = dims
    experts = cps * tps
    group = experts
    chips = tps // 2
    hslots = tps // 2
    piece = n * hslots
    pieces = 2 * cps
    lanes = 2 * hd
    qrows = qh * piece
    kdim = qh * hd
    c = lax.axis_index('cp')
    t = lax.axis_index('tp')
    me = c * tps + t
    xc = t // 2
    core = t % 2

    def slot(dx, other):
        return ((xc + dx) % chips) * 2 + (core if not other else 1 - core)

    right, left, sib = slot(1, False), slot(chips - 1, False), slot(0, True)

    def rcopy(src, dst, ssem, rsem, cc, tt):
        return pltpu.make_async_remote_copy(src_ref=src, dst_ref=dst, send_sem=ssem, recv_sem=rsem,
                                            device_id={'cp': cc, 'tp': tt}, device_id_type=MESH)

    loads = []

    def load(src, dst, i):
        cp = pltpu.make_async_copy(src, dst, loc_sem.at[i])
        cp.start()
        loads.append(cp)
        return cp

    ld_x = [load(x_hbm.at[s], xf.at[s, t], s) for s in range(seqs)]
    ld_wo = load(wo_hbm, wof.at[t], 2)
    ld_qkv = [load(wv_hbm, wqkv.at[pl.ds(0, hd)], 3), load(wk_hbm, wqkv.at[pl.ds(hd, hd)], 4)]
    for i in range(qh):
        ld_qkv.append(load(wq_hbm.at[pl.ds(i * hd, hd)], wqkv.at[pl.ds(lanes * (i + 1) + hd, hd)], 5 + i))
    ld_exp = [load(wg_hbm, wg, 5 + qh), load(wu_hbm, wu, 6 + qh), load(wd_hbm, wd, 7 + qh)]

    barrier = pltpu.get_barrier_semaphore()

    def sig(i, _):
        g = (me + i) % group
        pl.semaphore_signal(barrier, inc=1, device_id={'cp': g // tps, 'tp': g % tps}, device_id_type=MESH)
        return 0

    lax.fori_loop(1, group, sig, 0)
    pl.semaphore_wait(barrier, group - 1)

    def gather_parts(buf, rows, ss, rs, chunked):
        half = rows // 2
        lo, hi = pl.ds(0, half), pl.ds(half, half)

        def ref(sl, part):
            return buf.at[sl] if part is None else buf.at[sl, part]

        def cp(src_slot, part, kind, dst):
            return rcopy(ref(src_slot, part), ref(src_slot, part), ss.at[kind], rs.at[kind], c, dst)

        nl, nr, op = slot(chips - 1, False), slot(1, False), slot(2, False)
        snl, snr, sop = slot(chips - 1, True), slot(1, True), slot(2, True)
        own = t
        sends = [
            (own, lo, right), (own, hi, right), (own, hi, left), (own, lo, left),
            (nl, lo, right), (nr, hi, left),
            (own, None, sib), (nl, None, sib), (nr, None, sib), (op, lo, sib), (op, hi, sib),
        ]
        gets = [
            (nl, lo), (nl, hi), (nr, hi), (nr, lo),
            (op, lo), (op, hi),
            (sib, None), (snl, None), (snr, None), (sop, lo), (sop, hi),
        ]

        def start(k):
            s_, p_, d_ = sends[k]
            cp(s_, p_, k, d_).start()

        def got(k):
            s_, p_ = gets[k]
            cp(s_, p_, k, sib).wait_recv()

        def sent(k):
            s_, p_, d_ = sends[k]
            cp(s_, p_, k, d_).wait_send()

        return start, got, sent

    xg = [gather_parts(xf.at[s], n, xs_sem.at[s], xr_sem.at[s], False) for s in range(seqs)]
    wg_parts = gather_parts(wof, kdim, ws_sem, wr_sem, True)

    for s in range(seqs):
        ld_x[s].wait()
        for k in (0, 2, 1, 3, 6):
            xg[s][0](k)

    ecol = lax.broadcasted_iota(jnp.int32, (experts, n), 0)
    later = (lax.broadcasted_iota(jnp.int32, (n, n), 0) < lax.broadcasted_iota(jnp.int32, (n, n), 1)).astype(F32).astype(BF16)
    srow = lax.broadcasted_iota(jnp.int32, (experts * cap, n), 0)
    eye = lax.broadcasted_iota(jnp.int32, (n, n), 0) == lax.broadcasted_iota(jnp.int32, (n, n), 1)
    for s in range(seqs):
        first = jnp.zeros((experts, 1), F32)
        both = None
        for k in range(2):
            idk = ids_ref[s, k:k + 1, :]
            hits = (ecol == idk).astype(F32)
            before = mm(hits.astype(BF16), later) + first
            rank = jnp.sum(hits * before, axis=0, keepdims=True).astype(jnp.int32)
            first = first + jnp.sum(hits, axis=1, keepdims=True)
            dest = idk * cap + rank
            pick = (srow == dest).astype(F32)
            both = pick if both is None else both + pick
            onehot_t[s, k * n:(k + 1) * n, :] = pick.T.astype(BF16)
            gcol[s, k] = jnp.broadcast_to(jnp.sum(jnp.where(eye, gates_ref[s, k:k + 1, :], 0.0), axis=1, keepdims=True), (n, 128))
        onehot[s] = both.astype(BF16)
    for i in range(qh):
        wqkv[lanes * (i + 1):lanes * (i + 1) + hd, :] = jnp.zeros((hd, hid), BF16)

    def relay(parts):
        start, got, sent = parts
        got(0)
        start(4)
        got(2)
        start(5)
        got(1)
        start(7)
        got(3)
        start(8)

    def finish(parts):
        start, got, sent = parts
        got(4)
        start(9)
        got(5)
        start(10)
        for k in (6, 7, 8, 9, 10):
            got(k)

    for s in range(seqs):
        relay(xg[s])
    ld_wo.wait()
    for k in (0, 2, 1, 3, 6):
        wg_parts[0](k)
    for cp in ld_qkv:
        cp.wait()

    def kv_piece(half):
        return c if half == 0 else pieces - 1 - c

    def kv_copy(s, half, r, src):
        ref = kv.at[s, src if half == 0 else pieces - 1 - src]
        return rcopy(ref, ref, ks_sem.at[s, half, r], kr_sem.at[s, half, src], r, t)

    for s in range(seqs):
        finish(xg[s])
        for half in range(2):
            rows = xf[s, half * hslots:(half + 1) * hslots].reshape(piece, hid)
            out = mm_nt(rows, wqkv[...])
            kv[s, kv_piece(half)] = out[:, :lanes].astype(BF16)
            for i in range(qh):
                qs[s, half, i * piece:(i + 1) * piece, :] = out[:, lanes * (i + 1):lanes * (i + 2)].astype(BF16)
            for i in range(1, cps):
                r = (c + i) % cps
                if half == 0:
                    kv_copy(s, half, r, c).start()
                else:
                    @pl.when(r < c)
                    def _():
                        kv_copy(s, half, r, c).start()

    scale = hd ** -0.5
    causal = lax.broadcasted_iota(jnp.int32, (piece, piece), 1) <= lax.broadcasted_iota(jnp.int32, (piece, piece), 0)
    lane_lo = lax.broadcasted_iota(jnp.int32, (n, lanes), 1) < hd
    mid = piece // 2

    def attend(s, half):
        blocks = jnp.where(half == 0, c + 1, pieces - c)
        for i in range(qh):
            rs = slice(i * piece, (i + 1) * piece)
            mx[rs] = jnp.full((piece, mid), -jnp.inf, F32)

        def scores(j, diag):
            for i in range(qh):
                rs = slice(i * piece, (i + 1) * piece)
                sc = mm_nt(qs[s, half, rs, :], kv[s, j])
                if diag:
                    sc = jnp.where(causal, sc, -jnp.inf)
                sbuf[j, rs, :] = sc
                mx[rs] = jnp.maximum(mx[rs], jnp.maximum(sc[:, :mid], sc[:, mid:]))

        def one(j, _):
            scores(j, False)
            return 0

        lax.fori_loop(0, blocks - 1, one, 0)
        scores(blocks - 1, True)
        for i in range(qh):
            rs = slice(i * piece, (i + 1) * piece)
            mx[rs] = jnp.broadcast_to(jnp.max(mx[rs], axis=1, keepdims=True), (piece, mid))
            lsum[rs] = jnp.zeros((piece, mid), F32)
            acc[rs] = jnp.zeros((piece, lanes), F32)

        def two(j, _):
            for i in range(qh):
                rs = slice(i * piece, (i + 1) * piece)
                top = mx[rs]
                pa = jnp.exp((sbuf[j, rs, :mid] - top) * scale)
                pb = jnp.exp((sbuf[j, rs, mid:] - top) * scale)
                lsum[rs] += pa + pb
                acc[rs] += mm(jnp.concatenate([pa, pb], axis=1).astype(BF16), kv[s, j])
            return 0

        lax.fori_loop(0, blocks, two, 0)
        for u in range(hslots):
            heads = []
            for i in range(qh):
                rs = slice(i * piece + u * n, i * piece + (u + 1) * n)
                heads.append(acc[rs] / jnp.sum(lsum[rs], axis=1, keepdims=True))
            for b in range(0, qh, 2):
                if b + 1 < qh:
                    both = jnp.where(lane_lo, heads[b], pltpu.roll(heads[b + 1], hd, 1))
                else:
                    both = jnp.where(lane_lo, heads[b], 0.0)
                osend[s, half * hslots + u, :, b * hd:b * hd + lanes] = both.astype(BF16)
        for u in range(hslots):
            dst = half * hslots + u

            @pl.when(dst != t)
            def _():
                rcopy(osend.at[s, dst], orecv.at[s, t], os_sem.at[s, dst], or_sem.at[s, t], c, dst).start()

            @pl.when(dst == t)
            def _():
                orecv[s, t] = osend[s, t]

    for s in range(seqs):
        for i in range(1, cps):
            r = (c + i) % cps
            kv_copy(s, 0, c, r).wait_recv()

            @pl.when(r > c)
            def _():
                kv_copy(s, 1, c, r).wait_recv()

        def half_body(half, _, s=s):
            attend(s, half)
            return 0

        lax.fori_loop(0, 2, half_body, 0)

    relay(wg_parts)
    finish(wg_parts)

    def exchange(src, dst, ss, rs):
        def go(i, _):
            g = (me + i) % group
            rcopy(src.at[g], dst.at[me], ss, rs, g // tps, g % tps).start()
            return 0

        lax.fori_loop(1, group, go, 0)
        dst[me] = src[me]

    def arrived(dst, rs):
        part = dst.at[pl.ds(0, group - 1)]
        rcopy(part, part, rs, rs, c, t).wait_recv()

    def left_all(src, ss):
        part = src.at[pl.ds(0, group - 1)]
        rcopy(part, part, ss, ss, c, t).wait_send()

    for s in range(seqs):
        for i in range(1, tps):
            src = (t + i) % tps
            rcopy(orecv.at[s, src], orecv.at[s, src], os_sem.at[s, src], or_sem.at[s, src], c, src).wait_recv()
        total = xf[s, t].astype(F32)
        added = None
        for u in range(tps):
            term = mm(orecv[s, u][:, :kdim], wof[u])
            added = term if added is None else added + term
        mid_rows = (total + added).astype(BF16)
        hbuf[s] = mid_rows
        dsend[s] = mm(onehot[s], mid_rows).reshape(group, cap, hid).astype(BF16)
        exchange(dsend.at[s], drecv.at[s], ds_sem.at[s], dr_sem.at[s])

    for cp in ld_exp:
        cp.wait()
    for s in range(seqs):
        arrived(drecv.at[s], dr_sem.at[s])
        rows = drecv[s].astype(F32).reshape(group * cap, hid).astype(BF16)
        act = (jax.nn.silu(mm(rows, wg[...])) * mm(rows, wu[...])).astype(BF16)
        rsend[s] = mm(act, wd[...]).reshape(group, cap, hid).astype(BF16)
        exchange(rsend.at[s], rrecv.at[s], rs_sem.at[s], rr_sem.at[s])

    for s in range(seqs):
        arrived(rrecv.at[s], rr_sem.at[s])
        z = mm(onehot_t[s], rrecv[s].astype(F32).reshape(group * cap, hid).astype(BF16))
        g0 = gcol[s, 0][:, :1]
        g1 = gcol[s, 1][:, :1]
        y_ref[s] = (hbuf[s].astype(F32) + (g0 * z[:n] + g1 * z[n:])).astype(BF16)

    for s in range(seqs):
        for k in range(11):
            xg[s][2](k)
        for half in range(2):
            for i in range(1, cps):
                r = (c + i) % cps
                if half == 0:
                    kv_copy(s, half, r, c).wait_send()
                else:
                    @pl.when(r < c)
                    def _():
                        kv_copy(s, half, r, c).wait_send()
        for i in range(1, tps):
            dst = (t + i) % tps
            rcopy(osend.at[s, dst], orecv.at[s, t], os_sem.at[s, dst], or_sem.at[s, t], c, dst).wait_send()
        left_all(dsend.at[s], ds_sem.at[s])
        left_all(rsend.at[s], rs_sem.at[s])
    for k in range(11):
        wg_parts[2](k)


def solution(mesh):
    cps = mesh.shape['cp']
    tps = mesh.shape['tp']
    experts = cps * tps
    row_spec = P(None, ('data', 'cp', 'tp'), None)
    head_spec = P(None, 'tp', None)
    out_spec = P('tp', None, None)
    expert_spec = P(('cp', 'tp'), None, None)

    def device_step(act_in, route_ids, route_gates, w_query, w_key, w_value, w_out, w_gate, w_up, w_down):
        seqs, n, hid = act_in.shape
        qh, hd = w_query.shape[1], w_query.shape[2]
        ff = w_gate.shape[2]
        cap = (4 * n) // experts
        kdim = qh * hd
        lanes = 2 * hd
        hslots = tps // 2
        piece = n * hslots
        wq = jnp.transpose(w_query, (1, 2, 0)).reshape(kdim, hid)
        wk = jnp.transpose(w_key, (1, 2, 0)).reshape(hd, hid)
        wv = jnp.transpose(w_value, (1, 2, 0)).reshape(hd, hid)
        ids = jnp.transpose(route_ids, (0, 2, 1))
        gates = jnp.transpose(route_gates, (0, 2, 1))
        dims = (cps, tps, seqs, n, hid, hd, qh, cap)
        owid = lanes * ((qh + 1) // 2)
        vm = pl.BlockSpec(memory_space=pltpu.VMEM)
        anym = pl.BlockSpec(memory_space=pl.ANY)
        dma = pltpu.SemaphoreType.DMA
        scratch = [
            pltpu.VMEM((seqs, tps, n, hid), BF16),
            pltpu.VMEM((lanes * (qh + 1), hid), BF16),
            pltpu.VMEM((seqs, 2 * cps, piece, lanes), BF16),
            pltpu.VMEM((seqs, 2, qh * piece, lanes), BF16),
            pltpu.VMEM((2 * cps, qh * piece, piece), F32),
            pltpu.VMEM((qh * piece, piece // 2), F32),
            pltpu.VMEM((qh * piece, piece // 2), F32),
            pltpu.VMEM((qh * piece, lanes), F32),
            pltpu.VMEM((seqs, tps, n, owid), BF16),
            pltpu.VMEM((seqs, tps, n, owid), BF16),
            pltpu.VMEM((tps, kdim, hid), BF16),
            pltpu.VMEM((seqs, experts * cap, n), BF16),
            pltpu.VMEM((seqs, 2 * n, experts * cap), BF16),
            pltpu.VMEM((seqs, 2, n, 128), F32),
            pltpu.VMEM((seqs, n, hid), BF16),
            pltpu.VMEM((seqs, experts, cap, hid), BF16),
            pltpu.VMEM((seqs, experts, cap, hid), BF16),
            pltpu.VMEM((seqs, experts, cap, hid), BF16),
            pltpu.VMEM((seqs, experts, cap, hid), BF16),
            pltpu.VMEM((hid, ff), BF16),
            pltpu.VMEM((hid, ff), BF16),
            pltpu.VMEM((ff, hid), BF16),
            dma((8 + qh,)),
            dma((seqs, 11)), dma((seqs, 11)),
            dma((11,)), dma((11,)),
            dma((seqs, 2, cps)), dma((seqs, 2, cps)),
            dma((seqs, tps)), dma((seqs, tps)),
            dma((seqs,)), dma((seqs,)),
            dma((seqs,)), dma((seqs,)),
        ]
        return pl.pallas_call(
            functools.partial(layer_kernel, dims),
            out_shape=jax.ShapeDtypeStruct((seqs, n, hid), BF16),
            in_specs=[anym, vm, vm, anym, anym, anym, anym, anym, anym, anym],
            out_specs=vm,
            scratch_shapes=scratch,
            compiler_params=pltpu.CompilerParams(collective_id=0, has_side_effects=True, vmem_limit_bytes=58 * 1024 * 1024),
            name='layer',
        )(act_in, ids, gates, wq, wk, wv, w_out.reshape(kdim, hid), w_gate[0], w_up[0], w_down[0])

    return jax.shard_map(device_step, mesh=mesh, in_specs=(row_spec, row_spec, row_spec, head_spec, head_spec, head_spec, out_spec, expert_spec, expert_spec, expert_spec), out_specs=row_spec, check_vma=False)
```

```python
import functools

import jax
import jax.numpy as jnp
from jax import lax
from jax.experimental import pallas as pl
from jax.experimental.pallas import tpu as pltpu
from jax.sharding import PartitionSpec as P

MESH = pl.DeviceIdType.MESH
scope = jax.named_scope
F32 = jnp.float32
BF16 = jnp.bfloat16
NT = (((1,), (1,)), ((), ()))


def mm(a, b):
    return jnp.dot(a, b, preferred_element_type=F32)


def mm_nt(a, b):
    return lax.dot_general(a, b, NT, preferred_element_type=F32)


def layer_kernel(dims, x_hbm, ids_ref, gates_ref, wq_hbm, wk_hbm, wv_hbm, wo_hbm, wg_hbm, wu_hbm, wd_hbm, y_ref,
                 xf, wqkv, kv, qs, sbuf, mx, lsum, acc, osend, orecv, wof, onehot, onehot_t, gcol, hbuf,
                 dsend, drecv, rsend, rrecv, wg, wu, wd,
                 loc_sem, xs_sem, xr_sem, ws_sem, wr_sem, vs_sem, vr_sem, ss_sem, sr_sem, ks_sem, kr_sem, os_sem, or_sem,
                 ds_sem, dr_sem, rs_sem, rr_sem):
    cps, tps, seqs, n, hid, hd, qh, cap = dims
    experts = cps * tps
    group = experts
    chips = tps // 2
    hslots = tps // 2
    piece = n * hslots
    pieces = 2 * cps
    lanes = 2 * hd
    qrows = qh * piece
    kdim = qh * hd
    c = lax.axis_index('cp')
    t = lax.axis_index('tp')
    me = c * tps + t
    xc = t // 2
    core = t % 2

    unit = hid // (cps + 2)

    def slot(dx, other):
        return (xc + dx) % chips, (core if not other else 1 - core)

    def flat(sl):
        return sl[0] * 2 + sl[1]

    right, left, sib = slot(1, False), slot(chips - 1, False), slot(0, True)
    own, opposite = (xc, core), slot(2, False)

    def rcopy(src, dst, ssem, rsem, cc, tt):
        return pltpu.make_async_remote_copy(src_ref=src, dst_ref=dst, send_sem=ssem, recv_sem=rsem,
                                            device_id={'cp': cc, 'tp': tt}, device_id_type=MESH)

    def load(src, dst, i):
        cp = pltpu.make_async_copy(src, dst, loc_sem.at[i])
        cp.start()
        return cp

    ld_x = [load(x_hbm.at[s], xf.at[s, xc, core], s) for s in range(seqs)]
    ld_wo = load(wo_hbm, wof.at[xc, core], 2)
    ld_qkv = [load(wv_hbm, wqkv.at[pl.ds(0, hd)], 3), load(wk_hbm, wqkv.at[pl.ds(hd, hd)], 4)]
    for i in range(qh):
        ld_qkv.append(load(wq_hbm.at[pl.ds(i * hd, hd)], wqkv.at[pl.ds(lanes * (i + 1) + hd, hd)], 5 + i))
    ld_exp = [load(wg_hbm, wg, 5 + qh), load(wu_hbm, wu, 6 + qh), load(wd_hbm, wd, 7 + qh)]

    barrier = pltpu.get_barrier_semaphore()

    def sig(i, _):
        g = (me + i) % group
        pl.semaphore_signal(barrier, inc=1, device_id={'cp': g // tps, 'tp': g % tps}, device_id_type=MESH)
        return 0

    lax.fori_loop(1, group, sig, 0)
    pl.semaphore_wait(barrier, group - 1)

    def gather(get, ss, rs):
        l2, r2, o2 = slot(chips - 1, True), slot(1, True), slot(2, True)
        sends = [
            (own, 'lo', right), (own, 'hi', right), (own, 'hi', left), (own, 'lo', left),
            (left, 'lo', right), (right, 'hi', left),
            (own, 'all', sib), (left, 'all', sib), (right, 'all', sib), (opposite, 'lo', sib), (opposite, 'hi', sib),
        ]
        gets = [
            (left, 'lo'), (left, 'hi'), (right, 'hi'), (right, 'lo'),
            (opposite, 'lo'), (opposite, 'hi'),
            (sib, 'all'), (l2, 'all'), (r2, 'all'), (o2, 'lo'), (o2, 'hi'),
        ]

        def copy(sl, part, kind, dst):
            return rcopy(get(sl, part), get(sl, part), ss.at[kind], rs.at[kind], c, flat(dst))

        def start(*kinds):
            for k in kinds:
                copy(*sends[k][:2], k, sends[k][2]).start()

        def got(*kinds):
            for k in kinds:
                copy(*gets[k], k, sib).wait_recv()

        def sent(*kinds):
            for k in kinds:
                copy(*sends[k][:2], k, sends[k][2]).wait_send()

        return start, got, sent

    def rows_of(rows):
        return {'lo': pl.ds(0, rows // 2), 'hi': pl.ds(rows // 2, rows // 2), 'all': pl.ds(0, rows)}

    xparts, wparts = rows_of(n), rows_of(kdim)
    xg = [gather(lambda sl, part, s=s: xf.at[s, sl[0], sl[1], xparts[part]], xs_sem.at[s], xr_sem.at[s]) for s in range(seqs)]

    cols_a = pl.ds(0, 2 * unit)

    def cols_b(r):
        return pl.ds(pl.multiple_of((r + 2) * unit, unit), unit)

    wa = gather(lambda sl, part: wof.at[sl[0], sl[1], wparts[part], cols_a], ws_sem.at[0], wr_sem.at[0])
    wb = gather(lambda sl, part: wof.at[sl[0], sl[1], wparts[part], cols_b(c)], ws_sem.at[1], wr_sem.at[1])
    up, down, across = (c + 1) % cps, (c + cps - 1) % cps, (c + 2) % cps

    def spread(q, sl):
        sends = [(c, 'lo', up), (c, 'hi', up), (c, 'hi', down), (c, 'lo', down), (down, 'lo', up), (up, 'hi', down)]
        gets = [(down, 'lo'), (down, 'hi'), (up, 'hi'), (up, 'lo'), (across, 'lo'), (across, 'hi')]

        def copy(r, part, kind, dst):
            ref = wof.at[sl[0], sl[1], wparts[part], cols_b(r)]
            return rcopy(ref, ref, vs_sem.at[q, kind], vr_sem.at[q, kind], dst, t)

        def start(*kinds):
            for k in kinds:
                copy(*sends[k][:2], k, sends[k][2]).start()

        def got(*kinds):
            for k in kinds:
                copy(*gets[k], k, up).wait_recv()

        def sent(*kinds):
            for k in kinds:
                copy(*sends[k][:2], k, sends[k][2]).wait_send()

        return start, got, sent

    wy = [spread(q, sl) for q, sl in enumerate((left, right, opposite))]

    def share(b, mine):
        cr = core if mine else 1 - core
        blk = cols_a if b is None else cols_b(b)
        ref = wof.at[:, cr, :, blk]
        k = cps if b is None else b
        return rcopy(ref, ref, ss_sem.at[k], sr_sem.at[k], c, flat(sib))

    ld_x[0].wait()
    xg[0][0](0, 2, 1, 3, 6)
    ld_x[1].wait()
    xg[1][0](0, 2)

    ecol = lax.broadcasted_iota(jnp.int32, (experts, n), 0)
    later = (lax.broadcasted_iota(jnp.int32, (n, n), 0) < lax.broadcasted_iota(jnp.int32, (n, n), 1)).astype(F32).astype(BF16)
    srow = lax.broadcasted_iota(jnp.int32, (experts * cap, n), 0)
    eye = lax.broadcasted_iota(jnp.int32, (n, n), 0) == lax.broadcasted_iota(jnp.int32, (n, n), 1)
    for s in range(seqs):
        first = jnp.zeros((experts, 1), F32)
        both = None
        for k in range(2):
            idk = ids_ref[s, k:k + 1, :]
            hits = (ecol == idk).astype(F32)
            before = mm(hits.astype(BF16), later) + first
            rank = jnp.sum(hits * before, axis=0, keepdims=True).astype(jnp.int32)
            first = first + jnp.sum(hits, axis=1, keepdims=True)
            dest = idk * cap + rank
            pick = (srow == dest).astype(F32)
            both = pick if both is None else both + pick
            onehot_t[s, k * n:(k + 1) * n, :] = pick.T.astype(BF16)
            gcol[s, k] = jnp.broadcast_to(jnp.sum(jnp.where(eye, gates_ref[s, k:k + 1, :], 0.0), axis=1, keepdims=True), (n, 128))
        onehot[s] = both.astype(BF16)
    for i in range(qh):
        wqkv[lanes * (i + 1):lanes * (i + 1) + hd, :] = jnp.zeros((hd, hid), BF16)

    def kv_piece(half):
        return c if half == 0 else pieces - 1 - c

    def kv_copy(s, half, r, src):
        ref = kv.at[s, src if half == 0 else pieces - 1 - src]
        return rcopy(ref, ref, ks_sem.at[s, half, r], kr_sem.at[s, half, src], r, t)

    def project(s):
        for half in range(2):
            rows = xf[s, half * (chips // 2):(half + 1) * (chips // 2)].reshape(piece, hid)
            out = mm_nt(rows, wqkv[...])
            kv[s, kv_piece(half)] = out[:, :lanes].astype(BF16)
            for i in range(qh):
                qs[s, half, i * piece:(i + 1) * piece, :] = out[:, lanes * (i + 1):lanes * (i + 2)].astype(BF16)
            for i in range(1, cps):
                r = (c + i) % cps
                if half == 0:
                    kv_copy(s, half, r, c).start()
                else:
                    @pl.when(r < c)
                    def _():
                        kv_copy(s, half, r, c).start()

    with scope('xrelay0'):
        start, got, _ = xg[0]
        got(0)
        start(4)
        got(2)
        start(5)
        xg[1][0](1, 3, 6)
        got(1)
        start(7)
        got(3)
        start(8)
    with scope('xrelay1'):
        xg[1][1](0)
        xg[1][0](4)
        xg[1][1](2)
        xg[1][0](5)
    with scope('xfinish0'):
        start, got, _ = xg[0]
        got(4)
        start(9)
        got(5)
        start(10)
        for cp in ld_qkv:
            cp.wait()
        ld_wo.wait()
        wb[0](0, 2, 1, 3)
        wa[0](0, 2, 1, 3)
        got(6, 7, 8, 9, 10)
    with scope('qkv0'):
        project(0)
    with scope('xfinish1'):
        start, got, _ = xg[1]
        got(1)
        start(7)
        got(3)
        start(8)
        got(4)
        start(9)
        got(5)
        start(10)
        got(6, 7, 8, 9, 10)
    with scope('qkv1'):
        project(1)

    scale = hd ** -0.5
    causal = lax.broadcasted_iota(jnp.int32, (piece, piece), 1) <= lax.broadcasted_iota(jnp.int32, (piece, piece), 0)
    lane_lo = lax.broadcasted_iota(jnp.int32, (n, lanes), 1) < hd
    mid = piece // 2

    def attend(s, half):
        blocks = c + 1 if half == 0 else pieces - c
        for i in range(qh):
            rs = slice(i * piece, (i + 1) * piece)
            mx[rs] = jnp.full((piece, mid), -jnp.inf, F32)

        def scores(j, diag):
            for i in range(qh):
                rs = slice(i * piece, (i + 1) * piece)
                sc = mm_nt(qs[s, half, rs, :], kv[s, j])
                if diag:
                    sc = jnp.where(causal, sc, -jnp.inf)
                sbuf[j, rs, :] = sc
                mx[rs] = jnp.maximum(mx[rs], jnp.maximum(sc[:, :mid], sc[:, mid:]))

        def one(j, _):
            scores(j, False)
            return 0

        lax.fori_loop(0, blocks - 1, one, 0)
        scores(blocks - 1, True)
        for i in range(qh):
            rs = slice(i * piece, (i + 1) * piece)
            mx[rs] = jnp.broadcast_to(jnp.max(mx[rs], axis=1, keepdims=True), (piece, mid))
            lsum[rs] = jnp.zeros((piece, mid), F32)
            acc[rs] = jnp.zeros((piece, lanes), F32)

        def two(j, _):
            for i in range(qh):
                rs = slice(i * piece, (i + 1) * piece)
                top = mx[rs]
                pa = jnp.exp((sbuf[j, rs, :mid] - top) * scale)
                pb = jnp.exp((sbuf[j, rs, mid:] - top) * scale)
                lsum[rs] += pa + pb
                acc[rs] += mm(jnp.concatenate([pa, pb], axis=1).astype(BF16), kv[s, j])
            return 0

        lax.fori_loop(0, blocks, two, 0)
        for u in range(hslots):
            heads = []
            for i in range(qh):
                rs = slice(i * piece + u * n, i * piece + (u + 1) * n)
                heads.append(acc[rs] / jnp.sum(lsum[rs], axis=1, keepdims=True))
            for b in range(0, qh, 2):
                if b + 1 < qh:
                    both = jnp.where(lane_lo, heads[b], pltpu.roll(heads[b + 1], hd, 1))
                else:
                    both = jnp.where(lane_lo, heads[b], 0.0)
                osend[s, half * hslots + u, :, b * hd:b * hd + lanes] = both.astype(BF16)
        for u in range(hslots):
            dst = half * hslots + u

            @pl.when(dst != t)
            def _():
                rcopy(osend.at[s, dst], orecv.at[s, t], os_sem.at[s, dst], or_sem.at[s, t], c, dst).start()

            @pl.when(dst == t)
            def _():
                orecv[s, t] = osend[s, dst]

    def kv_wait(s):
        for i in range(1, cps):
            r = (c + i) % cps
            kv_copy(s, 0, c, r).wait_recv()

            @pl.when(r > c)
            def _():
                kv_copy(s, 1, c, r).wait_recv()

    def exchange(src, dst, ss, rs):
        def go(i, _):
            g = (me + i) % group
            rcopy(src.at[g], dst.at[me], ss, rs, g // tps, g % tps).start()
            return 0

        lax.fori_loop(1, group, go, 0)
        dst[me] = src[me]

    def arrived(dst, rs):
        part = dst.at[pl.ds(0, group - 1)]
        rcopy(part, part, rs, rs, c, t).wait_recv()

    def left_all(src, ss):
        part = src.at[pl.ds(0, group - 1)]
        rcopy(part, part, ss, ss, c, t).wait_send()

    def out_rows(s):
        for i in range(1, tps):
            src = (t + i) % tps
            rcopy(orecv.at[s, src], orecv.at[s, src], os_sem.at[s, src], or_sem.at[s, src], c, src).wait_recv()
        total = xf[s, xc, core].astype(F32)
        added = None
        for u in range(tps):
            term = mm(orecv[s, u][:, :kdim], wof[u // 2, u % 2])
            added = term if added is None else added + term
        mid_rows = (total + added).astype(BF16)
        hbuf[s] = mid_rows
        dsend[s] = mm(onehot[s], mid_rows).reshape(group, cap, hid).astype(BF16)
        exchange(dsend.at[s], drecv.at[s], ds_sem.at[s], dr_sem.at[s])

    with scope('wb1'):
        wb[1](0)
        wb[0](4)
        wb[1](2)
        wb[0](5)
        wb[1](1, 3)
        wy[0][0](0, 2, 1, 3)
        wy[1][0](0, 2, 1, 3)
    with scope('kvwait0'):
        kv_wait(0)
    with scope('attend01'):
        attend(0, 1)
    with scope('wb2'):
        wb[1](4, 5)
        wy[2][0](0, 2, 1, 3)
        share(c, True).start()
        wa[1](0)
        wa[0](4)
        wa[1](2)
        wa[0](5)
        wa[1](1, 3)
    with scope('attend00'):
        attend(0, 0)
    with scope('wy1'):
        for q in range(2):
            wy[q][1](0)
            wy[q][0](4)
            wy[q][1](2)
            wy[q][0](5)
            wy[q][1](1, 3)
    with scope('kvwait1'):
        kv_wait(1)
    with scope('attend11'):
        attend(1, 1)
    with scope('wy2'):
        wy[2][1](0)
        wy[2][0](4)
        wy[2][1](2)
        wy[2][0](5)
        wa[1](4, 5)
        share(None, True).start()
        wy[2][1](1, 3)
        share(down, True).start()
        share(up, True).start()
        for q in range(3):
            wy[q][1](4, 5)
        share(across, True).start()
    with scope('wshare'):
        for b in (c, None, down, up, across):
            share(b, False).wait_recv()
    with scope('out0'):
        out_rows(0)
    with scope('attend10'):
        attend(1, 0)
    with scope('out1'):
        out_rows(1)

    for cp in ld_exp:
        cp.wait()
    for s in range(seqs):
        with scope(f'dwait{s}'):
            arrived(drecv.at[s], dr_sem.at[s])
        rows = drecv[s].astype(F32).reshape(group * cap, hid).astype(BF16)
        act = (jax.nn.silu(mm(rows, wg[...])) * mm(rows, wu[...])).astype(BF16)
        rsend[s] = mm(act, wd[...]).reshape(group, cap, hid).astype(BF16)
        exchange(rsend.at[s], rrecv.at[s], rs_sem.at[s], rr_sem.at[s])

    for s in range(seqs):
        with scope(f'rwait{s}'):
            arrived(rrecv.at[s], rr_sem.at[s])
        z = mm(onehot_t[s], rrecv[s].astype(F32).reshape(group * cap, hid).astype(BF16))
        g0 = gcol[s, 0][:, :1]
        g1 = gcol[s, 1][:, :1]
        y_ref[s] = (hbuf[s].astype(F32) + (g0 * z[:n] + g1 * z[n:])).astype(BF16)

    for s in range(seqs):
        xg[s][2](*range(11))
        for half in range(2):
            for i in range(1, cps):
                r = (c + i) % cps
                if half == 0:
                    kv_copy(s, half, r, c).wait_send()
                else:
                    @pl.when(r < c)
                    def _():
                        kv_copy(s, half, r, c).wait_send()
        for i in range(1, tps):
            dst = (t + i) % tps
            rcopy(osend.at[s, dst], orecv.at[s, t], os_sem.at[s, dst], or_sem.at[s, t], c, dst).wait_send()
        left_all(dsend.at[s], ds_sem.at[s])
        left_all(rsend.at[s], rs_sem.at[s])
    for part in (wa, wb, *wy):
        part[2](*range(6))
    for b in (c, None, down, up, across):
        share(b, True).wait_send()


def solution(mesh):
    cps = mesh.shape['cp']
    tps = mesh.shape['tp']
    experts = cps * tps
    row_spec = P(None, ('data', 'cp', 'tp'), None)
    head_spec = P(None, 'tp', None)
    out_spec = P('tp', None, None)
    expert_spec = P(('cp', 'tp'), None, None)

    def device_step(act_in, route_ids, route_gates, w_query, w_key, w_value, w_out, w_gate, w_up, w_down):
        seqs, n, hid = act_in.shape
        qh, hd = w_query.shape[1], w_query.shape[2]
        ff = w_gate.shape[2]
        cap = (4 * n) // experts
        kdim = qh * hd
        lanes = 2 * hd
        hslots = tps // 2
        piece = n * hslots
        wq = jnp.transpose(w_query, (1, 2, 0)).reshape(kdim, hid)
        wk = jnp.transpose(w_key, (1, 2, 0)).reshape(hd, hid)
        wv = jnp.transpose(w_value, (1, 2, 0)).reshape(hd, hid)
        ids = jnp.transpose(route_ids, (0, 2, 1))
        gates = jnp.transpose(route_gates, (0, 2, 1))
        dims = (cps, tps, seqs, n, hid, hd, qh, cap)
        owid = lanes * ((qh + 1) // 2)
        vm = pl.BlockSpec(memory_space=pltpu.VMEM)
        anym = pl.BlockSpec(memory_space=pl.ANY)
        dma = pltpu.SemaphoreType.DMA
        scratch = [
            pltpu.VMEM((seqs, tps // 2, 2, n, hid), BF16),
            pltpu.VMEM((lanes * (qh + 1), hid), BF16),
            pltpu.VMEM((seqs, 2 * cps, piece, lanes), BF16),
            pltpu.VMEM((seqs, 2, qh * piece, lanes), BF16),
            pltpu.VMEM((2 * cps, qh * piece, piece), F32),
            pltpu.VMEM((qh * piece, piece // 2), F32),
            pltpu.VMEM((qh * piece, piece // 2), F32),
            pltpu.VMEM((qh * piece, lanes), F32),
            pltpu.VMEM((seqs, tps, n, owid), BF16),
            pltpu.VMEM((seqs, tps, n, owid), BF16),
            pltpu.VMEM((tps // 2, 2, kdim, hid), BF16),
            pltpu.VMEM((seqs, experts * cap, n), BF16),
            pltpu.VMEM((seqs, 2 * n, experts * cap), BF16),
            pltpu.VMEM((seqs, 2, n, 128), F32),
            pltpu.VMEM((seqs, n, hid), BF16),
            pltpu.VMEM((seqs, experts, cap, hid), BF16),
            pltpu.VMEM((seqs, experts, cap, hid), BF16),
            pltpu.VMEM((seqs, experts, cap, hid), BF16),
            pltpu.VMEM((seqs, experts, cap, hid), BF16),
            pltpu.VMEM((hid, ff), BF16),
            pltpu.VMEM((hid, ff), BF16),
            pltpu.VMEM((ff, hid), BF16),
            dma((8 + qh,)),
            dma((seqs, 11)), dma((seqs, 11)),
            dma((2, 6)), dma((2, 6)),
            dma((3, 6)), dma((3, 6)),
            dma((cps + 1,)), dma((cps + 1,)),
            dma((seqs, 2, cps)), dma((seqs, 2, cps)),
            dma((seqs, tps)), dma((seqs, tps)),
            dma((seqs,)), dma((seqs,)),
            dma((seqs,)), dma((seqs,)),
        ]
        return pl.pallas_call(
            functools.partial(layer_kernel, dims),
            out_shape=jax.ShapeDtypeStruct((seqs, n, hid), BF16),
            in_specs=[anym, vm, vm, anym, anym, anym, anym, anym, anym, anym],
            out_specs=vm,
            scratch_shapes=scratch,
            compiler_params=pltpu.CompilerParams(collective_id=0, has_side_effects=True, vmem_limit_bytes=58 * 1024 * 1024),
            name='layer',
        )(act_in, ids, gates, wq, wk, wv, w_out.reshape(kdim, hid), w_gate[0], w_up[0], w_down[0])

    return jax.shard_map(device_step, mesh=mesh, in_specs=(row_spec, row_spec, row_spec, head_spec, head_spec, head_spec, out_spec, expert_spec, expert_spec, expert_spec), out_specs=row_spec, check_vma=False)
```

```python
import functools

import jax
import jax.numpy as jnp
from jax import lax
from jax.experimental import pallas as pl
from jax.experimental.pallas import tpu as pltpu
from jax.sharding import PartitionSpec as P

MESH = pl.DeviceIdType.MESH
scope = jax.named_scope
F32 = jnp.float32
BF16 = jnp.bfloat16
NT = (((1,), (1,)), ((), ()))


def mm(a, b):
    return jnp.dot(a, b, preferred_element_type=F32)


def mm_nt(a, b):
    return lax.dot_general(a, b, NT, preferred_element_type=F32)


def layer_kernel(dims, x_hbm, ids_ref, gates_ref, wq_hbm, wk_hbm, wv_hbm, wo_hbm, wg_hbm, wu_hbm, wd_hbm, y_ref,
                 xf, wqkv, kv, qs, sbuf, mx, lsum, acc, osend, orecv, wof, onehot, onehot_t, gcol, hbuf,
                 dsend, drecv, rsend, rrecv, wg, wu, wd,
                 loc_sem, xs_sem, xr_sem, ws_sem, wr_sem, vs_sem, vr_sem, ss_sem, sr_sem, ks_sem, kr_sem, os_sem, or_sem,
                 ds_sem, dr_sem, rs_sem, rr_sem):
    cps, tps, seqs, n, hid, hd, qh, cap = dims
    experts = cps * tps
    group = experts
    chips = tps // 2
    hslots = tps // 2
    piece = n * hslots
    pieces = 2 * cps
    lanes = 2 * hd
    qrows = qh * piece
    kdim = qh * hd
    c = lax.axis_index('cp')
    t = lax.axis_index('tp')
    me = c * tps + t
    xc = t // 2
    core = t % 2

    unit = hid // (3 * cps)

    def slot(dx, other):
        return (xc + dx) % chips, (core if not other else 1 - core)

    def flat(sl):
        return sl[0] * 2 + sl[1]

    right, left, sib = slot(1, False), slot(chips - 1, False), slot(0, True)
    own, opposite = (xc, core), slot(2, False)

    def rcopy(src, dst, ssem, rsem, cc, tt):
        return pltpu.make_async_remote_copy(src_ref=src, dst_ref=dst, send_sem=ssem, recv_sem=rsem,
                                            device_id={'cp': cc, 'tp': tt}, device_id_type=MESH)

    def load(src, dst, i):
        cp = pltpu.make_async_copy(src, dst, loc_sem.at[i])
        cp.start()
        return cp

    ld_x = [load(x_hbm.at[s], xf.at[s, xc, core], s) for s in range(seqs)]
    ld_wo = load(wo_hbm, wof.at[xc, core], 2)
    ld_qkv = [load(wv_hbm, wqkv.at[pl.ds(0, hd)], 3), load(wk_hbm, wqkv.at[pl.ds(hd, hd)], 4)]
    for i in range(qh):
        ld_qkv.append(load(wq_hbm.at[pl.ds(i * hd, hd)], wqkv.at[pl.ds(lanes * (i + 1) + hd, hd)], 5 + i))
    ld_exp = [load(wg_hbm, wg, 5 + qh), load(wu_hbm, wu, 6 + qh), load(wd_hbm, wd, 7 + qh)]

    barrier = pltpu.get_barrier_semaphore()

    def sig(i, _):
        g = (me + i) % group
        pl.semaphore_signal(barrier, inc=1, device_id={'cp': g // tps, 'tp': g % tps}, device_id_type=MESH)
        return 0

    lax.fori_loop(1, group, sig, 0)
    pl.semaphore_wait(barrier, group - 1)

    def gather(get, ss, rs):
        l2, r2, o2 = slot(chips - 1, True), slot(1, True), slot(2, True)
        sends = [
            (own, 'lo', right), (own, 'hi', right), (own, 'hi', left), (own, 'lo', left),
            (left, 'lo', right), (right, 'hi', left),
            (own, 'all', sib), (left, 'all', sib), (right, 'all', sib), (opposite, 'lo', sib), (opposite, 'hi', sib),
        ]
        gets = [
            (left, 'lo'), (left, 'hi'), (right, 'hi'), (right, 'lo'),
            (opposite, 'lo'), (opposite, 'hi'),
            (sib, 'all'), (l2, 'all'), (r2, 'all'), (o2, 'lo'), (o2, 'hi'),
        ]

        def copy(sl, part, kind, dst):
            return rcopy(get(sl, part), get(sl, part), ss.at[kind], rs.at[kind], c, flat(dst))

        def start(*kinds):
            for k in kinds:
                copy(*sends[k][:2], k, sends[k][2]).start()

        def got(*kinds):
            for k in kinds:
                copy(*gets[k], k, sib).wait_recv()

        def sent(*kinds):
            for k in kinds:
                copy(*sends[k][:2], k, sends[k][2]).wait_send()

        return start, got, sent

    def rows_of(rows):
        return {'lo': pl.ds(0, rows // 2), 'hi': pl.ds(rows // 2, rows // 2), 'all': pl.ds(0, rows)}

    xparts, wparts = rows_of(n), rows_of(kdim)
    xg = [gather(lambda sl, part, s=s: xf.at[s, sl[0], sl[1], xparts[part]], xs_sem.at[s], xr_sem.at[s]) for s in range(seqs)]

    cols_a = pl.ds(0, hid - cps * unit)

    def cols_b(r):
        return pl.ds(pl.multiple_of(hid - cps * unit + r * unit, unit), unit)

    wa = gather(lambda sl, part: wof.at[sl[0], sl[1], wparts[part], cols_a], ws_sem.at[0], wr_sem.at[0])
    wb = gather(lambda sl, part: wof.at[sl[0], sl[1], wparts[part], cols_b(c)], ws_sem.at[1], wr_sem.at[1])
    up, down, across = (c + 1) % cps, (c + cps - 1) % cps, (c + 2) % cps

    def spread(q, sl):
        sends = [(c, 'lo', up), (c, 'hi', up), (c, 'hi', down), (c, 'lo', down), (down, 'lo', up), (up, 'hi', down)]
        gets = [(down, 'lo'), (down, 'hi'), (up, 'hi'), (up, 'lo'), (across, 'lo'), (across, 'hi')]

        def copy(r, part, kind, dst):
            ref = wof.at[sl[0], sl[1], wparts[part], cols_b(r)]
            return rcopy(ref, ref, vs_sem.at[q, kind], vr_sem.at[q, kind], dst, t)

        def start(*kinds):
            for k in kinds:
                copy(*sends[k][:2], k, sends[k][2]).start()

        def got(*kinds):
            for k in kinds:
                copy(*gets[k], k, up).wait_recv()

        def sent(*kinds):
            for k in kinds:
                copy(*sends[k][:2], k, sends[k][2]).wait_send()

        return start, got, sent

    wy = [spread(q, sl) for q, sl in enumerate((left, right, opposite))]

    def share(b, mine):
        cr = core if mine else 1 - core
        blk = cols_a if b is None else cols_b(b)
        ref = wof.at[:, cr, :, blk]
        k = cps if b is None else b
        return rcopy(ref, ref, ss_sem.at[k], sr_sem.at[k], c, flat(sib))

    ld_x[0].wait()
    xg[0][0](0, 2, 1, 3, 6)
    ld_x[1].wait()
    xg[1][0](0, 2)

    ecol = lax.broadcasted_iota(jnp.int32, (experts, n), 0)
    later = (lax.broadcasted_iota(jnp.int32, (n, n), 0) < lax.broadcasted_iota(jnp.int32, (n, n), 1)).astype(F32).astype(BF16)
    srow = lax.broadcasted_iota(jnp.int32, (experts * cap, n), 0)
    eye = lax.broadcasted_iota(jnp.int32, (n, n), 0) == lax.broadcasted_iota(jnp.int32, (n, n), 1)
    for s in range(seqs):
        first = jnp.zeros((experts, 1), F32)
        both = None
        for k in range(2):
            idk = ids_ref[s, k:k + 1, :]
            hits = (ecol == idk).astype(F32)
            before = mm(hits.astype(BF16), later) + first
            rank = jnp.sum(hits * before, axis=0, keepdims=True).astype(jnp.int32)
            first = first + jnp.sum(hits, axis=1, keepdims=True)
            dest = idk * cap + rank
            pick = (srow == dest).astype(F32)
            both = pick if both is None else both + pick
            onehot_t[s, k * n:(k + 1) * n, :] = pick.T.astype(BF16)
            gcol[s, k] = jnp.broadcast_to(jnp.sum(jnp.where(eye, gates_ref[s, k:k + 1, :], 0.0), axis=1, keepdims=True), (n, 128))
        onehot[s] = both.astype(BF16)
    for i in range(qh):
        wqkv[lanes * (i + 1):lanes * (i + 1) + hd, :] = jnp.zeros((hd, hid), BF16)

    def kv_piece(half):
        return c if half == 0 else pieces - 1 - c

    def kv_copy(s, half, r, src):
        ref = kv.at[s, src if half == 0 else pieces - 1 - src]
        return rcopy(ref, ref, ks_sem.at[s, half, r], kr_sem.at[s, half, src], r, t)

    def project(s):
        for half in range(2):
            rows = xf[s, half * (chips // 2):(half + 1) * (chips // 2)].reshape(piece, hid)
            out = mm_nt(rows, wqkv[...])
            kv[s, kv_piece(half)] = out[:, :lanes].astype(BF16)
            for i in range(qh):
                qs[s, half, i * piece:(i + 1) * piece, :] = out[:, lanes * (i + 1):lanes * (i + 2)].astype(BF16)
            for i in range(1, cps):
                r = (c + i) % cps
                if half == 0:
                    kv_copy(s, half, r, c).start()
                else:
                    @pl.when(r < c)
                    def _():
                        kv_copy(s, half, r, c).start()

    with scope('xrelay0'):
        start, got, _ = xg[0]
        got(0)
        start(4)
        got(2)
        start(5)
        xg[1][0](1, 3, 6)
        got(1)
        start(7)
        got(3)
        start(8)
    with scope('xrelay1'):
        xg[1][1](0)
        xg[1][0](4)
        xg[1][1](2)
        xg[1][0](5)
    with scope('xfinish0'):
        start, got, _ = xg[0]
        got(4)
        start(9)
        got(5)
        start(10)
        for cp in ld_qkv:
            cp.wait()
        ld_wo.wait()
        wb[0](0, 2, 1, 3)
        wa[0](0, 2, 1, 3)
        got(6, 7, 8, 9, 10)
    with scope('qkv0'):
        project(0)
    with scope('xfinish1'):
        start, got, _ = xg[1]
        got(1)
        start(7)
        got(3)
        start(8)
        got(4)
        start(9)
        got(5)
        start(10)
        got(6, 7, 8, 9, 10)
    with scope('qkv1'):
        project(1)

    scale = hd ** -0.5
    causal = lax.broadcasted_iota(jnp.int32, (piece, piece), 1) <= lax.broadcasted_iota(jnp.int32, (piece, piece), 0)
    lane_lo = lax.broadcasted_iota(jnp.int32, (n, lanes), 1) < hd
    mid = piece // 2

    def attend(s, half):
        blocks = c + 1 if half == 0 else pieces - c
        for i in range(qh):
            rs = slice(i * piece, (i + 1) * piece)
            mx[rs] = jnp.full((piece, mid), -jnp.inf, F32)

        def scores(j, diag):
            for i in range(qh):
                rs = slice(i * piece, (i + 1) * piece)
                sc = mm_nt(qs[s, half, rs, :], kv[s, j])
                if diag:
                    sc = jnp.where(causal, sc, -jnp.inf)
                sbuf[j, rs, :] = sc
                mx[rs] = jnp.maximum(mx[rs], jnp.maximum(sc[:, :mid], sc[:, mid:]))

        def one(j, _):
            scores(j, False)
            return 0

        lax.fori_loop(0, blocks - 1, one, 0)
        scores(blocks - 1, True)
        for i in range(qh):
            rs = slice(i * piece, (i + 1) * piece)
            mx[rs] = jnp.broadcast_to(jnp.max(mx[rs], axis=1, keepdims=True), (piece, mid))
            lsum[rs] = jnp.zeros((piece, mid), F32)
            acc[rs] = jnp.zeros((piece, lanes), F32)

        def two(j, _):
            for i in range(qh):
                rs = slice(i * piece, (i + 1) * piece)
                top = mx[rs]
                pa = jnp.exp((sbuf[j, rs, :mid] - top) * scale)
                pb = jnp.exp((sbuf[j, rs, mid:] - top) * scale)
                lsum[rs] += pa + pb
                acc[rs] += mm(jnp.concatenate([pa, pb], axis=1).astype(BF16), kv[s, j])
            return 0

        lax.fori_loop(0, blocks, two, 0)
        for u in range(hslots):
            heads = []
            for i in range(qh):
                rs = slice(i * piece + u * n, i * piece + (u + 1) * n)
                heads.append(acc[rs] / jnp.sum(lsum[rs], axis=1, keepdims=True))
            for b in range(0, qh, 2):
                if b + 1 < qh:
                    both = jnp.where(lane_lo, heads[b], pltpu.roll(heads[b + 1], hd, 1))
                else:
                    both = jnp.where(lane_lo, heads[b], 0.0)
                osend[s, half * hslots + u, :, b * hd:b * hd + lanes] = both.astype(BF16)
        for u in range(hslots):
            dst = half * hslots + u

            @pl.when(dst != t)
            def _():
                rcopy(osend.at[s, dst], orecv.at[s, t], os_sem.at[s, dst], or_sem.at[s, t], c, dst).start()

            @pl.when(dst == t)
            def _():
                orecv[s, t] = osend[s, dst]

    def kv_wait(s):
        for i in range(1, cps):
            r = (c + i) % cps
            kv_copy(s, 0, c, r).wait_recv()

            @pl.when(r > c)
            def _():
                kv_copy(s, 1, c, r).wait_recv()

    def exchange(src, dst, ss, rs):
        def go(i, _):
            g = (me + i) % group
            rcopy(src.at[g], dst.at[me], ss, rs, g // tps, g % tps).start()
            return 0

        lax.fori_loop(1, group, go, 0)
        dst[me] = src[me]

    def arrived(dst, rs):
        part = dst.at[pl.ds(0, group - 1)]
        rcopy(part, part, rs, rs, c, t).wait_recv()

    def left_all(src, ss):
        part = src.at[pl.ds(0, group - 1)]
        rcopy(part, part, ss, ss, c, t).wait_send()

    def out_rows(s):
        for i in range(1, tps):
            src = (t + i) % tps
            rcopy(orecv.at[s, src], orecv.at[s, src], os_sem.at[s, src], or_sem.at[s, src], c, src).wait_recv()
        total = xf[s, xc, core].astype(F32)
        added = None
        for u in range(tps):
            term = mm(orecv[s, u][:, :kdim], wof[u // 2, u % 2])
            added = term if added is None else added + term
        mid_rows = (total + added).astype(BF16)
        hbuf[s] = mid_rows
        dsend[s] = mm(onehot[s], mid_rows).reshape(group, cap, hid).astype(BF16)
        exchange(dsend.at[s], drecv.at[s], ds_sem.at[s], dr_sem.at[s])

    with scope('wb1'):
        wb[1](0)
        wb[0](4)
        wb[1](2)
        wb[0](5)
        wb[1](1, 3)
        wy[0][0](0, 2, 1, 3)
        wy[1][0](0, 2, 1, 3)
    with scope('kvwait0'):
        kv_wait(0)
    with scope('attend01'):
        attend(0, 1)
    with scope('wb2'):
        wb[1](4, 5)
        wy[2][0](0, 2, 1, 3)
        share(c, True).start()
        wa[1](0)
        wa[0](4)
        wa[1](2)
        wa[0](5)
        wa[1](1, 3)
    with scope('attend00'):
        attend(0, 0)
    with scope('wy1'):
        for q in range(2):
            wy[q][1](0)
            wy[q][0](4)
            wy[q][1](2)
            wy[q][0](5)
            wy[q][1](1, 3)
    with scope('kvwait1'):
        kv_wait(1)
    with scope('attend11'):
        attend(1, 1)
    with scope('wy2'):
        wy[2][1](0)
        wy[2][0](4)
        wy[2][1](2)
        wy[2][0](5)
        wa[1](4, 5)
        share(None, True).start()
        wy[2][1](1, 3)
        share(down, True).start()
        share(up, True).start()
    with scope('attend10'):
        attend(1, 0)
    with scope('wy3'):
        for q in range(3):
            wy[q][1](4, 5)
        share(across, True).start()
    with scope('wshare'):
        for b in (c, None, down, up, across):
            share(b, False).wait_recv()
    with scope('out0'):
        out_rows(0)
    with scope('out1'):
        out_rows(1)

    for cp in ld_exp:
        cp.wait()
    for s in range(seqs):
        with scope(f'dwait{s}'):
            arrived(drecv.at[s], dr_sem.at[s])
        rows = drecv[s].astype(F32).reshape(group * cap, hid).astype(BF16)
        act = (jax.nn.silu(mm(rows, wg[...])) * mm(rows, wu[...])).astype(BF16)
        rsend[s] = mm(act, wd[...]).reshape(group, cap, hid).astype(BF16)
        exchange(rsend.at[s], rrecv.at[s], rs_sem.at[s], rr_sem.at[s])

    for s in range(seqs):
        with scope(f'rwait{s}'):
            arrived(rrecv.at[s], rr_sem.at[s])
        z = mm(onehot_t[s], rrecv[s].astype(F32).reshape(group * cap, hid).astype(BF16))
        g0 = gcol[s, 0][:, :1]
        g1 = gcol[s, 1][:, :1]
        y_ref[s] = (hbuf[s].astype(F32) + (g0 * z[:n] + g1 * z[n:])).astype(BF16)

    for s in range(seqs):
        xg[s][2](*range(11))
        for half in range(2):
            for i in range(1, cps):
                r = (c + i) % cps
                if half == 0:
                    kv_copy(s, half, r, c).wait_send()
                else:
                    @pl.when(r < c)
                    def _():
                        kv_copy(s, half, r, c).wait_send()
        for i in range(1, tps):
            dst = (t + i) % tps
            rcopy(osend.at[s, dst], orecv.at[s, t], os_sem.at[s, dst], or_sem.at[s, t], c, dst).wait_send()
        left_all(dsend.at[s], ds_sem.at[s])
        left_all(rsend.at[s], rs_sem.at[s])
    for part in (wa, wb, *wy):
        part[2](*range(6))
    for b in (c, None, down, up, across):
        share(b, True).wait_send()


def solution(mesh):
    cps = mesh.shape['cp']
    tps = mesh.shape['tp']
    experts = cps * tps
    row_spec = P(None, ('data', 'cp', 'tp'), None)
    head_spec = P(None, 'tp', None)
    out_spec = P('tp', None, None)
    expert_spec = P(('cp', 'tp'), None, None)

    def device_step(act_in, route_ids, route_gates, w_query, w_key, w_value, w_out, w_gate, w_up, w_down):
        seqs, n, hid = act_in.shape
        qh, hd = w_query.shape[1], w_query.shape[2]
        ff = w_gate.shape[2]
        cap = (4 * n) // experts
        kdim = qh * hd
        lanes = 2 * hd
        hslots = tps // 2
        piece = n * hslots
        wq = jnp.transpose(w_query, (1, 2, 0)).reshape(kdim, hid)
        wk = jnp.transpose(w_key, (1, 2, 0)).reshape(hd, hid)
        wv = jnp.transpose(w_value, (1, 2, 0)).reshape(hd, hid)
        ids = jnp.transpose(route_ids, (0, 2, 1))
        gates = jnp.transpose(route_gates, (0, 2, 1))
        dims = (cps, tps, seqs, n, hid, hd, qh, cap)
        owid = lanes * ((qh + 1) // 2)
        vm = pl.BlockSpec(memory_space=pltpu.VMEM)
        anym = pl.BlockSpec(memory_space=pl.ANY)
        dma = pltpu.SemaphoreType.DMA
        scratch = [
            pltpu.VMEM((seqs, tps // 2, 2, n, hid), BF16),
            pltpu.VMEM((lanes * (qh + 1), hid), BF16),
            pltpu.VMEM((seqs, 2 * cps, piece, lanes), BF16),
            pltpu.VMEM((seqs, 2, qh * piece, lanes), BF16),
            pltpu.VMEM((2 * cps, qh * piece, piece), F32),
            pltpu.VMEM((qh * piece, piece // 2), F32),
            pltpu.VMEM((qh * piece, piece // 2), F32),
            pltpu.VMEM((qh * piece, lanes), F32),
            pltpu.VMEM((seqs, tps, n, owid), BF16),
            pltpu.VMEM((seqs, tps, n, owid), BF16),
            pltpu.VMEM((tps // 2, 2, kdim, hid), BF16),
            pltpu.VMEM((seqs, experts * cap, n), BF16),
            pltpu.VMEM((seqs, 2 * n, experts * cap), BF16),
            pltpu.VMEM((seqs, 2, n, 128), F32),
            pltpu.VMEM((seqs, n, hid), BF16),
            pltpu.VMEM((seqs, experts, cap, hid), BF16),
            pltpu.VMEM((seqs, experts, cap, hid), BF16),
            pltpu.VMEM((seqs, experts, cap, hid), BF16),
            pltpu.VMEM((seqs, experts, cap, hid), BF16),
            pltpu.VMEM((hid, ff), BF16),
            pltpu.VMEM((hid, ff), BF16),
            pltpu.VMEM((ff, hid), BF16),
            dma((8 + qh,)),
            dma((seqs, 11)), dma((seqs, 11)),
            dma((2, 6)), dma((2, 6)),
            dma((3, 6)), dma((3, 6)),
            dma((cps + 1,)), dma((cps + 1,)),
            dma((seqs, 2, cps)), dma((seqs, 2, cps)),
            dma((seqs, tps)), dma((seqs, tps)),
            dma((seqs,)), dma((seqs,)),
            dma((seqs,)), dma((seqs,)),
        ]
        return pl.pallas_call(
            functools.partial(layer_kernel, dims),
            out_shape=jax.ShapeDtypeStruct((seqs, n, hid), BF16),
            in_specs=[anym, vm, vm, anym, anym, anym, anym, anym, anym, anym],
            out_specs=vm,
            scratch_shapes=scratch,
            compiler_params=pltpu.CompilerParams(collective_id=0, has_side_effects=True, vmem_limit_bytes=58 * 1024 * 1024),
            name='layer',
        )(act_in, ids, gates, wq, wk, wv, w_out.reshape(kdim, hid), w_gate[0], w_up[0], w_down[0])

    return jax.shard_map(device_step, mesh=mesh, in_specs=(row_spec, row_spec, row_spec, head_spec, head_spec, head_spec, out_spec, expert_spec, expert_spec, expert_spec), out_specs=row_spec, check_vma=False)
```

```python
import functools

import jax
import jax.numpy as jnp
from jax import lax
from jax.experimental import pallas as pl
from jax.experimental.pallas import tpu as pltpu
from jax.sharding import PartitionSpec as P

MESH = pl.DeviceIdType.MESH
scope = jax.named_scope
F32 = jnp.float32
BF16 = jnp.bfloat16
NT = (((1,), (1,)), ((), ()))


def mm(a, b):
    return jnp.dot(a, b, preferred_element_type=F32)


def mm_nt(a, b):
    return lax.dot_general(a, b, NT, preferred_element_type=F32)


def layer_kernel(dims, x_hbm, ids_ref, gates_ref, wq_hbm, wk_hbm, wv_hbm, wo_hbm, wg_hbm, wu_hbm, wd_hbm, y_ref,
                 xf, wqkv, kv, qs, sbuf, mx, lsum, acc, osend, orecv, wof, onehot, onehot_t, gcol, hbuf,
                 dsend, drecv, rsend, rrecv, wg, wu, wd,
                 loc_sem, xs_sem, xr_sem, ws_sem, wr_sem, vs_sem, vr_sem, ss_sem, sr_sem, ks_sem, kr_sem, os_sem, or_sem,
                 ds_sem, dr_sem, rs_sem, rr_sem):
    cps, tps, seqs, n, hid, hd, qh, cap = dims
    experts = cps * tps
    group = experts
    chips = tps // 2
    hslots = tps // 2
    piece = n * hslots
    pieces = 2 * cps
    lanes = 2 * hd
    qrows = qh * piece
    kdim = qh * hd
    c = lax.axis_index('cp')
    t = lax.axis_index('tp')
    me = c * tps + t
    xc = t // 2
    core = t % 2

    unit = hid // (3 * cps)

    def slot(dx, other):
        return (xc + dx) % chips, (core if not other else 1 - core)

    def flat(sl):
        return sl[0] * 2 + sl[1]

    right, left, sib = slot(1, False), slot(chips - 1, False), slot(0, True)
    own, opposite = (xc, core), slot(2, False)

    def rcopy(src, dst, ssem, rsem, cc, tt):
        return pltpu.make_async_remote_copy(src_ref=src, dst_ref=dst, send_sem=ssem, recv_sem=rsem,
                                            device_id={'cp': cc, 'tp': tt}, device_id_type=MESH)

    def load(src, dst, i):
        cp = pltpu.make_async_copy(src, dst, loc_sem.at[i])
        cp.start()
        return cp

    ld_x = [load(x_hbm.at[s], xf.at[s, xc, core], s) for s in range(seqs)]
    ld_wo = load(wo_hbm, wof.at[xc, core], 2)
    ld_qkv = [load(wv_hbm, wqkv.at[pl.ds(0, hd)], 3), load(wk_hbm, wqkv.at[pl.ds(hd, hd)], 4)]
    for i in range(qh):
        ld_qkv.append(load(wq_hbm.at[pl.ds(i * hd, hd)], wqkv.at[pl.ds(lanes * (i + 1) + hd, hd)], 5 + i))
    ld_exp = [load(wg_hbm, wg, 5 + qh), load(wu_hbm, wu, 6 + qh), load(wd_hbm, wd, 7 + qh)]

    barrier = pltpu.get_barrier_semaphore()

    def sig(i, _):
        g = (me + i) % group
        pl.semaphore_signal(barrier, inc=1, device_id={'cp': g // tps, 'tp': g % tps}, device_id_type=MESH)
        return 0

    lax.fori_loop(1, group, sig, 0)
    pl.semaphore_wait(barrier, group - 1)

    def gather(get, ss, rs):
        l2, r2, o2 = slot(chips - 1, True), slot(1, True), slot(2, True)
        sends = [
            (own, 'lo', right), (own, 'hi', right), (own, 'hi', left), (own, 'lo', left),
            (left, 'lo', right), (right, 'hi', left),
            (own, 'all', sib), (left, 'all', sib), (right, 'all', sib), (opposite, 'lo', sib), (opposite, 'hi', sib),
        ]
        gets = [
            (left, 'lo'), (left, 'hi'), (right, 'hi'), (right, 'lo'),
            (opposite, 'lo'), (opposite, 'hi'),
            (sib, 'all'), (l2, 'all'), (r2, 'all'), (o2, 'lo'), (o2, 'hi'),
        ]

        def copy(sl, part, kind, dst):
            return rcopy(get(sl, part), get(sl, part), ss.at[kind], rs.at[kind], c, flat(dst))

        def start(*kinds):
            for k in kinds:
                copy(*sends[k][:2], k, sends[k][2]).start()

        def got(*kinds):
            for k in kinds:
                copy(*gets[k], k, sib).wait_recv()

        def sent(*kinds):
            for k in kinds:
                copy(*sends[k][:2], k, sends[k][2]).wait_send()

        return start, got, sent

    def rows_of(rows):
        return {'lo': pl.ds(0, rows // 2), 'hi': pl.ds(rows // 2, rows // 2), 'all': pl.ds(0, rows)}

    xparts, wparts = rows_of(n), rows_of(kdim)
    xg = [gather(lambda sl, part, s=s: xf.at[s, sl[0], sl[1], xparts[part]], xs_sem.at[s], xr_sem.at[s]) for s in range(seqs)]

    cols_a = pl.ds(0, hid - cps * unit)

    def cols_b(r):
        return pl.ds(pl.multiple_of(hid - cps * unit + r * unit, unit), unit)

    wa = gather(lambda sl, part: wof.at[sl[0], sl[1], wparts[part], cols_a], ws_sem.at[0], wr_sem.at[0])
    wb = gather(lambda sl, part: wof.at[sl[0], sl[1], wparts[part], cols_b(c)], ws_sem.at[1], wr_sem.at[1])

    remote = (left, right, opposite)

    def spread(q, r, src):
        sl = remote[q]
        ref = wof.at[sl[0], sl[1], :, cols_b(src)]
        return rcopy(ref, ref, vs_sem.at[q, r], vr_sem.at[q, src], r, t)

    def share(k, mine):
        cr = core if mine else 1 - core
        if k == 0:
            ref = wof.at[xc, cr]
        elif k < 5:
            q, part = ((0, 'all'), (1, 'all'), (2, 'lo'), (2, 'hi'))[k - 1]
            ref = wof.at[remote[q][0], cr, wparts[part], cols_a]
        else:
            q, i = (k - 5) % 3, (k - 5) // 3
            ref = wof.at[remote[q][0], cr, :, cols_b((c + i) % cps)]
        return rcopy(ref, ref, ss_sem.at[k], sr_sem.at[k], c, flat(sib))

    shares = 5 + 3 * cps

    ld_x[0].wait()
    xg[0][0](0, 2, 1, 3, 6)
    ld_x[1].wait()
    xg[1][0](0, 2)

    ecol = lax.broadcasted_iota(jnp.int32, (experts, n), 0)
    later = (lax.broadcasted_iota(jnp.int32, (n, n), 0) < lax.broadcasted_iota(jnp.int32, (n, n), 1)).astype(F32).astype(BF16)
    srow = lax.broadcasted_iota(jnp.int32, (experts * cap, n), 0)
    eye = lax.broadcasted_iota(jnp.int32, (n, n), 0) == lax.broadcasted_iota(jnp.int32, (n, n), 1)
    for s in range(seqs):
        first = jnp.zeros((experts, 1), F32)
        both = None
        for k in range(2):
            idk = ids_ref[s, k:k + 1, :]
            hits = (ecol == idk).astype(F32)
            before = mm(hits.astype(BF16), later) + first
            rank = jnp.sum(hits * before, axis=0, keepdims=True).astype(jnp.int32)
            first = first + jnp.sum(hits, axis=1, keepdims=True)
            dest = idk * cap + rank
            pick = (srow == dest).astype(F32)
            both = pick if both is None else both + pick
            onehot_t[s, k * n:(k + 1) * n, :] = pick.T.astype(BF16)
            gcol[s, k] = jnp.broadcast_to(jnp.sum(jnp.where(eye, gates_ref[s, k:k + 1, :], 0.0), axis=1, keepdims=True), (n, 128))
        onehot[s] = both.astype(BF16)
    for i in range(qh):
        wqkv[lanes * (i + 1):lanes * (i + 1) + hd, :] = jnp.zeros((hd, hid), BF16)

    def kv_piece(half):
        return c if half == 0 else pieces - 1 - c

    def kv_copy(s, half, r, src):
        ref = kv.at[s, src if half == 0 else pieces - 1 - src]
        return rcopy(ref, ref, ks_sem.at[s, half, r], kr_sem.at[s, half, src], r, t)

    def project(s):
        for half in range(2):
            rows = xf[s, half * (chips // 2):(half + 1) * (chips // 2)].reshape(piece, hid)
            out = mm_nt(rows, wqkv[...])
            kv[s, kv_piece(half)] = out[:, :lanes].astype(BF16)
            for i in range(qh):
                qs[s, half, i * piece:(i + 1) * piece, :] = out[:, lanes * (i + 1):lanes * (i + 2)].astype(BF16)
            for i in range(1, cps):
                r = (c + i) % cps
                if half == 0:
                    kv_copy(s, half, r, c).start()
                else:
                    @pl.when(r < c)
                    def _():
                        kv_copy(s, half, r, c).start()

    with scope('xrelay0'):
        start, got, _ = xg[0]
        got(0)
        start(4)
        got(2)
        start(5)
        xg[1][0](1, 3, 6)
        got(1)
        start(7)
        got(3)
        start(8)
    with scope('xrelay1'):
        xg[1][1](0)
        xg[1][0](4)
        xg[1][1](2)
        xg[1][0](5)
    with scope('xfinish0'):
        start, got, _ = xg[0]
        got(4)
        start(9)
        got(5)
        start(10)
        for cp in ld_qkv:
            cp.wait()
        ld_wo.wait()
        wb[0](0, 2, 1, 3)
        wa[0](0, 2, 1, 3)
        share(0, True).start()
        got(6, 7, 8, 9, 10)
    with scope('qkv0'):
        project(0)
    with scope('xfinish1'):
        start, got, _ = xg[1]
        got(1)
        start(7)
        got(3)
        start(8)
        got(4)
        start(9)
        got(5)
        start(10)
        got(6, 7, 8, 9, 10)
    with scope('qkv1'):
        project(1)

    scale = hd ** -0.5
    causal = lax.broadcasted_iota(jnp.int32, (piece, piece), 1) <= lax.broadcasted_iota(jnp.int32, (piece, piece), 0)
    lane_lo = lax.broadcasted_iota(jnp.int32, (n, lanes), 1) < hd
    mid = piece // 2

    def attend(s, half):
        blocks = c + 1 if half == 0 else pieces - c
        for i in range(qh):
            rs = slice(i * piece, (i + 1) * piece)
            mx[rs] = jnp.full((piece, mid), -jnp.inf, F32)

        def scores(j, diag):
            for i in range(qh):
                rs = slice(i * piece, (i + 1) * piece)
                sc = mm_nt(qs[s, half, rs, :], kv[s, j])
                if diag:
                    sc = jnp.where(causal, sc, -jnp.inf)
                sbuf[j, rs, :] = sc
                mx[rs] = jnp.maximum(mx[rs], jnp.maximum(sc[:, :mid], sc[:, mid:]))

        def one(j, _):
            scores(j, False)
            return 0

        lax.fori_loop(0, blocks - 1, one, 0)
        scores(blocks - 1, True)
        for i in range(qh):
            rs = slice(i * piece, (i + 1) * piece)
            mx[rs] = jnp.broadcast_to(jnp.max(mx[rs], axis=1, keepdims=True), (piece, mid))
            lsum[rs] = jnp.zeros((piece, mid), F32)
            acc[rs] = jnp.zeros((piece, lanes), F32)

        def two(j, _):
            for i in range(qh):
                rs = slice(i * piece, (i + 1) * piece)
                top = mx[rs]
                pa = jnp.exp((sbuf[j, rs, :mid] - top) * scale)
                pb = jnp.exp((sbuf[j, rs, mid:] - top) * scale)
                lsum[rs] += pa + pb
                acc[rs] += mm(jnp.concatenate([pa, pb], axis=1).astype(BF16), kv[s, j])
            return 0

        lax.fori_loop(0, blocks, two, 0)
        for u in range(hslots):
            heads = []
            for i in range(qh):
                rs = slice(i * piece + u * n, i * piece + (u + 1) * n)
                heads.append(acc[rs] / jnp.sum(lsum[rs], axis=1, keepdims=True))
            for b in range(0, qh, 2):
                if b + 1 < qh:
                    both = jnp.where(lane_lo, heads[b], pltpu.roll(heads[b + 1], hd, 1))
                else:
                    both = jnp.where(lane_lo, heads[b], 0.0)
                osend[s, half * hslots + u, :, b * hd:b * hd + lanes] = both.astype(BF16)
        for u in range(hslots):
            dst = half * hslots + u

            @pl.when(dst != t)
            def _():
                rcopy(osend.at[s, dst], orecv.at[s, t], os_sem.at[s, dst], or_sem.at[s, t], c, dst).start()

            @pl.when(dst == t)
            def _():
                orecv[s, t] = osend[s, dst]

    def kv_wait(s, half):
        for i in range(1, cps):
            r = (c + i) % cps
            if half == 0:
                @pl.when(r < c)
                def _():
                    kv_copy(s, 0, c, r).wait_recv()
            else:
                @pl.when(r > c)
                def _():
                    kv_copy(s, 0, c, r).wait_recv()
                    kv_copy(s, 1, c, r).wait_recv()

    def exchange(src, dst, ss, rs):
        def go(i, _):
            g = (me + i) % group
            rcopy(src.at[g], dst.at[me], ss, rs, g // tps, g % tps).start()
            return 0

        lax.fori_loop(1, group, go, 0)
        dst[me] = src[me]

    def arrived(dst, rs):
        part = dst.at[pl.ds(0, group - 1)]
        rcopy(part, part, rs, rs, c, t).wait_recv()

    def left_all(src, ss):
        part = src.at[pl.ds(0, group - 1)]
        rcopy(part, part, ss, ss, c, t).wait_send()

    def out_rows(s):
        for i in range(1, tps):
            src = (t + i) % tps
            rcopy(orecv.at[s, src], orecv.at[s, src], os_sem.at[s, src], or_sem.at[s, src], c, src).wait_recv()
        total = xf[s, xc, core].astype(F32)
        added = None
        for u in range(tps):
            term = mm(orecv[s, u][:, :kdim], wof[u // 2, u % 2])
            added = term if added is None else added + term
        mid_rows = (total + added).astype(BF16)
        hbuf[s] = mid_rows
        dsend[s] = mm(onehot[s], mid_rows).reshape(group, cap, hid).astype(BF16)
        exchange(dsend.at[s], drecv.at[s], ds_sem.at[s], dr_sem.at[s])

    with scope('wb1'):
        wb[1](0)
        wb[0](4)
        wb[1](2)
        wb[0](5)
        wb[1](1, 3)
        for q in range(2):
            for i in range(1, cps):
                spread(q, (c + i) % cps, c).start()
    with scope('kvwait00'):
        kv_wait(0, 0)
    with scope('attend00'):
        attend(0, 0)
    with scope('wb2'):
        wb[1](4, 5)
        for i in range(1, cps):
            spread(2, (c + i) % cps, c).start()
        for k in (5, 6, 7):
            share(k, True).start()
        wa[1](0)
        wa[0](4)
        wa[1](2)
        wa[0](5)
    with scope('kvwait01'):
        kv_wait(0, 1)
    with scope('attend01'):
        attend(0, 1)
    with scope('wa2'):
        wa[1](1, 3)
        share(1, True).start()
        share(2, True).start()
    with scope('kvwait10'):
        kv_wait(1, 0)
    with scope('attend10'):
        attend(1, 0)
    with scope('kvwait11'):
        kv_wait(1, 1)
    with scope('attend11'):
        attend(1, 1)
    with scope('wa3'):
        wa[1](4)
        share(3, True).start()
        wa[1](5)
        share(4, True).start()
    with scope('wy'):
        for q in range(3):
            for i in range(1, cps):
                spread(q, (c + i) % cps, (c + i) % cps).wait_recv()
                share(5 + 3 * i + q, True).start()
    with scope('wshare'):
        for k in range(shares):
            share(k, False).wait_recv()
    with scope('out0'):
        out_rows(0)
    with scope('out1'):
        out_rows(1)

    for cp in ld_exp:
        cp.wait()
    for s in range(seqs):
        with scope(f'dwait{s}'):
            arrived(drecv.at[s], dr_sem.at[s])
        rows = drecv[s].astype(F32).reshape(group * cap, hid).astype(BF16)
        act = (jax.nn.silu(mm(rows, wg[...])) * mm(rows, wu[...])).astype(BF16)
        rsend[s] = mm(act, wd[...]).reshape(group, cap, hid).astype(BF16)
        exchange(rsend.at[s], rrecv.at[s], rs_sem.at[s], rr_sem.at[s])

    for s in range(seqs):
        with scope(f'rwait{s}'):
            arrived(rrecv.at[s], rr_sem.at[s])
        z = mm(onehot_t[s], rrecv[s].astype(F32).reshape(group * cap, hid).astype(BF16))
        g0 = gcol[s, 0][:, :1]
        g1 = gcol[s, 1][:, :1]
        y_ref[s] = (hbuf[s].astype(F32) + (g0 * z[:n] + g1 * z[n:])).astype(BF16)

    for s in range(seqs):
        xg[s][2](*range(11))
        for half in range(2):
            for i in range(1, cps):
                r = (c + i) % cps
                if half == 0:
                    kv_copy(s, half, r, c).wait_send()
                else:
                    @pl.when(r < c)
                    def _():
                        kv_copy(s, half, r, c).wait_send()
        for i in range(1, tps):
            dst = (t + i) % tps
            rcopy(osend.at[s, dst], orecv.at[s, t], os_sem.at[s, dst], or_sem.at[s, t], c, dst).wait_send()
        left_all(dsend.at[s], ds_sem.at[s])
        left_all(rsend.at[s], rs_sem.at[s])
    for part in (wa, wb):
        part[2](*range(6))
    for q in range(3):
        for i in range(1, cps):
            spread(q, (c + i) % cps, c).wait_send()
    for k in range(shares):
        share(k, True).wait_send()


def solution(mesh):
    cps = mesh.shape['cp']
    tps = mesh.shape['tp']
    experts = cps * tps
    row_spec = P(None, ('data', 'cp', 'tp'), None)
    head_spec = P(None, 'tp', None)
    out_spec = P('tp', None, None)
    expert_spec = P(('cp', 'tp'), None, None)

    def device_step(act_in, route_ids, route_gates, w_query, w_key, w_value, w_out, w_gate, w_up, w_down):
        seqs, n, hid = act_in.shape
        qh, hd = w_query.shape[1], w_query.shape[2]
        ff = w_gate.shape[2]
        cap = (4 * n) // experts
        kdim = qh * hd
        lanes = 2 * hd
        hslots = tps // 2
        piece = n * hslots
        wq = jnp.transpose(w_query, (1, 2, 0)).reshape(kdim, hid)
        wk = jnp.transpose(w_key, (1, 2, 0)).reshape(hd, hid)
        wv = jnp.transpose(w_value, (1, 2, 0)).reshape(hd, hid)
        ids = jnp.transpose(route_ids, (0, 2, 1))
        gates = jnp.transpose(route_gates, (0, 2, 1))
        dims = (cps, tps, seqs, n, hid, hd, qh, cap)
        owid = lanes * ((qh + 1) // 2)
        vm = pl.BlockSpec(memory_space=pltpu.VMEM)
        anym = pl.BlockSpec(memory_space=pl.ANY)
        dma = pltpu.SemaphoreType.DMA
        scratch = [
            pltpu.VMEM((seqs, tps // 2, 2, n, hid), BF16),
            pltpu.VMEM((lanes * (qh + 1), hid), BF16),
            pltpu.VMEM((seqs, 2 * cps, piece, lanes), BF16),
            pltpu.VMEM((seqs, 2, qh * piece, lanes), BF16),
            pltpu.VMEM((2 * cps, qh * piece, piece), F32),
            pltpu.VMEM((qh * piece, piece // 2), F32),
            pltpu.VMEM((qh * piece, piece // 2), F32),
            pltpu.VMEM((qh * piece, lanes), F32),
            pltpu.VMEM((seqs, tps, n, owid), BF16),
            pltpu.VMEM((seqs, tps, n, owid), BF16),
            pltpu.VMEM((tps // 2, 2, kdim, hid), BF16),
            pltpu.VMEM((seqs, experts * cap, n), BF16),
            pltpu.VMEM((seqs, 2 * n, experts * cap), BF16),
            pltpu.VMEM((seqs, 2, n, 128), F32),
            pltpu.VMEM((seqs, n, hid), BF16),
            pltpu.VMEM((seqs, experts, cap, hid), BF16),
            pltpu.VMEM((seqs, experts, cap, hid), BF16),
            pltpu.VMEM((seqs, experts, cap, hid), BF16),
            pltpu.VMEM((seqs, experts, cap, hid), BF16),
            pltpu.VMEM((hid, ff), BF16),
            pltpu.VMEM((hid, ff), BF16),
            pltpu.VMEM((ff, hid), BF16),
            dma((8 + qh,)),
            dma((seqs, 11)), dma((seqs, 11)),
            dma((2, 6)), dma((2, 6)),
            dma((3, cps)), dma((3, cps)),
            dma((5 + 3 * cps,)), dma((5 + 3 * cps,)),
            dma((seqs, 2, cps)), dma((seqs, 2, cps)),
            dma((seqs, tps)), dma((seqs, tps)),
            dma((seqs,)), dma((seqs,)),
            dma((seqs,)), dma((seqs,)),
        ]
        return pl.pallas_call(
            functools.partial(layer_kernel, dims),
            out_shape=jax.ShapeDtypeStruct((seqs, n, hid), BF16),
            in_specs=[anym, vm, vm, anym, anym, anym, anym, anym, anym, anym],
            out_specs=vm,
            scratch_shapes=scratch,
            compiler_params=pltpu.CompilerParams(collective_id=0, has_side_effects=True, vmem_limit_bytes=58 * 1024 * 1024),
            name='layer',
        )(act_in, ids, gates, wq, wk, wv, w_out.reshape(kdim, hid), w_gate[0], w_up[0], w_down[0])

    return jax.shard_map(device_step, mesh=mesh, in_specs=(row_spec, row_spec, row_spec, head_spec, head_spec, head_spec, out_spec, expert_spec, expert_spec, expert_spec), out_specs=row_spec, check_vma=False)
```

```python
import functools

import jax
import jax.numpy as jnp
from jax import lax
from jax.experimental import pallas as pl
from jax.experimental.pallas import tpu as pltpu
from jax.sharding import PartitionSpec as P

MESH = pl.DeviceIdType.MESH
scope = jax.named_scope
F32 = jnp.float32
BF16 = jnp.bfloat16
NT = (((1,), (1,)), ((), ()))


def mm(a, b):
    return jnp.dot(a, b, preferred_element_type=F32)


def mm_nt(a, b):
    return lax.dot_general(a, b, NT, preferred_element_type=F32)


def layer_kernel(dims, x_hbm, ids_ref, gates_ref, wq_hbm, wk_hbm, wv_hbm, wo_hbm, wg_hbm, wu_hbm, wd_hbm, h_out, w_out,
                 xf, wqkv, kv, qs, sbuf, mx, lsum, acc, osend, orecv, wof, onehot, onehot_t, gcol, hbuf, wbuf,
                 dsend, drecv, rsend, rrecv, wg, wu, wd,
                 loc_sem, xs_sem, xr_sem, ws_sem, wr_sem, vs_sem, vr_sem, ss_sem, sr_sem, ks_sem, kr_sem, os_sem, or_sem,
                 ds_sem, dr_sem, rs_sem, rr_sem):
    cps, tps, seqs, n, hid, hd, qh, cap = dims
    experts = cps * tps
    group = experts
    chips = tps // 2
    hslots = tps // 2
    piece = n * hslots
    pieces = 2 * cps
    lanes = 2 * hd
    qrows = qh * piece
    kdim = qh * hd
    c = lax.axis_index('cp')
    t = lax.axis_index('tp')
    me = c * tps + t
    xc = t // 2
    core = t % 2

    unit = hid // (3 * cps)

    def slot(dx, other):
        return (xc + dx) % chips, (core if not other else 1 - core)

    def flat(sl):
        return sl[0] * 2 + sl[1]

    right, left, sib = slot(1, False), slot(chips - 1, False), slot(0, True)
    own, opposite = (xc, core), slot(2, False)

    def rcopy(src, dst, ssem, rsem, cc, tt):
        return pltpu.make_async_remote_copy(src_ref=src, dst_ref=dst, send_sem=ssem, recv_sem=rsem,
                                            device_id={'cp': cc, 'tp': tt}, device_id_type=MESH)

    def load(src, dst, i):
        cp = pltpu.make_async_copy(src, dst, loc_sem.at[i])
        cp.start()
        return cp

    ld_x = [load(x_hbm.at[s], xf.at[s, xc, core], s) for s in range(seqs)]
    ld_wo = load(wo_hbm, wof.at[xc, core], 2)
    ld_qkv = [load(wv_hbm, wqkv.at[pl.ds(0, hd)], 3), load(wk_hbm, wqkv.at[pl.ds(hd, hd)], 4)]
    for i in range(qh):
        ld_qkv.append(load(wq_hbm.at[pl.ds(i * hd, hd)], wqkv.at[pl.ds(lanes * (i + 1) + hd, hd)], 5 + i))
    ld_exp = [load(wg_hbm, wg, 5 + qh), load(wu_hbm, wu, 6 + qh), load(wd_hbm, wd, 7 + qh)]

    barrier = pltpu.get_barrier_semaphore()

    def sig(i, _):
        g = (me + i) % group
        pl.semaphore_signal(barrier, inc=1, device_id={'cp': g // tps, 'tp': g % tps}, device_id_type=MESH)
        return 0

    lax.fori_loop(1, group, sig, 0)
    pl.semaphore_wait(barrier, group - 1)

    def gather(get, ss, rs):
        l2, r2, o2 = slot(chips - 1, True), slot(1, True), slot(2, True)
        sends = [
            (own, 'lo', right), (own, 'hi', right), (own, 'hi', left), (own, 'lo', left),
            (left, 'lo', right), (right, 'hi', left),
            (own, 'all', sib), (left, 'all', sib), (right, 'all', sib), (opposite, 'lo', sib), (opposite, 'hi', sib),
        ]
        gets = [
            (left, 'lo'), (left, 'hi'), (right, 'hi'), (right, 'lo'),
            (opposite, 'lo'), (opposite, 'hi'),
            (sib, 'all'), (l2, 'all'), (r2, 'all'), (o2, 'lo'), (o2, 'hi'),
        ]

        def copy(sl, part, kind, dst):
            return rcopy(get(sl, part), get(sl, part), ss.at[kind], rs.at[kind], c, flat(dst))

        def start(*kinds):
            for k in kinds:
                copy(*sends[k][:2], k, sends[k][2]).start()

        def got(*kinds):
            for k in kinds:
                copy(*gets[k], k, sib).wait_recv()

        def sent(*kinds):
            for k in kinds:
                copy(*sends[k][:2], k, sends[k][2]).wait_send()

        return start, got, sent

    def rows_of(rows):
        return {'lo': pl.ds(0, rows // 2), 'hi': pl.ds(rows // 2, rows // 2), 'all': pl.ds(0, rows)}

    xparts, wparts = rows_of(n), rows_of(kdim)
    xg = [gather(lambda sl, part, s=s: xf.at[s, sl[0], sl[1], xparts[part]], xs_sem.at[s], xr_sem.at[s]) for s in range(seqs)]

    cols_a = pl.ds(0, hid - cps * unit)

    def cols_b(r):
        return pl.ds(pl.multiple_of(hid - cps * unit + r * unit, unit), unit)

    wa = gather(lambda sl, part: wof.at[sl[0], sl[1], wparts[part], cols_a], ws_sem.at[0], wr_sem.at[0])
    wb = gather(lambda sl, part: wof.at[sl[0], sl[1], wparts[part], cols_b(c)], ws_sem.at[1], wr_sem.at[1])

    remote = (left, right, opposite)

    def spread(q, r, src):
        sl = remote[q]
        ref = wof.at[sl[0], sl[1], :, cols_b(src)]
        return rcopy(ref, ref, vs_sem.at[q, r], vr_sem.at[q, src], r, t)

    def share(k, mine):
        cr = core if mine else 1 - core
        if k == 0:
            ref = wof.at[xc, cr]
        elif k < 5:
            q, part = ((0, 'all'), (1, 'all'), (2, 'lo'), (2, 'hi'))[k - 1]
            ref = wof.at[remote[q][0], cr, wparts[part], cols_a]
        else:
            q, i = (k - 5) % 3, (k - 5) // 3
            ref = wof.at[remote[q][0], cr, :, cols_b((c + i) % cps)]
        return rcopy(ref, ref, ss_sem.at[k], sr_sem.at[k], c, flat(sib))

    shares = 5 + 3 * cps

    ld_x[0].wait()
    xg[0][0](0, 2, 1, 3, 6)
    ld_x[1].wait()
    xg[1][0](0, 2)

    ecol = lax.broadcasted_iota(jnp.int32, (experts, n), 0)
    later = (lax.broadcasted_iota(jnp.int32, (n, n), 0) < lax.broadcasted_iota(jnp.int32, (n, n), 1)).astype(F32).astype(BF16)
    srow = lax.broadcasted_iota(jnp.int32, (experts * cap, n), 0)
    eye = lax.broadcasted_iota(jnp.int32, (n, n), 0) == lax.broadcasted_iota(jnp.int32, (n, n), 1)
    for s in range(seqs):
        first = jnp.zeros((experts, 1), F32)
        both = None
        for k in range(2):
            idk = ids_ref[s, k:k + 1, :]
            hits = (ecol == idk).astype(F32)
            before = mm(hits.astype(BF16), later) + first
            rank = jnp.sum(hits * before, axis=0, keepdims=True).astype(jnp.int32)
            first = first + jnp.sum(hits, axis=1, keepdims=True)
            dest = idk * cap + rank
            pick = (srow == dest).astype(F32)
            both = pick if both is None else both + pick
            onehot_t[s, k * n:(k + 1) * n, :] = pick.T.astype(BF16)
            gcol[s, k] = jnp.broadcast_to(jnp.sum(jnp.where(eye, gates_ref[s, k:k + 1, :], 0.0), axis=1, keepdims=True), (n, 128))
        onehot[s] = both.astype(BF16)
    for i in range(qh):
        wqkv[lanes * (i + 1):lanes * (i + 1) + hd, :] = jnp.zeros((hd, hid), BF16)

    def kv_piece(half):
        return c if half == 0 else pieces - 1 - c

    def kv_copy(s, half, r, src):
        ref = kv.at[s, src if half == 0 else pieces - 1 - src]
        return rcopy(ref, ref, ks_sem.at[s, half, r], kr_sem.at[s, half, src], r, t)

    def project(s):
        for half in range(2):
            rows = xf[s, half * (chips // 2):(half + 1) * (chips // 2)].reshape(piece, hid)
            out = mm_nt(rows, wqkv[...])
            kv[s, kv_piece(half)] = out[:, :lanes].astype(BF16)
            for i in range(qh):
                qs[s, half, i * piece:(i + 1) * piece, :] = out[:, lanes * (i + 1):lanes * (i + 2)].astype(BF16)
            for i in range(1, cps):
                r = (c + i) % cps
                if half == 0:
                    kv_copy(s, half, r, c).start()
                else:
                    @pl.when(r < c)
                    def _():
                        kv_copy(s, half, r, c).start()

    with scope('xrelay0'):
        start, got, _ = xg[0]
        got(0)
        start(4)
        got(2)
        start(5)
        xg[1][0](1, 3, 6)
        got(1)
        start(7)
        got(3)
        start(8)
    with scope('xrelay1'):
        xg[1][1](0)
        xg[1][0](4)
        xg[1][1](2)
        xg[1][0](5)
    with scope('xfinish0'):
        start, got, _ = xg[0]
        got(4)
        start(9)
        got(5)
        start(10)
        for cp in ld_qkv:
            cp.wait()
        ld_wo.wait()
        wb[0](0, 2, 1, 3)
        wa[0](0, 2, 1, 3)
        share(0, True).start()
        got(6, 7, 8, 9, 10)
    with scope('qkv0'):
        project(0)
    with scope('xfinish1'):
        start, got, _ = xg[1]
        got(1)
        start(7)
        got(3)
        start(8)
        got(4)
        start(9)
        got(5)
        start(10)
        got(6, 7, 8, 9, 10)
    with scope('qkv1'):
        project(1)

    scale = hd ** -0.5
    causal = lax.broadcasted_iota(jnp.int32, (piece, piece), 1) <= lax.broadcasted_iota(jnp.int32, (piece, piece), 0)
    lane_lo = lax.broadcasted_iota(jnp.int32, (n, lanes), 1) < hd
    mid = piece // 2

    def attend(s, half):
        blocks = c + 1 if half == 0 else pieces - c
        for i in range(qh):
            rs = slice(i * piece, (i + 1) * piece)
            mx[rs] = jnp.full((piece, mid), -jnp.inf, F32)

        def scores(j, diag):
            for i in range(qh):
                rs = slice(i * piece, (i + 1) * piece)
                sc = mm_nt(qs[s, half, rs, :], kv[s, j])
                if diag:
                    sc = jnp.where(causal, sc, -jnp.inf)
                sbuf[j, rs, :] = sc
                mx[rs] = jnp.maximum(mx[rs], jnp.maximum(sc[:, :mid], sc[:, mid:]))

        def one(j, _):
            scores(j, False)
            return 0

        lax.fori_loop(0, blocks - 1, one, 0)
        scores(blocks - 1, True)
        for i in range(qh):
            rs = slice(i * piece, (i + 1) * piece)
            mx[rs] = jnp.broadcast_to(jnp.max(mx[rs], axis=1, keepdims=True), (piece, mid))
            lsum[rs] = jnp.zeros((piece, mid), F32)
            acc[rs] = jnp.zeros((piece, lanes), F32)

        def two(j, _):
            for i in range(qh):
                rs = slice(i * piece, (i + 1) * piece)
                top = mx[rs]
                pa = jnp.exp((sbuf[j, rs, :mid] - top) * scale)
                pb = jnp.exp((sbuf[j, rs, mid:] - top) * scale)
                lsum[rs] += pa + pb
                acc[rs] += mm(jnp.concatenate([pa, pb], axis=1).astype(BF16), kv[s, j])
            return 0

        lax.fori_loop(0, blocks, two, 0)
        for u in range(hslots):
            heads = []
            for i in range(qh):
                rs = slice(i * piece + u * n, i * piece + (u + 1) * n)
                heads.append(acc[rs] / jnp.sum(lsum[rs], axis=1, keepdims=True))
            for b in range(0, qh, 2):
                if b + 1 < qh:
                    both = jnp.where(lane_lo, heads[b], pltpu.roll(heads[b + 1], hd, 1))
                else:
                    both = jnp.where(lane_lo, heads[b], 0.0)
                osend[s, half * hslots + u, :, b * hd:b * hd + lanes] = both.astype(BF16)
        for u in range(hslots):
            dst = half * hslots + u

            @pl.when(dst != t)
            def _():
                rcopy(osend.at[s, dst], orecv.at[s, t], os_sem.at[s, dst], or_sem.at[s, t], c, dst).start()

            @pl.when(dst == t)
            def _():
                orecv[s, t] = osend[s, dst]

    def kv_wait(s, half):
        for i in range(1, cps):
            r = (c + i) % cps
            if half == 0:
                @pl.when(r < c)
                def _():
                    kv_copy(s, 0, c, r).wait_recv()
            else:
                @pl.when(r > c)
                def _():
                    kv_copy(s, 0, c, r).wait_recv()
                    kv_copy(s, 1, c, r).wait_recv()

    def exchange(src, dst, ss, rs):
        def go(i, _):
            g = (me + i) % group
            rcopy(src.at[g], dst.at[me], ss, rs, g // tps, g % tps).start()
            return 0

        lax.fori_loop(1, group, go, 0)
        dst[me] = src[me]

    def arrived(dst, rs):
        part = dst.at[pl.ds(0, group - 1)]
        rcopy(part, part, rs, rs, c, t).wait_recv()

    def left_all(src, ss):
        part = src.at[pl.ds(0, group - 1)]
        rcopy(part, part, ss, ss, c, t).wait_send()

    def out_rows(s):
        for i in range(1, tps):
            src = (t + i) % tps
            rcopy(orecv.at[s, src], orecv.at[s, src], os_sem.at[s, src], or_sem.at[s, src], c, src).wait_recv()
        total = xf[s, xc, core].astype(F32)
        added = None
        for u in range(tps):
            term = mm(orecv[s, u][:, :kdim], wof[u // 2, u % 2])
            added = term if added is None else added + term
        mid_rows = (total + added).astype(BF16)
        hbuf[s] = mid_rows
        pltpu.make_async_copy(hbuf.at[s], h_out.at[s], loc_sem.at[s]).start()
        dsend[s] = mm(onehot[s], mid_rows).reshape(group, cap, hid).astype(BF16)
        exchange(dsend.at[s], drecv.at[s], ds_sem.at[s], dr_sem.at[s])

    with scope('wb1'):
        wb[1](0)
        wb[0](4)
        wb[1](2)
        wb[0](5)
        wb[1](1, 3)
        for q in range(2):
            for i in range(1, cps):
                spread(q, (c + i) % cps, c).start()
    with scope('kvwait00'):
        kv_wait(0, 0)
    with scope('attend00'):
        attend(0, 0)
    with scope('wb2'):
        wb[1](4, 5)
        for i in range(1, cps):
            spread(2, (c + i) % cps, c).start()
        for k in (5, 6, 7):
            share(k, True).start()
    with scope('kvwait01'):
        kv_wait(0, 1)
    with scope('attend01'):
        attend(0, 1)
    with scope('wa2'):
        wa[1](0)
        wa[0](4)
        wa[1](2)
        wa[0](5)
        wa[1](1, 3)
        share(1, True).start()
        share(2, True).start()
    with scope('kvwait10'):
        kv_wait(1, 0)
    with scope('attend10'):
        attend(1, 0)
    with scope('kvwait11'):
        kv_wait(1, 1)
    with scope('attend11'):
        attend(1, 1)
    with scope('wa3'):
        wa[1](4)
        share(3, True).start()
        wa[1](5)
        share(4, True).start()
    with scope('wy'):
        for q in range(3):
            for i in range(1, cps):
                spread(q, (c + i) % cps, (c + i) % cps).wait_recv()
                share(5 + 3 * i + q, True).start()
    with scope('wshare'):
        for k in range(shares):
            share(k, False).wait_recv()
    with scope('out0'):
        out_rows(0)
    with scope('out1'):
        out_rows(1)

    for cp in ld_exp:
        cp.wait()
    for s in range(seqs):
        with scope(f'dwait{s}'):
            arrived(drecv.at[s], dr_sem.at[s])
        rows = drecv[s].astype(F32).reshape(group * cap, hid).astype(BF16)
        act = (jax.nn.silu(mm(rows, wg[...])) * mm(rows, wu[...])).astype(BF16)
        rsend[s] = mm(act, wd[...]).reshape(group, cap, hid).astype(BF16)
        exchange(rsend.at[s], rrecv.at[s], rs_sem.at[s], rr_sem.at[s])

    for s in range(seqs):
        with scope(f'rwait{s}'):
            arrived(rrecv.at[s], rr_sem.at[s])
        z = mm(onehot_t[s], rrecv[s].astype(F32).reshape(group * cap, hid).astype(BF16))
        g0 = gcol[s, 0][:, :1]
        g1 = gcol[s, 1][:, :1]
        wbuf[s] = g0 * z[:n] + g1 * z[n:]
        pltpu.make_async_copy(wbuf.at[s], w_out.at[s], loc_sem.at[2 + s]).start()

    for s in range(seqs):
        pltpu.make_async_copy(hbuf.at[s], h_out.at[s], loc_sem.at[s]).wait()
        pltpu.make_async_copy(wbuf.at[s], w_out.at[s], loc_sem.at[2 + s]).wait()
        xg[s][2](*range(11))
        for half in range(2):
            for i in range(1, cps):
                r = (c + i) % cps
                if half == 0:
                    kv_copy(s, half, r, c).wait_send()
                else:
                    @pl.when(r < c)
                    def _():
                        kv_copy(s, half, r, c).wait_send()
        for i in range(1, tps):
            dst = (t + i) % tps
            rcopy(osend.at[s, dst], orecv.at[s, t], os_sem.at[s, dst], or_sem.at[s, t], c, dst).wait_send()
        left_all(dsend.at[s], ds_sem.at[s])
        left_all(rsend.at[s], rs_sem.at[s])
    for part in (wa, wb):
        part[2](*range(6))
    for q in range(3):
        for i in range(1, cps):
            spread(q, (c + i) % cps, c).wait_send()
    for k in range(shares):
        share(k, True).wait_send()


def solution(mesh):
    cps = mesh.shape['cp']
    tps = mesh.shape['tp']
    experts = cps * tps
    row_spec = P(None, ('data', 'cp', 'tp'), None)
    head_spec = P(None, 'tp', None)
    out_spec = P('tp', None, None)
    expert_spec = P(('cp', 'tp'), None, None)

    def device_step(act_in, route_ids, route_gates, w_query, w_key, w_value, w_out, w_gate, w_up, w_down):
        seqs, n, hid = act_in.shape
        qh, hd = w_query.shape[1], w_query.shape[2]
        ff = w_gate.shape[2]
        cap = (4 * n) // experts
        kdim = qh * hd
        lanes = 2 * hd
        hslots = tps // 2
        piece = n * hslots
        wq = jnp.transpose(w_query, (1, 2, 0)).reshape(kdim, hid)
        wk = jnp.transpose(w_key, (1, 2, 0)).reshape(hd, hid)
        wv = jnp.transpose(w_value, (1, 2, 0)).reshape(hd, hid)
        ids = jnp.transpose(route_ids, (0, 2, 1))
        gates = jnp.transpose(route_gates, (0, 2, 1))
        dims = (cps, tps, seqs, n, hid, hd, qh, cap)
        owid = lanes * ((qh + 1) // 2)
        vm = pl.BlockSpec(memory_space=pltpu.VMEM)
        anym = pl.BlockSpec(memory_space=pl.ANY)
        dma = pltpu.SemaphoreType.DMA
        scratch = [
            pltpu.VMEM((seqs, tps // 2, 2, n, hid), BF16),
            pltpu.VMEM((lanes * (qh + 1), hid), BF16),
            pltpu.VMEM((seqs, 2 * cps, piece, lanes), BF16),
            pltpu.VMEM((seqs, 2, qh * piece, lanes), BF16),
            pltpu.VMEM((2 * cps, qh * piece, piece), F32),
            pltpu.VMEM((qh * piece, piece // 2), F32),
            pltpu.VMEM((qh * piece, piece // 2), F32),
            pltpu.VMEM((qh * piece, lanes), F32),
            pltpu.VMEM((seqs, tps, n, owid), BF16),
            pltpu.VMEM((seqs, tps, n, owid), BF16),
            pltpu.VMEM((tps // 2, 2, kdim, hid), BF16),
            pltpu.VMEM((seqs, experts * cap, n), BF16),
            pltpu.VMEM((seqs, 2 * n, experts * cap), BF16),
            pltpu.VMEM((seqs, 2, n, 128), F32),
            pltpu.VMEM((seqs, n, hid), BF16),
            pltpu.VMEM((seqs, n, hid), F32),
            pltpu.VMEM((seqs, experts, cap, hid), BF16),
            pltpu.VMEM((seqs, experts, cap, hid), BF16),
            pltpu.VMEM((seqs, experts, cap, hid), BF16),
            pltpu.VMEM((seqs, experts, cap, hid), BF16),
            pltpu.VMEM((hid, ff), BF16),
            pltpu.VMEM((hid, ff), BF16),
            pltpu.VMEM((ff, hid), BF16),
            dma((8 + qh,)),
            dma((seqs, 11)), dma((seqs, 11)),
            dma((2, 6)), dma((2, 6)),
            dma((3, cps)), dma((3, cps)),
            dma((5 + 3 * cps,)), dma((5 + 3 * cps,)),
            dma((seqs, 2, cps)), dma((seqs, 2, cps)),
            dma((seqs, tps)), dma((seqs, tps)),
            dma((seqs,)), dma((seqs,)),
            dma((seqs,)), dma((seqs,)),
        ]
        mid, added = pl.pallas_call(
            functools.partial(layer_kernel, dims),
            out_shape=[jax.ShapeDtypeStruct((seqs, n, hid), BF16), jax.ShapeDtypeStruct((seqs, n, hid), F32)],
            in_specs=[anym, vm, vm, anym, anym, anym, anym, anym, anym, anym],
            out_specs=[anym, anym],
            scratch_shapes=scratch,
            compiler_params=pltpu.CompilerParams(collective_id=0, has_side_effects=True, vmem_limit_bytes=58 * 1024 * 1024),
            name='layer',
        )(act_in, ids, gates, wq, wk, wv, w_out.reshape(kdim, hid), w_gate[0], w_up[0], w_down[0])
        return (mid.astype(F32) + added).astype(BF16)

    return jax.shard_map(device_step, mesh=mesh, in_specs=(row_spec, row_spec, row_spec, head_spec, head_spec, head_spec, out_spec, expert_spec, expert_spec, expert_spec), out_specs=row_spec, check_vma=False)
```

```python
import functools

import jax
import jax.numpy as jnp
from jax import lax
from jax.experimental import pallas as pl
from jax.experimental.pallas import tpu as pltpu
from jax.sharding import PartitionSpec as P

MESH = pl.DeviceIdType.MESH
scope = jax.named_scope
F32 = jnp.float32
BF16 = jnp.bfloat16
NT = (((1,), (1,)), ((), ()))


def mm(a, b):
    return jnp.dot(a, b, preferred_element_type=F32)


def mm_nt(a, b):
    return lax.dot_general(a, b, NT, preferred_element_type=F32)


def layer_kernel(dims, x_hbm, ids_ref, gates_ref, wq_hbm, wk_hbm, wv_hbm, wo_hbm, wg_hbm, wu_hbm, wd_hbm, y_ref,
                 xf, wqkv, kv, qs, sbuf, mx, lsum, acc, osend, orecv, wof, onehot, onehot_t, gcol, hbuf,
                 dsend, drecv, rsend, rrecv, wg, wu, wd,
                 loc_sem, xs_sem, xr_sem, ws_sem, wr_sem, vs_sem, vr_sem, ss_sem, sr_sem, ks_sem, kr_sem, os_sem, or_sem,
                 ds_sem, dr_sem, rs_sem, rr_sem):
    cps, tps, seqs, n, hid, hd, qh, cap = dims
    experts = cps * tps
    group = experts
    chips = tps // 2
    hslots = tps // 2
    piece = n * hslots
    pieces = 2 * cps
    lanes = 2 * hd
    qrows = qh * piece
    kdim = qh * hd
    c = lax.axis_index('cp')
    t = lax.axis_index('tp')
    me = c * tps + t
    xc = t // 2
    core = t % 2

    unit = hid // (3 * cps)

    def slot(dx, other):
        return (xc + dx) % chips, (core if not other else 1 - core)

    def flat(sl):
        return sl[0] * 2 + sl[1]

    right, left, sib = slot(1, False), slot(chips - 1, False), slot(0, True)
    own, opposite = (xc, core), slot(2, False)

    def rcopy(src, dst, ssem, rsem, cc, tt):
        return pltpu.make_async_remote_copy(src_ref=src, dst_ref=dst, send_sem=ssem, recv_sem=rsem,
                                            device_id={'cp': cc, 'tp': tt}, device_id_type=MESH)

    def load(src, dst, i):
        cp = pltpu.make_async_copy(src, dst, loc_sem.at[i])
        cp.start()
        return cp

    ld_x = [load(x_hbm.at[s], xf.at[s, xc, core], s) for s in range(seqs)]
    ld_wo = load(wo_hbm, wof.at[xc, core], 2)
    ld_qkv = [load(wv_hbm, wqkv.at[pl.ds(0, hd)], 3), load(wk_hbm, wqkv.at[pl.ds(hd, hd)], 4)]
    for i in range(qh):
        ld_qkv.append(load(wq_hbm.at[pl.ds(i * hd, hd)], wqkv.at[pl.ds(lanes * (i + 1) + hd, hd)], 5 + i))
    ld_exp = [load(wg_hbm, wg, 5 + qh), load(wu_hbm, wu, 6 + qh), load(wd_hbm, wd, 7 + qh)]

    barrier = pltpu.get_barrier_semaphore()

    def sig(i, _):
        g = (me + i) % group
        pl.semaphore_signal(barrier, inc=1, device_id={'cp': g // tps, 'tp': g % tps}, device_id_type=MESH)
        return 0

    lax.fori_loop(1, group, sig, 0)
    pl.semaphore_wait(barrier, group - 1)

    def gather(get, ss, rs):
        l2, r2, o2 = slot(chips - 1, True), slot(1, True), slot(2, True)
        sends = [
            (own, 'lo', right), (own, 'hi', right), (own, 'hi', left), (own, 'lo', left),
            (left, 'lo', right), (right, 'hi', left),
            (own, 'all', sib), (left, 'all', sib), (right, 'all', sib), (opposite, 'lo', sib), (opposite, 'hi', sib),
        ]
        gets = [
            (left, 'lo'), (left, 'hi'), (right, 'hi'), (right, 'lo'),
            (opposite, 'lo'), (opposite, 'hi'),
            (sib, 'all'), (l2, 'all'), (r2, 'all'), (o2, 'lo'), (o2, 'hi'),
        ]

        def copy(sl, part, kind, dst):
            return rcopy(get(sl, part), get(sl, part), ss.at[kind], rs.at[kind], c, flat(dst))

        def start(*kinds):
            for k in kinds:
                copy(*sends[k][:2], k, sends[k][2]).start()

        def got(*kinds):
            for k in kinds:
                copy(*gets[k], k, sib).wait_recv()

        def sent(*kinds):
            for k in kinds:
                copy(*sends[k][:2], k, sends[k][2]).wait_send()

        return start, got, sent

    def rows_of(rows):
        return {'lo': pl.ds(0, rows // 2), 'hi': pl.ds(rows // 2, rows // 2), 'all': pl.ds(0, rows)}

    xparts, wparts = rows_of(n), rows_of(kdim)
    xg = [gather(lambda sl, part, s=s: xf.at[s, sl[0], sl[1], xparts[part]], xs_sem.at[s], xr_sem.at[s]) for s in range(seqs)]

    cols_a = pl.ds(0, hid - cps * unit)

    def cols_b(r):
        return pl.ds(pl.multiple_of(hid - cps * unit + r * unit, unit), unit)

    wa = gather(lambda sl, part: wof.at[sl[0], sl[1], wparts[part], cols_a], ws_sem.at[0], wr_sem.at[0])

    def wb(q, mine):
        sl = own if mine else (left, right, opposite)[q]
        ref = wof.at[sl[0], sl[1], :, cols_b(c)]
        dst = (right, left, opposite)[q]
        return rcopy(ref, ref, ws_sem.at[1, q], wr_sem.at[1, q], c, flat(dst))


    remote = (left, right, opposite)

    def spread(q, r, src):
        sl = remote[q]
        ref = wof.at[sl[0], sl[1], :, cols_b(src)]
        return rcopy(ref, ref, vs_sem.at[q, r], vr_sem.at[q, src], r, t)

    def share(k, mine):
        cr = core if mine else 1 - core
        if k == 0:
            ref = wof.at[xc, cr]
        elif k < 5:
            q, part = ((0, 'all'), (1, 'all'), (2, 'lo'), (2, 'hi'))[k - 1]
            ref = wof.at[remote[q][0], cr, wparts[part], cols_a]
        else:
            q, i = (k - 5) % 3, (k - 5) // 3
            ref = wof.at[remote[q][0], cr, :, cols_b((c + i) % cps)]
        return rcopy(ref, ref, ss_sem.at[k], sr_sem.at[k], c, flat(sib))

    shares = 5 + 3 * cps

    ld_x[0].wait()
    xg[0][0](0, 2, 1, 3, 6)
    ld_x[1].wait()
    xg[1][0](0, 2)

    ecol = lax.broadcasted_iota(jnp.int32, (experts, n), 0)
    later = (lax.broadcasted_iota(jnp.int32, (n, n), 0) < lax.broadcasted_iota(jnp.int32, (n, n), 1)).astype(F32).astype(BF16)
    srow = lax.broadcasted_iota(jnp.int32, (experts * cap, n), 0)
    eye = lax.broadcasted_iota(jnp.int32, (n, n), 0) == lax.broadcasted_iota(jnp.int32, (n, n), 1)
    for s in range(seqs):
        first = jnp.zeros((experts, 1), F32)
        both = None
        for k in range(2):
            idk = ids_ref[s, k:k + 1, :]
            hits = (ecol == idk).astype(F32)
            before = mm(hits.astype(BF16), later) + first
            rank = jnp.sum(hits * before, axis=0, keepdims=True).astype(jnp.int32)
            first = first + jnp.sum(hits, axis=1, keepdims=True)
            dest = idk * cap + rank
            pick = (srow == dest).astype(F32)
            both = pick if both is None else both + pick
            onehot_t[s, k * n:(k + 1) * n, :] = pick.T.astype(BF16)
            gcol[s, k] = jnp.broadcast_to(jnp.sum(jnp.where(eye, gates_ref[s, k:k + 1, :], 0.0), axis=1, keepdims=True), (n, 128))
        onehot[s] = both.astype(BF16)
    for i in range(qh):
        wqkv[lanes * (i + 1):lanes * (i + 1) + hd, :] = jnp.zeros((hd, hid), BF16)

    def kv_piece(half):
        return c if half == 0 else pieces - 1 - c

    def kv_copy(s, half, r, src):
        ref = kv.at[s, src if half == 0 else pieces - 1 - src]
        return rcopy(ref, ref, ks_sem.at[s, half, r], kr_sem.at[s, half, src], r, t)

    def project(s):
        for half in range(2):
            rows = xf[s, half * (chips // 2):(half + 1) * (chips // 2)].reshape(piece, hid)
            out = mm_nt(rows, wqkv[...])
            kv[s, kv_piece(half)] = out[:, :lanes].astype(BF16)
            for i in range(qh):
                qs[s, half, i * piece:(i + 1) * piece, :] = out[:, lanes * (i + 1):lanes * (i + 2)].astype(BF16)
            for i in range(1, cps):
                r = (c + i) % cps
                if half == 0:
                    kv_copy(s, half, r, c).start()
                else:
                    @pl.when(r < c)
                    def _():
                        kv_copy(s, half, r, c).start()

    with scope('xrelay0'):
        start, got, _ = xg[0]
        got(0)
        start(4)
        got(2)
        start(5)
        xg[1][0](1, 3, 6)
        got(1)
        start(7)
        got(3)
        start(8)
    with scope('xrelay1'):
        xg[1][1](0)
        xg[1][0](4)
        xg[1][1](2)
        xg[1][0](5)
    with scope('xfinish0'):
        start, got, _ = xg[0]
        got(4)
        start(9)
        got(5)
        start(10)
        for cp in ld_qkv:
            cp.wait()
        ld_wo.wait()
        for q in range(3):
            wb(q, True).start()
        wa[0](0, 2, 1, 3)
        share(0, True).start()
        got(6, 7, 8, 9, 10)
    with scope('qkv0'):
        project(0)
    with scope('xfinish1'):
        start, got, _ = xg[1]
        got(1)
        start(7)
        got(3)
        start(8)
        got(4)
        start(9)
        got(5)
        start(10)
        got(6, 7, 8, 9, 10)
    with scope('qkv1'):
        project(1)

    scale = hd ** -0.5
    causal = lax.broadcasted_iota(jnp.int32, (piece, piece), 1) <= lax.broadcasted_iota(jnp.int32, (piece, piece), 0)
    lane_lo = lax.broadcasted_iota(jnp.int32, (n, lanes), 1) < hd
    mid = piece // 2

    def attend(s, half):
        blocks = c + 1 if half == 0 else pieces - c
        for i in range(qh):
            rs = slice(i * piece, (i + 1) * piece)
            mx[rs] = jnp.full((piece, mid), -jnp.inf, F32)

        def scores(j, diag):
            for i in range(qh):
                rs = slice(i * piece, (i + 1) * piece)
                sc = mm_nt(qs[s, half, rs, :], kv[s, j])
                if diag:
                    sc = jnp.where(causal, sc, -jnp.inf)
                sbuf[j, rs, :] = sc
                mx[rs] = jnp.maximum(mx[rs], jnp.maximum(sc[:, :mid], sc[:, mid:]))

        def one(j, _):
            scores(j, False)
            return 0

        lax.fori_loop(0, blocks - 1, one, 0)
        scores(blocks - 1, True)
        for i in range(qh):
            rs = slice(i * piece, (i + 1) * piece)
            mx[rs] = jnp.broadcast_to(jnp.max(mx[rs], axis=1, keepdims=True), (piece, mid))
            lsum[rs] = jnp.zeros((piece, mid), F32)
            acc[rs] = jnp.zeros((piece, lanes), F32)

        def two(j, _):
            for i in range(qh):
                rs = slice(i * piece, (i + 1) * piece)
                top = mx[rs]
                pa = jnp.exp((sbuf[j, rs, :mid] - top) * scale)
                pb = jnp.exp((sbuf[j, rs, mid:] - top) * scale)
                lsum[rs] += pa + pb
                acc[rs] += mm(jnp.concatenate([pa, pb], axis=1).astype(BF16), kv[s, j])
            return 0

        lax.fori_loop(0, blocks, two, 0)
        for u in range(hslots):
            heads = []
            for i in range(qh):
                rs = slice(i * piece + u * n, i * piece + (u + 1) * n)
                heads.append(acc[rs] / jnp.sum(lsum[rs], axis=1, keepdims=True))
            for b in range(0, qh, 2):
                if b + 1 < qh:
                    both = jnp.where(lane_lo, heads[b], pltpu.roll(heads[b + 1], hd, 1))
                else:
                    both = jnp.where(lane_lo, heads[b], 0.0)
                osend[s, half * hslots + u, :, b * hd:b * hd + lanes] = both.astype(BF16)
        for u in range(hslots):
            dst = half * hslots + u

            @pl.when(dst != t)
            def _():
                rcopy(osend.at[s, dst], orecv.at[s, t], os_sem.at[s, dst], or_sem.at[s, t], c, dst).start()

            @pl.when(dst == t)
            def _():
                orecv[s, t] = osend[s, dst]

    def kv_wait(s, half):
        for i in range(1, cps):
            r = (c + i) % cps
            if half == 0:
                @pl.when(r < c)
                def _():
                    kv_copy(s, 0, c, r).wait_recv()
            else:
                @pl.when(r > c)
                def _():
                    kv_copy(s, 0, c, r).wait_recv()
                    kv_copy(s, 1, c, r).wait_recv()

    def exchange(src, dst, ss, rs):
        def go(r, _):
            for a, dx in enumerate((1, chips - 1, 2, 0)):
                cc = (c + r + a) % cps
                for dk in range(2):
                    tt = flat(slot(dx, dk == 1))
                    g = cc * tps + tt

                    def send(g=g, cc=cc, tt=tt):
                        rcopy(src.at[g], dst.at[me], ss, rs, cc, tt).start()

                    if dx == 0 and dk == 0:
                        pl.when(r != (cps - a) % cps)(send)
                    else:
                        send()
            return 0

        lax.fori_loop(0, cps, go, 0)
        dst[me] = src[me]

    def arrived(dst, rs):
        part = dst.at[pl.ds(0, group - 1)]
        rcopy(part, part, rs, rs, c, t).wait_recv()

    def left_all(src, ss):
        part = src.at[pl.ds(0, group - 1)]
        rcopy(part, part, ss, ss, c, t).wait_send()

    def out_rows(s):
        for i in range(1, tps):
            src = (t + i) % tps
            rcopy(orecv.at[s, src], orecv.at[s, src], os_sem.at[s, src], or_sem.at[s, src], c, src).wait_recv()
        total = xf[s, xc, core].astype(F32)
        rows = jnp.concatenate([orecv[s, u][:, :kdim] for u in range(tps)], axis=1)
        added = mm(rows, wof[...].reshape(tps * kdim, hid))
        mid_rows = (total + added).astype(BF16)
        hbuf[s] = mid_rows
        dsend[s] = mm(onehot[s], mid_rows).reshape(group, cap, hid).astype(BF16)
        exchange(dsend.at[s], drecv.at[s], ds_sem.at[s], dr_sem.at[s])

    with scope('wb1'):
        for q in range(3):
            wb(q, False).wait_recv()
            for i in range(1, cps):
                spread(q, (c + i) % cps, c).start()
            share(5 + q, True).start()
    with scope('kvwait00'):
        kv_wait(0, 0)
    with scope('attend00'):
        attend(0, 0)
    with scope('kvwait01'):
        kv_wait(0, 1)
    with scope('attend01'):
        attend(0, 1)
    with scope('wa2'):
        wa[1](0)
        wa[0](4)
        wa[1](2)
        wa[0](5)
        wa[1](1, 3)
        share(1, True).start()
        share(2, True).start()
    with scope('kvwait10'):
        kv_wait(1, 0)
    with scope('attend10'):
        attend(1, 0)
    with scope('kvwait11'):
        kv_wait(1, 1)
    with scope('attend11'):
        attend(1, 1)
    with scope('wa3'):
        wa[1](4)
        share(3, True).start()
        wa[1](5)
        share(4, True).start()
    with scope('wy'):
        for q in range(3):
            for i in range(1, cps):
                spread(q, (c + i) % cps, (c + i) % cps).wait_recv()
                share(5 + 3 * i + q, True).start()
    with scope('wshare'):
        for k in range(shares):
            share(k, False).wait_recv()
    with scope('out0'):
        out_rows(0)
    with scope('out1'):
        out_rows(1)

    for cp in ld_exp:
        cp.wait()
    for s in range(seqs):
        with scope(f'dwait{s}'):
            arrived(drecv.at[s], dr_sem.at[s])
        rows = drecv[s].astype(F32).reshape(group * cap, hid).astype(BF16)
        act = (jax.nn.silu(mm(rows, wg[...])) * mm(rows, wu[...])).astype(BF16)
        rsend[s] = mm(act, wd[...]).reshape(group, cap, hid).astype(BF16)
        exchange(rsend.at[s], rrecv.at[s], rs_sem.at[s], rr_sem.at[s])

    for s in range(seqs):
        with scope(f'rwait{s}'):
            arrived(rrecv.at[s], rr_sem.at[s])
        z = mm(onehot_t[s], rrecv[s].astype(F32).reshape(group * cap, hid).astype(BF16))
        g0 = gcol[s, 0][:, :1]
        g1 = gcol[s, 1][:, :1]
        y_ref[s] = (hbuf[s].astype(F32) + (g0 * z[:n] + g1 * z[n:])).astype(BF16)

    for s in range(seqs):
        xg[s][2](*range(11))
        for half in range(2):
            for i in range(1, cps):
                r = (c + i) % cps
                if half == 0:
                    kv_copy(s, half, r, c).wait_send()
                else:
                    @pl.when(r < c)
                    def _():
                        kv_copy(s, half, r, c).wait_send()
        for i in range(1, tps):
            dst = (t + i) % tps
            rcopy(osend.at[s, dst], orecv.at[s, t], os_sem.at[s, dst], or_sem.at[s, t], c, dst).wait_send()
        left_all(dsend.at[s], ds_sem.at[s])
        left_all(rsend.at[s], rs_sem.at[s])
    wa[2](*range(6))
    for q in range(3):
        wb(q, True).wait_send()
    for q in range(3):
        for i in range(1, cps):
            spread(q, (c + i) % cps, c).wait_send()
    for k in range(shares):
        share(k, True).wait_send()


def solution(mesh):
    cps = mesh.shape['cp']
    tps = mesh.shape['tp']
    experts = cps * tps
    row_spec = P(None, ('data', 'cp', 'tp'), None)
    head_spec = P(None, 'tp', None)
    out_spec = P('tp', None, None)
    expert_spec = P(('cp', 'tp'), None, None)

    def device_step(act_in, route_ids, route_gates, w_query, w_key, w_value, w_out, w_gate, w_up, w_down):
        seqs, n, hid = act_in.shape
        qh, hd = w_query.shape[1], w_query.shape[2]
        ff = w_gate.shape[2]
        cap = (4 * n) // experts
        kdim = qh * hd
        lanes = 2 * hd
        hslots = tps // 2
        piece = n * hslots
        wq = jnp.transpose(w_query, (1, 2, 0)).reshape(kdim, hid)
        wk = jnp.transpose(w_key, (1, 2, 0)).reshape(hd, hid)
        wv = jnp.transpose(w_value, (1, 2, 0)).reshape(hd, hid)
        ids = jnp.transpose(route_ids, (0, 2, 1))
        gates = jnp.transpose(route_gates, (0, 2, 1))
        dims = (cps, tps, seqs, n, hid, hd, qh, cap)
        owid = lanes * ((qh + 1) // 2)
        vm = pl.BlockSpec(memory_space=pltpu.VMEM)
        anym = pl.BlockSpec(memory_space=pl.ANY)
        dma = pltpu.SemaphoreType.DMA
        scratch = [
            pltpu.VMEM((seqs, tps // 2, 2, n, hid), BF16),
            pltpu.VMEM((lanes * (qh + 1), hid), BF16),
            pltpu.VMEM((seqs, 2 * cps, piece, lanes), BF16),
            pltpu.VMEM((seqs, 2, qh * piece, lanes), BF16),
            pltpu.VMEM((2 * cps, qh * piece, piece), F32),
            pltpu.VMEM((qh * piece, piece // 2), F32),
            pltpu.VMEM((qh * piece, piece // 2), F32),
            pltpu.VMEM((qh * piece, lanes), F32),
            pltpu.VMEM((seqs, tps, n, owid), BF16),
            pltpu.VMEM((seqs, tps, n, owid), BF16),
            pltpu.VMEM((tps // 2, 2, kdim, hid), BF16),
            pltpu.VMEM((seqs, experts * cap, n), BF16),
            pltpu.VMEM((seqs, 2 * n, experts * cap), BF16),
            pltpu.VMEM((seqs, 2, n, 128), F32),
            pltpu.VMEM((seqs, n, hid), BF16),
            pltpu.VMEM((seqs, experts, cap, hid), BF16),
            pltpu.VMEM((seqs, experts, cap, hid), BF16),
            pltpu.VMEM((seqs, experts, cap, hid), BF16),
            pltpu.VMEM((seqs, experts, cap, hid), BF16),
            pltpu.VMEM((hid, ff), BF16),
            pltpu.VMEM((hid, ff), BF16),
            pltpu.VMEM((ff, hid), BF16),
            dma((8 + qh,)),
            dma((seqs, 11)), dma((seqs, 11)),
            dma((2, 6)), dma((2, 6)),
            dma((3, cps)), dma((3, cps)),
            dma((5 + 3 * cps,)), dma((5 + 3 * cps,)),
            dma((seqs, 2, cps)), dma((seqs, 2, cps)),
            dma((seqs, tps)), dma((seqs, tps)),
            dma((seqs,)), dma((seqs,)),
            dma((seqs,)), dma((seqs,)),
        ]
        return pl.pallas_call(
            functools.partial(layer_kernel, dims),
            out_shape=jax.ShapeDtypeStruct((seqs, n, hid), BF16),
            in_specs=[anym, vm, vm, anym, anym, anym, anym, anym, anym, anym],
            out_specs=vm,
            scratch_shapes=scratch,
            compiler_params=pltpu.CompilerParams(collective_id=0, has_side_effects=True, vmem_limit_bytes=58 * 1024 * 1024),
            name='layer',
        )(act_in, ids, gates, wq, wk, wv, w_out.reshape(kdim, hid), w_gate[0], w_up[0], w_down[0])

    return jax.shard_map(device_step, mesh=mesh, in_specs=(row_spec, row_spec, row_spec, head_spec, head_spec, head_spec, out_spec, expert_spec, expert_spec, expert_spec), out_specs=row_spec, check_vma=False)
```

```python
import functools
import math

import jax
import jax.numpy as jnp
from jax import lax
from jax.experimental import pallas as pl
from jax.experimental.pallas import tpu as pltpu
from jax.sharding import PartitionSpec as P

MESH = pl.DeviceIdType.MESH
scope = jax.named_scope
F32 = jnp.float32
BF16 = jnp.bfloat16
NT = (((1,), (1,)), ((), ()))


def mm(a, b):
    return jnp.dot(a, b, preferred_element_type=F32)


def mm_nt(a, b):
    return lax.dot_general(a, b, NT, preferred_element_type=F32)


def layer_kernel(dims, x_hbm, ids_ref, gates_ref, wq_hbm, wk_hbm, wv_hbm, wo_hbm, wg_hbm, wu_hbm, wd_hbm, y_ref,
                 xf, wqkv, kv, qs, sbuf, mx, lsum, acc, osend, orecv, wof, onehot, onehot_t, gcol, abuf, hbuf,
                 dsend, drecv, rsend, rrecv, wg, wu, wd,
                 loc_sem, xs_sem, xr_sem, ws_sem, wr_sem, vs_sem, vr_sem, ss_sem, sr_sem, ks_sem, kr_sem, os_sem, or_sem,
                 ds_sem, dr_sem, rs_sem, rr_sem):
    cps, tps, seqs, n, hid, hd, qh, cap = dims
    experts = cps * tps
    group = experts
    chips = tps // 2
    hslots = tps // 2
    piece = n * hslots
    pieces = 2 * cps
    lanes = 2 * hd
    qrows = qh * piece
    kdim = qh * hd
    c = lax.axis_index('cp')
    t = lax.axis_index('tp')
    me = c * tps + t
    xc = t // 2
    core = t % 2

    unit = hid // (3 * cps)

    def slot(dx, other):
        return (xc + dx) % chips, (core if not other else 1 - core)

    def flat(sl):
        return sl[0] * 2 + sl[1]

    right, left, sib = slot(1, False), slot(chips - 1, False), slot(0, True)
    own, opposite = (xc, core), slot(2, False)

    def rcopy(src, dst, ssem, rsem, cc, tt):
        return pltpu.make_async_remote_copy(src_ref=src, dst_ref=dst, send_sem=ssem, recv_sem=rsem,
                                            device_id={'cp': cc, 'tp': tt}, device_id_type=MESH)

    def load(src, dst, i):
        cp = pltpu.make_async_copy(src, dst, loc_sem.at[i])
        cp.start()
        return cp

    ld_x = [load(x_hbm.at[s], xf.at[s, xc, core], s) for s in range(seqs)]
    ld_wo = load(wo_hbm, wof.at[xc, core], 2)
    ld_qkv = [load(wv_hbm, wqkv.at[pl.ds(0, hd)], 3), load(wk_hbm, wqkv.at[pl.ds(hd, hd)], 4)]
    for i in range(qh):
        ld_qkv.append(load(wq_hbm.at[pl.ds(i * hd, hd)], wqkv.at[pl.ds(lanes * (i + 1) + hd, hd)], 5 + i))
    ld_exp = [load(wg_hbm, wg, 5 + qh), load(wu_hbm, wu, 6 + qh), load(wd_hbm, wd, 7 + qh)]

    barrier = pltpu.get_barrier_semaphore()

    def sig(i, _):
        g = (me + i) % group
        pl.semaphore_signal(barrier, inc=1, device_id={'cp': g // tps, 'tp': g % tps}, device_id_type=MESH)
        return 0

    lax.fori_loop(1, group, sig, 0)
    pl.semaphore_wait(barrier, group - 1)

    def gather(get, ss, rs):
        l2, r2, o2 = slot(chips - 1, True), slot(1, True), slot(2, True)
        sends = [
            (own, 'lo', right), (own, 'hi', right), (own, 'hi', left), (own, 'lo', left),
            (left, 'lo', right), (right, 'hi', left),
            (own, 'all', sib), (left, 'all', sib), (right, 'all', sib), (opposite, 'lo', sib), (opposite, 'hi', sib),
        ]
        gets = [
            (left, 'lo'), (left, 'hi'), (right, 'hi'), (right, 'lo'),
            (opposite, 'lo'), (opposite, 'hi'),
            (sib, 'all'), (l2, 'all'), (r2, 'all'), (o2, 'lo'), (o2, 'hi'),
        ]

        def copy(sl, part, kind, dst):
            return rcopy(get(sl, part), get(sl, part), ss.at[kind], rs.at[kind], c, flat(dst))

        def start(*kinds):
            for k in kinds:
                copy(*sends[k][:2], k, sends[k][2]).start()

        def got(*kinds):
            for k in kinds:
                copy(*gets[k], k, sib).wait_recv()

        def sent(*kinds):
            for k in kinds:
                copy(*sends[k][:2], k, sends[k][2]).wait_send()

        return start, got, sent

    def rows_of(rows):
        return {'lo': pl.ds(0, rows // 2), 'hi': pl.ds(rows // 2, rows // 2), 'all': pl.ds(0, rows)}

    xparts, wparts = rows_of(n), rows_of(kdim)
    xg = [gather(lambda sl, part, s=s: xf.at[s, sl[0], sl[1], xparts[part]], xs_sem.at[s], xr_sem.at[s]) for s in range(seqs)]

    cols_a = pl.ds(0, hid - cps * unit)

    def cols_b(r):
        return pl.ds(pl.multiple_of(hid - cps * unit + r * unit, unit), unit)

    wa = gather(lambda sl, part: wof.at[sl[0], sl[1], wparts[part], cols_a], ws_sem.at[0], wr_sem.at[0])

    def wb(q, mine):
        sl = own if mine else (left, right, opposite)[q]
        ref = wof.at[sl[0], sl[1], :, cols_b(c)]
        dst = (right, left, opposite)[q]
        return rcopy(ref, ref, ws_sem.at[1, q], wr_sem.at[1, q], c, flat(dst))


    remote = (left, right, opposite)

    def spread(q, r, src):
        sl = remote[q]
        ref = wof.at[sl[0], sl[1], :, cols_b(src)]
        return rcopy(ref, ref, vs_sem.at[q, r], vr_sem.at[q, src], r, t)

    def share(k, mine):
        cr = core if mine else 1 - core
        if k == 0:
            ref = wof.at[xc, cr]
        elif k < 5:
            q, part = ((0, 'all'), (1, 'all'), (2, 'lo'), (2, 'hi'))[k - 1]
            ref = wof.at[remote[q][0], cr, wparts[part], cols_a]
        else:
            q, i = (k - 5) % 3, (k - 5) // 3
            ref = wof.at[remote[q][0], cr, :, cols_b((c + i) % cps)]
        return rcopy(ref, ref, ss_sem.at[k], sr_sem.at[k], c, flat(sib))

    shares = 5 + 3 * cps

    ld_x[0].wait()
    xg[0][0](0, 2, 1, 3, 6)
    ld_x[1].wait()
    xg[1][0](0, 2)

    ecol = lax.broadcasted_iota(jnp.int32, (experts, n), 0)
    later = (lax.broadcasted_iota(jnp.int32, (n, n), 0) < lax.broadcasted_iota(jnp.int32, (n, n), 1)).astype(F32).astype(BF16)
    srow = lax.broadcasted_iota(jnp.int32, (experts * cap, n), 0)
    eye = lax.broadcasted_iota(jnp.int32, (n, n), 0) == lax.broadcasted_iota(jnp.int32, (n, n), 1)
    for s in range(seqs):
        first = jnp.zeros((experts, 1), F32)
        both = None
        for k in range(2):
            idk = ids_ref[s, k:k + 1, :]
            hits = (ecol == idk).astype(F32)
            before = mm(hits.astype(BF16), later) + first
            rank = jnp.sum(hits * before, axis=0, keepdims=True).astype(jnp.int32)
            first = first + jnp.sum(hits, axis=1, keepdims=True)
            dest = idk * cap + rank
            pick = (srow == dest).astype(F32)
            both = pick if both is None else both + pick
            onehot_t[s, k * n:(k + 1) * n, :] = pick.T.astype(BF16)
            gcol[s, k] = jnp.broadcast_to(jnp.sum(jnp.where(eye, gates_ref[s, k:k + 1, :], 0.0), axis=1, keepdims=True), (n, 128))
        onehot[s] = both.astype(BF16)
    for i in range(qh):
        wqkv[lanes * (i + 1):lanes * (i + 1) + hd, :] = jnp.zeros((hd, hid), BF16)

    def kv_piece(half):
        return c if half == 0 else pieces - 1 - c

    def kv_copy(s, half, r, src):
        ref = kv.at[s, src if half == 0 else pieces - 1 - src]
        return rcopy(ref, ref, ks_sem.at[s, half, r], kr_sem.at[s, half, src], r, t)

    def project(s):
        for half in range(2):
            rows = xf[s, half * (chips // 2):(half + 1) * (chips // 2)].reshape(piece, hid)
            out = mm_nt(rows, wqkv[...])
            kv[s, kv_piece(half)] = out[:, :lanes].astype(BF16)
            for i in range(qh):
                qs[s, half, i * piece:(i + 1) * piece, :] = out[:, lanes * (i + 1):lanes * (i + 2)].astype(BF16)
            for i in range(1, cps):
                r = (c + i) % cps
                if half == 0:
                    kv_copy(s, half, r, c).start()
                else:
                    @pl.when(r < c)
                    def _():
                        kv_copy(s, half, r, c).start()

    with scope('xrelay0'):
        start, got, _ = xg[0]
        got(0)
        start(4)
        got(2)
        start(5)
        xg[1][0](1, 3, 6)
        got(1)
        start(7)
        got(3)
        start(8)
    with scope('xrelay1'):
        xg[1][1](0)
        xg[1][0](4)
        xg[1][1](2)
        xg[1][0](5)
    with scope('xfinish0'):
        start, got, _ = xg[0]
        got(4)
        start(9)
        got(5)
        start(10)
        for cp in ld_qkv:
            cp.wait()
        ld_wo.wait()
        for q in range(3):
            wb(q, True).start()
        wa[0](0, 2, 1, 3)
        share(0, True).start()
        got(6, 7, 8, 9, 10)
    with scope('qkv0'):
        project(0)
    with scope('xfinish1'):
        start, got, _ = xg[1]
        got(1)
        start(7)
        got(3)
        start(8)
        got(4)
        start(9)
        got(5)
        start(10)
        got(6, 7, 8, 9, 10)
    with scope('qkv1'):
        project(1)

    scale = hd ** -0.5 * math.log2(math.e)
    causal = lax.broadcasted_iota(jnp.int32, (piece, piece), 1) <= lax.broadcasted_iota(jnp.int32, (piece, piece), 0)
    lane_lo = lax.broadcasted_iota(jnp.int32, (n, lanes), 1) < hd
    mid = piece // 2

    def attend(s, half):
        blocks = c + 1 if half == 0 else pieces - c
        for i in range(qh):
            rs = slice(i * piece, (i + 1) * piece)
            mx[rs] = jnp.full((piece, mid), -jnp.inf, F32)

        def scores(j, diag):
            for i in range(qh):
                rs = slice(i * piece, (i + 1) * piece)
                sc = mm_nt(qs[s, half, rs, :], kv[s, j])
                if diag:
                    sc = jnp.where(causal, sc, -jnp.inf)
                sbuf[j, rs, :] = sc
                mx[rs] = jnp.maximum(mx[rs], jnp.maximum(sc[:, :mid], sc[:, mid:]))

        def one(j, _):
            scores(j, False)
            return 0

        lax.fori_loop(0, blocks - 1, one, 0)
        scores(blocks - 1, True)
        for i in range(qh):
            rs = slice(i * piece, (i + 1) * piece)
            mx[rs] = jnp.broadcast_to(jnp.max(mx[rs], axis=1, keepdims=True), (piece, mid))
            lsum[rs] = jnp.zeros((piece, mid), F32)
            acc[rs] = jnp.zeros((piece, lanes), F32)

        def two(j, _):
            for i in range(qh):
                rs = slice(i * piece, (i + 1) * piece)
                top = mx[rs]
                pa = jnp.exp2((sbuf[j, rs, :mid] - top) * scale)
                pb = jnp.exp2((sbuf[j, rs, mid:] - top) * scale)
                lsum[rs] += pa + pb
                acc[rs] += mm(jnp.concatenate([pa, pb], axis=1).astype(BF16), kv[s, j])
            return 0

        lax.fori_loop(0, blocks, two, 0)
        for u in range(hslots):
            heads = []
            for i in range(qh):
                rs = slice(i * piece + u * n, i * piece + (u + 1) * n)
                heads.append(acc[rs] / jnp.sum(lsum[rs], axis=1, keepdims=True))
            for b in range(0, qh, 2):
                if b + 1 < qh:
                    both = jnp.where(lane_lo, heads[b], pltpu.roll(heads[b + 1], hd, 1))
                else:
                    both = jnp.where(lane_lo, heads[b], 0.0)
                osend[s, half * hslots + u, :, b * hd:b * hd + lanes] = both.astype(BF16)
        for u in range(hslots):
            dst = half * hslots + u

            @pl.when(dst != t)
            def _():
                rcopy(osend.at[s, dst], orecv.at[s, t], os_sem.at[s, dst], or_sem.at[s, t], c, dst).start()

            @pl.when(dst == t)
            def _():
                orecv[s, t] = osend[s, dst]

    def kv_wait(s, half):
        for i in range(1, cps):
            r = (c + i) % cps
            if half == 0:
                @pl.when(r < c)
                def _():
                    kv_copy(s, 0, c, r).wait_recv()
            else:
                @pl.when(r > c)
                def _():
                    kv_copy(s, 0, c, r).wait_recv()
                    kv_copy(s, 1, c, r).wait_recv()

    def exchange(src, dst, ss, rs):
        def go(r, _):
            for a, dx in enumerate((1, chips - 1, 2, 0)):
                cc = (c + r + a) % cps
                for dk in range(2):
                    tt = flat(slot(dx, dk == 1))
                    g = cc * tps + tt

                    def send(g=g, cc=cc, tt=tt):
                        rcopy(src.at[g], dst.at[me], ss, rs, cc, tt).start()

                    if dx == 0 and dk == 0:
                        pl.when(r != (cps - a) % cps)(send)
                    else:
                        send()
            return 0

        lax.fori_loop(0, cps, go, 0)
        dst[me] = src[me]

    def arrived(dst, rs):
        part = dst.at[pl.ds(0, group - 1)]
        rcopy(part, part, rs, rs, c, t).wait_recv()

    def left_all(src, ss):
        part = src.at[pl.ds(0, group - 1)]
        rcopy(part, part, ss, ss, c, t).wait_send()

    def o_wait(s):
        for i in range(1, tps):
            src = (t + i) % tps
            rcopy(orecv.at[s, src], orecv.at[s, src], os_sem.at[s, src], or_sem.at[s, src], c, src).wait_recv()

    def out_part(s, dxs):
        heads, weights = [], []
        for dx in dxs:
            xq = (xc + dx) % chips
            for cr in range(2):
                heads.append(orecv[s, xq * 2 + cr][:, :kdim])
            weights.append(wof[xq].reshape(2 * kdim, hid))
        return mm(jnp.concatenate(heads, axis=1), jnp.concatenate(weights, axis=0))

    def dispatch(s, added):
        mid_rows = (xf[s, xc, core].astype(F32) + added).astype(BF16)
        hbuf[s] = mid_rows
        dsend[s] = mm(onehot[s], mid_rows).reshape(group, cap, hid).astype(BF16)
        exchange(dsend.at[s], drecv.at[s], ds_sem.at[s], dr_sem.at[s])

    with scope('wb1'):
        for q in range(3):
            wb(q, False).wait_recv()
            for i in range(1, cps):
                spread(q, (c + i) % cps, c).start()
            share(5 + q, True).start()
    with scope('kvwait00'):
        kv_wait(0, 0)
    with scope('attend00'):
        attend(0, 0)
    with scope('kvwait01'):
        kv_wait(0, 1)
    with scope('attend01'):
        attend(0, 1)
    with scope('wa2'):
        wa[1](0)
        wa[0](4)
        wa[1](2)
        wa[0](5)
        wa[1](1, 3)
        share(1, True).start()
        share(2, True).start()
    with scope('kvwait10'):
        kv_wait(1, 0)
    with scope('attend10'):
        attend(1, 0)
    with scope('kvwait11'):
        kv_wait(1, 1)
    with scope('attend11'):
        attend(1, 1)
    with scope('wa3'):
        wa[1](4)
        share(3, True).start()
        wa[1](5)
        share(4, True).start()
    with scope('wy'):
        for q in range(3):
            for i in range(1, cps):
                spread(q, (c + i) % cps, (c + i) % cps).wait_recv()
                share(5 + 3 * i + q, True).start()
    with scope('wshare0'):
        for k in (0, 1, 2) + tuple(5 + 3 * i + q for i in range(cps) for q in range(2)):
            share(k, False).wait_recv()
        o_wait(0)
    with scope('part0'):
        abuf[...] = out_part(0, (0, 1, chips - 1))
    with scope('wshare1'):
        for k in (3, 4) + tuple(5 + 3 * i + 2 for i in range(cps)):
            share(k, False).wait_recv()
    with scope('out0'):
        dispatch(0, abuf[...] + out_part(0, (2,)))
    with scope('owait1'):
        o_wait(1)
    with scope('out1'):
        dispatch(1, mm(jnp.concatenate([orecv[1, u][:, :kdim] for u in range(tps)], axis=1), wof[...].reshape(tps * kdim, hid)))

    for cp in ld_exp:
        cp.wait()
    for s in range(seqs):
        with scope(f'dwait{s}'):
            arrived(drecv.at[s], dr_sem.at[s])
        rows = drecv[s].astype(F32).reshape(group * cap, hid).astype(BF16)
        act = (jax.nn.silu(mm(rows, wg[...])) * mm(rows, wu[...])).astype(BF16)
        rsend[s] = mm(act, wd[...]).reshape(group, cap, hid).astype(BF16)
        exchange(rsend.at[s], rrecv.at[s], rs_sem.at[s], rr_sem.at[s])

    for s in range(seqs):
        with scope(f'rwait{s}'):
            arrived(rrecv.at[s], rr_sem.at[s])
        z = mm(onehot_t[s], rrecv[s].astype(F32).reshape(group * cap, hid).astype(BF16))
        g0 = gcol[s, 0][:, :1]
        g1 = gcol[s, 1][:, :1]
        y_ref[s] = (hbuf[s].astype(F32) + (g0 * z[:n] + g1 * z[n:])).astype(BF16)

    for s in range(seqs):
        xg[s][2](*range(11))
        for half in range(2):
            for i in range(1, cps):
                r = (c + i) % cps
                if half == 0:
                    kv_copy(s, half, r, c).wait_send()
                else:
                    @pl.when(r < c)
                    def _():
                        kv_copy(s, half, r, c).wait_send()
        for i in range(1, tps):
            dst = (t + i) % tps
            rcopy(osend.at[s, dst], orecv.at[s, t], os_sem.at[s, dst], or_sem.at[s, t], c, dst).wait_send()
        left_all(dsend.at[s], ds_sem.at[s])
        left_all(rsend.at[s], rs_sem.at[s])
    wa[2](*range(6))
    for q in range(3):
        wb(q, True).wait_send()
    for q in range(3):
        for i in range(1, cps):
            spread(q, (c + i) % cps, c).wait_send()
    for k in range(shares):
        share(k, True).wait_send()


def solution(mesh):
    cps = mesh.shape['cp']
    tps = mesh.shape['tp']
    experts = cps * tps
    row_spec = P(None, ('data', 'cp', 'tp'), None)
    head_spec = P(None, 'tp', None)
    out_spec = P('tp', None, None)
    expert_spec = P(('cp', 'tp'), None, None)

    def device_step(act_in, route_ids, route_gates, w_query, w_key, w_value, w_out, w_gate, w_up, w_down):
        seqs, n, hid = act_in.shape
        qh, hd = w_query.shape[1], w_query.shape[2]
        ff = w_gate.shape[2]
        cap = (4 * n) // experts
        kdim = qh * hd
        lanes = 2 * hd
        hslots = tps // 2
        piece = n * hslots
        wq = jnp.transpose(w_query, (1, 2, 0)).reshape(kdim, hid)
        wk = jnp.transpose(w_key, (1, 2, 0)).reshape(hd, hid)
        wv = jnp.transpose(w_value, (1, 2, 0)).reshape(hd, hid)
        ids = jnp.transpose(route_ids, (0, 2, 1))
        gates = jnp.transpose(route_gates, (0, 2, 1))
        dims = (cps, tps, seqs, n, hid, hd, qh, cap)
        owid = lanes * ((qh + 1) // 2)
        vm = pl.BlockSpec(memory_space=pltpu.VMEM)
        anym = pl.BlockSpec(memory_space=pl.ANY)
        dma = pltpu.SemaphoreType.DMA
        scratch = [
            pltpu.VMEM((seqs, tps // 2, 2, n, hid), BF16),
            pltpu.VMEM((lanes * (qh + 1), hid), BF16),
            pltpu.VMEM((seqs, 2 * cps, piece, lanes), BF16),
            pltpu.VMEM((seqs, 2, qh * piece, lanes), BF16),
            pltpu.VMEM((2 * cps, qh * piece, piece), F32),
            pltpu.VMEM((qh * piece, piece // 2), F32),
            pltpu.VMEM((qh * piece, piece // 2), F32),
            pltpu.VMEM((qh * piece, lanes), F32),
            pltpu.VMEM((seqs, tps, n, owid), BF16),
            pltpu.VMEM((seqs, tps, n, owid), BF16),
            pltpu.VMEM((tps // 2, 2, kdim, hid), BF16),
            pltpu.VMEM((seqs, experts * cap, n), BF16),
            pltpu.VMEM((seqs, 2 * n, experts * cap), BF16),
            pltpu.VMEM((seqs, 2, n, 128), F32),
            pltpu.VMEM((n, hid), F32),
            pltpu.VMEM((seqs, n, hid), BF16),
            pltpu.VMEM((seqs, experts, cap, hid), BF16),
            pltpu.VMEM((seqs, experts, cap, hid), BF16),
            pltpu.VMEM((seqs, experts, cap, hid), BF16),
            pltpu.VMEM((seqs, experts, cap, hid), BF16),
            pltpu.VMEM((hid, ff), BF16),
            pltpu.VMEM((hid, ff), BF16),
            pltpu.VMEM((ff, hid), BF16),
            dma((8 + qh,)),
            dma((seqs, 11)), dma((seqs, 11)),
            dma((2, 6)), dma((2, 6)),
            dma((3, cps)), dma((3, cps)),
            dma((5 + 3 * cps,)), dma((5 + 3 * cps,)),
            dma((seqs, 2, cps)), dma((seqs, 2, cps)),
            dma((seqs, tps)), dma((seqs, tps)),
            dma((seqs,)), dma((seqs,)),
            dma((seqs,)), dma((seqs,)),
        ]
        return pl.pallas_call(
            functools.partial(layer_kernel, dims),
            out_shape=pltpu.VMEM((seqs, n, hid), BF16),
            in_specs=[anym, vm, vm, anym, anym, anym, anym, anym, anym, anym],
            out_specs=vm,
            scratch_shapes=scratch,
            compiler_params=pltpu.CompilerParams(collective_id=0, has_side_effects=True, vmem_limit_bytes=58 * 1024 * 1024),
            name='layer',
        )(act_in, ids, gates, wq, wk, wv, w_out.reshape(kdim, hid), w_gate[0], w_up[0], w_down[0])

    return jax.shard_map(device_step, mesh=mesh, in_specs=(row_spec, row_spec, row_spec, head_spec, head_spec, head_spec, out_spec, expert_spec, expert_spec, expert_spec), out_specs=row_spec, check_vma=False)
```

```python
import functools
import math

import jax
import jax.numpy as jnp
from jax import lax
from jax.experimental import pallas as pl
from jax.experimental.pallas import tpu as pltpu
from jax.sharding import PartitionSpec as P

MESH = pl.DeviceIdType.MESH
scope = jax.named_scope
F32 = jnp.float32
BF16 = jnp.bfloat16
NT = (((1,), (1,)), ((), ()))


def mm(a, b):
    return jnp.dot(a, b, preferred_element_type=F32)


def mm_nt(a, b):
    return lax.dot_general(a, b, NT, preferred_element_type=F32)


def layer_kernel(dims, x_hbm, ids_ref, gates_ref, wq_hbm, wk_hbm, wv_hbm, wo_hbm, wg_hbm, wu_hbm, wd_hbm, y_ref,
                 xf, wqkv, kv, qs, sbuf, mx, lsum, acc, osend, orecv, wof, onehot, onehot_t, gcol, abuf, hbuf,
                 dsend, drecv, rsend, rrecv, wg, wu, wd,
                 loc_sem, xs_sem, xr_sem, ws_sem, wr_sem, vs_sem, vr_sem, ss_sem, sr_sem, ks_sem, kr_sem, os_sem, or_sem,
                 ds_sem, dr_sem, rs_sem, rr_sem):
    cps, tps, seqs, n, hid, hd, qh, cap = dims
    experts = cps * tps
    group = experts
    chips = tps // 2
    hslots = tps // 2
    piece = n * hslots
    pieces = 2 * cps
    lanes = 2 * hd
    qrows = qh * piece
    kdim = qh * hd
    c = lax.axis_index('cp')
    t = lax.axis_index('tp')
    me = c * tps + t
    xc = t // 2
    core = t % 2

    unit = hid // (3 * cps)

    def slot(dx, other):
        return (xc + dx) % chips, (core if not other else 1 - core)

    def flat(sl):
        return sl[0] * 2 + sl[1]

    right, left, sib = slot(1, False), slot(chips - 1, False), slot(0, True)
    own, opposite = (xc, core), slot(2, False)

    def rcopy(src, dst, ssem, rsem, cc, tt):
        return pltpu.make_async_remote_copy(src_ref=src, dst_ref=dst, send_sem=ssem, recv_sem=rsem,
                                            device_id={'cp': cc, 'tp': tt}, device_id_type=MESH)

    def load(src, dst, i):
        cp = pltpu.make_async_copy(src, dst, loc_sem.at[i])
        cp.start()
        return cp

    ld_x = [load(x_hbm.at[s], xf.at[s, xc, core], s) for s in range(seqs)]
    ld_wo = load(wo_hbm, wof.at[xc, core], 2)
    ld_qkv = [load(wv_hbm, wqkv.at[pl.ds(0, hd)], 3), load(wk_hbm, wqkv.at[pl.ds(hd, hd)], 4)]
    for i in range(qh):
        ld_qkv.append(load(wq_hbm.at[pl.ds(i * hd, hd)], wqkv.at[pl.ds(lanes * (i + 1) + hd, hd)], 5 + i))
    ld_exp = [load(wg_hbm, wg, 5 + qh), load(wu_hbm, wu, 6 + qh), load(wd_hbm, wd, 7 + qh)]

    barrier = pltpu.get_barrier_semaphore()

    def sig(i, _):
        g = (me + i) % group
        pl.semaphore_signal(barrier, inc=1, device_id={'cp': g // tps, 'tp': g % tps}, device_id_type=MESH)
        return 0

    lax.fori_loop(1, group, sig, 0)
    pl.semaphore_wait(barrier, group - 1)

    def gather(get, ss, rs):
        l2, r2, o2 = slot(chips - 1, True), slot(1, True), slot(2, True)
        sends = [
            (own, 'lo', right), (own, 'hi', right), (own, 'hi', left), (own, 'lo', left),
            (left, 'lo', right), (right, 'hi', left),
            (own, 'all', sib), (left, 'all', sib), (right, 'all', sib), (opposite, 'lo', sib), (opposite, 'hi', sib),
        ]
        gets = [
            (left, 'lo'), (left, 'hi'), (right, 'hi'), (right, 'lo'),
            (opposite, 'lo'), (opposite, 'hi'),
            (sib, 'all'), (l2, 'all'), (r2, 'all'), (o2, 'lo'), (o2, 'hi'),
        ]

        def copy(sl, part, kind, dst):
            return rcopy(get(sl, part), get(sl, part), ss.at[kind], rs.at[kind], c, flat(dst))

        def start(*kinds):
            for k in kinds:
                copy(*sends[k][:2], k, sends[k][2]).start()

        def got(*kinds):
            for k in kinds:
                copy(*gets[k], k, sib).wait_recv()

        def sent(*kinds):
            for k in kinds:
                copy(*sends[k][:2], k, sends[k][2]).wait_send()

        return start, got, sent

    def rows_of(rows):
        return {'lo': pl.ds(0, rows // 2), 'hi': pl.ds(rows // 2, rows // 2), 'all': pl.ds(0, rows)}

    xparts, wparts = rows_of(n), rows_of(kdim)
    xg = [gather(lambda sl, part, s=s: xf.at[s, sl[0], sl[1], xparts[part]], xs_sem.at[s], xr_sem.at[s]) for s in range(seqs)]

    cols_a = pl.ds(0, hid - cps * unit)

    def cols_b(r):
        return pl.ds(pl.multiple_of(hid - cps * unit + r * unit, unit), unit)

    wa = gather(lambda sl, part: wof.at[sl[0], sl[1], wparts[part], cols_a], ws_sem.at[0], wr_sem.at[0])

    def wb(q, mine):
        sl = own if mine else (left, right, opposite)[q]
        ref = wof.at[sl[0], sl[1], :, cols_b(c)]
        dst = (right, left, opposite)[q]
        return rcopy(ref, ref, ws_sem.at[1, q], wr_sem.at[1, q], c, flat(dst))


    remote = (left, right, opposite)

    def spread(q, r, src):
        sl = remote[q]
        ref = wof.at[sl[0], sl[1], :, cols_b(src)]
        return rcopy(ref, ref, vs_sem.at[q, r], vr_sem.at[q, src], r, t)

    def share(k, mine):
        cr = core if mine else 1 - core
        if k == 0:
            ref = wof.at[xc, cr]
        elif k < 5:
            q, part = ((0, 'all'), (1, 'all'), (2, 'lo'), (2, 'hi'))[k - 1]
            ref = wof.at[remote[q][0], cr, wparts[part], cols_a]
        else:
            q, i = (k - 5) % 3, (k - 5) // 3
            ref = wof.at[remote[q][0], cr, :, cols_b((c + i) % cps)]
        return rcopy(ref, ref, ss_sem.at[k], sr_sem.at[k], c, flat(sib))

    shares = 5 + 3 * cps

    ld_x[0].wait()
    xg[0][0](0, 2, 1, 3, 6)
    ld_x[1].wait()
    xg[1][0](0, 2)

    ecol = lax.broadcasted_iota(jnp.int32, (experts, n), 0)
    later = (lax.broadcasted_iota(jnp.int32, (n, n), 0) < lax.broadcasted_iota(jnp.int32, (n, n), 1)).astype(F32).astype(BF16)
    srow = lax.broadcasted_iota(jnp.int32, (experts * cap, n), 0)
    eye = lax.broadcasted_iota(jnp.int32, (n, n), 0) == lax.broadcasted_iota(jnp.int32, (n, n), 1)
    for s in range(seqs):
        first = jnp.zeros((experts, 1), F32)
        both = None
        for k in range(2):
            idk = ids_ref[s, k:k + 1, :]
            hits = (ecol == idk).astype(F32)
            before = mm(hits.astype(BF16), later) + first
            rank = jnp.sum(hits * before, axis=0, keepdims=True).astype(jnp.int32)
            first = first + jnp.sum(hits, axis=1, keepdims=True)
            dest = idk * cap + rank
            pick = (srow == dest).astype(F32)
            both = pick if both is None else both + pick
            onehot_t[s, k * n:(k + 1) * n, :] = pick.T.astype(BF16)
            gcol[s, k] = jnp.broadcast_to(jnp.sum(jnp.where(eye, gates_ref[s, k:k + 1, :], 0.0), axis=1, keepdims=True), (n, 128))
        onehot[s] = both.astype(BF16)
    for i in range(qh):
        wqkv[lanes * (i + 1):lanes * (i + 1) + hd, :] = jnp.zeros((hd, hid), BF16)

    def kv_piece(half):
        return c if half == 0 else pieces - 1 - c

    def kv_copy(s, half, r, src):
        ref = kv.at[s, src if half == 0 else pieces - 1 - src]
        return rcopy(ref, ref, ks_sem.at[s, half, r], kr_sem.at[s, half, src], r, t)

    def project(s):
        for half in range(2):
            rows = xf[s, half * (chips // 2):(half + 1) * (chips // 2)].reshape(piece, hid)
            out = mm_nt(rows, wqkv[...])
            kv[s, kv_piece(half)] = out[:, :lanes].astype(BF16)
            for i in range(qh):
                qs[s, half, i * piece:(i + 1) * piece, :] = out[:, lanes * (i + 1):lanes * (i + 2)].astype(BF16)
            for i in range(1, cps):
                r = (c + i) % cps
                if half == 0:
                    kv_copy(s, half, r, c).start()
                else:
                    @pl.when(r < c)
                    def _():
                        kv_copy(s, half, r, c).start()

    with scope('xrelay0'):
        start, got, _ = xg[0]
        got(0)
        start(4)
        got(2)
        start(5)
        xg[1][0](1, 3, 6)
        got(1)
        start(7)
        got(3)
        start(8)
    with scope('xrelay1'):
        xg[1][1](0)
        xg[1][0](4)
        xg[1][1](2)
        xg[1][0](5)
    with scope('xfinish0'):
        start, got, _ = xg[0]
        got(4)
        start(9)
        got(5)
        start(10)
        for cp in ld_qkv:
            cp.wait()
        ld_wo.wait()
        for q in range(3):
            wb(q, True).start()
        wa[0](0, 2, 1, 3)
        share(0, True).start()
        got(6, 7, 8, 9, 10)
    with scope('qkv0'):
        project(0)
    with scope('xfinish1'):
        start, got, _ = xg[1]
        got(1)
        start(7)
        got(3)
        start(8)
        got(4)
        start(9)
        got(5)
        start(10)
        got(6, 7, 8, 9, 10)
    with scope('qkv1'):
        project(1)

    scale = hd ** -0.5 * math.log2(math.e)
    causal = lax.broadcasted_iota(jnp.int32, (piece, piece), 1) <= lax.broadcasted_iota(jnp.int32, (piece, piece), 0)
    lane_lo = lax.broadcasted_iota(jnp.int32, (n, lanes), 1) < hd
    mid = piece // 2

    def attend(s, half):
        blocks = c + 1 if half == 0 else pieces - c
        for i in range(qh):
            rs = slice(i * piece, (i + 1) * piece)
            mx[rs] = jnp.full((piece, mid), -jnp.inf, F32)

        def scores(j, diag):
            for i in range(qh):
                rs = slice(i * piece, (i + 1) * piece)
                sc = mm_nt(qs[s, half, rs, :], kv[s, j])
                if diag:
                    sc = jnp.where(causal, sc, -jnp.inf)
                sbuf[j, rs, :] = sc
                mx[rs] = jnp.maximum(mx[rs], jnp.maximum(sc[:, :mid], sc[:, mid:]))

        def one(j, _):
            scores(j, False)
            return 0

        lax.fori_loop(0, blocks - 1, one, 0)
        scores(blocks - 1, True)
        for i in range(qh):
            rs = slice(i * piece, (i + 1) * piece)
            mx[rs] = jnp.broadcast_to(jnp.max(mx[rs], axis=1, keepdims=True), (piece, mid))
            lsum[rs] = jnp.zeros((piece, mid), F32)
            acc[rs] = jnp.zeros((piece, lanes), F32)

        def two(j, _):
            for i in range(qh):
                rs = slice(i * piece, (i + 1) * piece)
                top = mx[rs]
                pa = jnp.exp2((sbuf[j, rs, :mid] - top) * scale)
                pb = jnp.exp2((sbuf[j, rs, mid:] - top) * scale)
                lsum[rs] += pa + pb
                acc[rs] += mm(jnp.concatenate([pa, pb], axis=1).astype(BF16), kv[s, j])
            return 0

        lax.fori_loop(0, blocks, two, 0)
        for u in range(hslots):
            heads = []
            for i in range(qh):
                rs = slice(i * piece + u * n, i * piece + (u + 1) * n)
                heads.append(acc[rs] / jnp.sum(lsum[rs], axis=1, keepdims=True))
            for b in range(0, qh - 1, 2):
                both = jnp.where(lane_lo, heads[b], pltpu.roll(heads[b + 1], hd, 1))
                osend[s, half * hslots + u, b // 2 * n:(b // 2 + 1) * n, :] = both.astype(BF16)
            last = heads[qh - 1]
            both = jnp.where(lane_lo[:n // 2], last[:n // 2], pltpu.roll(last[n // 2:], hd, 1))
            osend[s, half * hslots + u, qh // 2 * n:, :] = both.astype(BF16)
        for u in range(hslots):
            dst = half * hslots + u

            @pl.when(dst != t)
            def _():
                rcopy(osend.at[s, dst], orecv.at[s, t], os_sem.at[s, dst], or_sem.at[s, t], c, dst).start()

            @pl.when(dst == t)
            def _():
                orecv[s, t] = osend[s, dst]

    def kv_wait(s, half):
        for i in range(1, cps):
            r = (c + i) % cps
            if half == 0:
                @pl.when(r < c)
                def _():
                    kv_copy(s, 0, c, r).wait_recv()
            else:
                @pl.when(r > c)
                def _():
                    kv_copy(s, 0, c, r).wait_recv()
                    kv_copy(s, 1, c, r).wait_recv()

    def exchange(src, dst, ss, rs):
        def go(r, _):
            for a, dx in enumerate((1, chips - 1, 2, 0)):
                cc = (c + r + a) % cps
                for dk in range(2):
                    tt = flat(slot(dx, dk == 1))
                    g = cc * tps + tt

                    def send(g=g, cc=cc, tt=tt):
                        rcopy(src.at[g], dst.at[me], ss, rs, cc, tt).start()

                    if dx == 0 and dk == 0:
                        pl.when(r != (cps - a) % cps)(send)
                    else:
                        send()
            return 0

        lax.fori_loop(0, cps, go, 0)
        dst[me] = src[me]

    def arrived(dst, rs):
        part = dst.at[pl.ds(0, group - 1)]
        rcopy(part, part, rs, rs, c, t).wait_recv()

    def left_all(src, ss):
        part = src.at[pl.ds(0, group - 1)]
        rcopy(part, part, ss, ss, c, t).wait_send()

    def o_wait(s):
        for i in range(1, tps):
            src = (t + i) % tps
            rcopy(orecv.at[s, src], orecv.at[s, src], os_sem.at[s, src], or_sem.at[s, src], c, src).wait_recv()

    def unpack(s, u):
        full = [orecv[s, u, b * n:(b + 1) * n, :] for b in range(qh // 2)]
        last = orecv[s, u, qh // 2 * n:, :]
        return full + [jnp.concatenate([last[:, :hd], last[:, hd:]], axis=0)]

    def out_part(s, dxs):
        heads, weights = [], []
        for dx in dxs:
            xq = (xc + dx) % chips
            for cr in range(2):
                heads += unpack(s, xq * 2 + cr)
            weights.append(wof[xq].reshape(2 * kdim, hid))
        return mm(jnp.concatenate(heads, axis=1), jnp.concatenate(weights, axis=0))

    def dispatch(s, added):
        mid_rows = (xf[s, xc, core].astype(F32) + added).astype(BF16)
        hbuf[s] = mid_rows
        dsend[s] = mm(onehot[s], mid_rows).reshape(group, cap, hid).astype(BF16)
        exchange(dsend.at[s], drecv.at[s], ds_sem.at[s], dr_sem.at[s])

    with scope('wb1'):
        for q in range(3):
            wb(q, False).wait_recv()
            for i in range(1, cps):
                spread(q, (c + i) % cps, c).start()
            share(5 + q, True).start()
    with scope('kvwait00'):
        kv_wait(0, 0)
    with scope('attend00'):
        attend(0, 0)
    with scope('kvwait01'):
        kv_wait(0, 1)
    with scope('attend01'):
        attend(0, 1)
    with scope('wa2'):
        wa[1](0)
        wa[0](4)
        wa[1](2)
        wa[0](5)
        wa[1](1, 3)
        share(1, True).start()
        share(2, True).start()
    with scope('kvwait10'):
        kv_wait(1, 0)
    with scope('attend10'):
        attend(1, 0)
    with scope('kvwait11'):
        kv_wait(1, 1)
    with scope('attend11'):
        attend(1, 1)
    def y_shares(q):
        for i in range(1, cps):
            spread(q, (c + i) % cps, (c + i) % cps).wait_recv()
            share(5 + 3 * i + q, True).start()

    with scope('wy01'):
        y_shares(0)
        y_shares(1)
    with scope('wa3'):
        wa[1](4)
        share(3, True).start()
        wa[1](5)
        share(4, True).start()
        y_shares(2)
    with scope('wshare0'):
        for k in (0, 1, 2) + tuple(5 + 3 * i + q for i in range(cps) for q in range(2)):
            share(k, False).wait_recv()
        o_wait(0)
    with scope('part0'):
        abuf[...] = out_part(0, (0, 1, chips - 1))
    with scope('wshare1'):
        for k in (3, 4) + tuple(5 + 3 * i + 2 for i in range(cps)):
            share(k, False).wait_recv()
    with scope('out0'):
        dispatch(0, abuf[...] + out_part(0, (2,)))
    with scope('owait1'):
        o_wait(1)
    with scope('out1'):
        dispatch(1, mm(jnp.concatenate(sum([unpack(1, u) for u in range(tps)], []), axis=1), wof[...].reshape(tps * kdim, hid)))

    for cp in ld_exp:
        cp.wait()
    for s in range(seqs):
        with scope(f'dwait{s}'):
            arrived(drecv.at[s], dr_sem.at[s])
        rows = drecv[s].astype(F32).reshape(group * cap, hid).astype(BF16)
        act = (jax.nn.silu(mm(rows, wg[...])) * mm(rows, wu[...])).astype(BF16)
        rsend[s] = mm(act, wd[...]).reshape(group, cap, hid).astype(BF16)
        exchange(rsend.at[s], rrecv.at[s], rs_sem.at[s], rr_sem.at[s])

    for s in range(seqs):
        with scope(f'rwait{s}'):
            arrived(rrecv.at[s], rr_sem.at[s])
        z = mm(onehot_t[s], rrecv[s].astype(F32).reshape(group * cap, hid).astype(BF16))
        g0 = gcol[s, 0][:, :1]
        g1 = gcol[s, 1][:, :1]
        y_ref[s] = (hbuf[s].astype(F32) + (g0 * z[:n] + g1 * z[n:])).astype(BF16)

    for s in range(seqs):
        xg[s][2](*range(11))
        for half in range(2):
            for i in range(1, cps):
                r = (c + i) % cps
                if half == 0:
                    kv_copy(s, half, r, c).wait_send()
                else:
                    @pl.when(r < c)
                    def _():
                        kv_copy(s, half, r, c).wait_send()
        for i in range(1, tps):
            dst = (t + i) % tps
            rcopy(osend.at[s, dst], orecv.at[s, t], os_sem.at[s, dst], or_sem.at[s, t], c, dst).wait_send()
        left_all(dsend.at[s], ds_sem.at[s])
        left_all(rsend.at[s], rs_sem.at[s])
    wa[2](*range(6))
    for q in range(3):
        wb(q, True).wait_send()
    for q in range(3):
        for i in range(1, cps):
            spread(q, (c + i) % cps, c).wait_send()
    for k in range(shares):
        share(k, True).wait_send()


def solution(mesh):
    cps = mesh.shape['cp']
    tps = mesh.shape['tp']
    experts = cps * tps
    row_spec = P(None, ('data', 'cp', 'tp'), None)
    head_spec = P(None, 'tp', None)
    out_spec = P('tp', None, None)
    expert_spec = P(('cp', 'tp'), None, None)

    def device_step(act_in, route_ids, route_gates, w_query, w_key, w_value, w_out, w_gate, w_up, w_down):
        seqs, n, hid = act_in.shape
        qh, hd = w_query.shape[1], w_query.shape[2]
        ff = w_gate.shape[2]
        cap = (4 * n) // experts
        kdim = qh * hd
        lanes = 2 * hd
        hslots = tps // 2
        piece = n * hslots
        wq = jnp.transpose(w_query, (1, 2, 0)).reshape(kdim, hid)
        wk = jnp.transpose(w_key, (1, 2, 0)).reshape(hd, hid)
        wv = jnp.transpose(w_value, (1, 2, 0)).reshape(hd, hid)
        ids = jnp.transpose(route_ids, (0, 2, 1))
        gates = jnp.transpose(route_gates, (0, 2, 1))
        dims = (cps, tps, seqs, n, hid, hd, qh, cap)
        orows = n * (qh // 2) + n // 2
        vm = pl.BlockSpec(memory_space=pltpu.VMEM)
        anym = pl.BlockSpec(memory_space=pl.ANY)
        dma = pltpu.SemaphoreType.DMA
        scratch = [
            pltpu.VMEM((seqs, tps // 2, 2, n, hid), BF16),
            pltpu.VMEM((lanes * (qh + 1), hid), BF16),
            pltpu.VMEM((seqs, 2 * cps, piece, lanes), BF16),
            pltpu.VMEM((seqs, 2, qh * piece, lanes), BF16),
            pltpu.VMEM((2 * cps, qh * piece, piece), F32),
            pltpu.VMEM((qh * piece, piece // 2), F32),
            pltpu.VMEM((qh * piece, piece // 2), F32),
            pltpu.VMEM((qh * piece, lanes), F32),
            pltpu.VMEM((seqs, tps, orows, lanes), BF16),
            pltpu.VMEM((seqs, tps, orows, lanes), BF16),
            pltpu.VMEM((tps // 2, 2, kdim, hid), BF16),
            pltpu.VMEM((seqs, experts * cap, n), BF16),
            pltpu.VMEM((seqs, 2 * n, experts * cap), BF16),
            pltpu.VMEM((seqs, 2, n, 128), F32),
            pltpu.VMEM((n, hid), F32),
            pltpu.VMEM((seqs, n, hid), BF16),
            pltpu.VMEM((seqs, experts, cap, hid), BF16),
            pltpu.VMEM((seqs, experts, cap, hid), BF16),
            pltpu.VMEM((seqs, experts, cap, hid), BF16),
            pltpu.VMEM((seqs, experts, cap, hid), BF16),
            pltpu.VMEM((hid, ff), BF16),
            pltpu.VMEM((hid, ff), BF16),
            pltpu.VMEM((ff, hid), BF16),
            dma((8 + qh,)),
            dma((seqs, 11)), dma((seqs, 11)),
            dma((2, 6)), dma((2, 6)),
            dma((3, cps)), dma((3, cps)),
            dma((5 + 3 * cps,)), dma((5 + 3 * cps,)),
            dma((seqs, 2, cps)), dma((seqs, 2, cps)),
            dma((seqs, tps)), dma((seqs, tps)),
            dma((seqs,)), dma((seqs,)),
            dma((seqs,)), dma((seqs,)),
        ]
        return pl.pallas_call(
            functools.partial(layer_kernel, dims),
            out_shape=pltpu.VMEM((seqs, n, hid), BF16),
            in_specs=[anym, vm, vm, anym, anym, anym, anym, anym, anym, anym],
            out_specs=vm,
            scratch_shapes=scratch,
            compiler_params=pltpu.CompilerParams(collective_id=0, has_side_effects=True, vmem_limit_bytes=58 * 1024 * 1024),
            name='layer',
        )(act_in, ids, gates, wq, wk, wv, w_out.reshape(kdim, hid), w_gate[0], w_up[0], w_down[0])

    return jax.shard_map(device_step, mesh=mesh, in_specs=(row_spec, row_spec, row_spec, head_spec, head_spec, head_spec, out_spec, expert_spec, expert_spec, expert_spec), out_specs=row_spec, check_vma=False)
```

```python
import functools
import math

import jax
import jax.numpy as jnp
from jax import lax
from jax.experimental import pallas as pl
from jax.experimental.pallas import tpu as pltpu
from jax.sharding import PartitionSpec as P

MESH = pl.DeviceIdType.MESH
scope = jax.named_scope
F32 = jnp.float32
BF16 = jnp.bfloat16
NT = (((1,), (1,)), ((), ()))


def mm(a, b):
    return jnp.dot(a, b, preferred_element_type=F32)


def mm_nt(a, b):
    return lax.dot_general(a, b, NT, preferred_element_type=F32)


def layer_kernel(dims, x_hbm, ids_ref, gates_ref, wq_hbm, wk_hbm, wv_hbm, wo_hbm, wg_hbm, wu_hbm, wd_hbm, y_ref,
                 xf, wqkv, kv, qs, sbuf, mx, lsum, acc, osend, orecv, wof, onehot, onehot_t, gcol, abuf, hbuf,
                 dsend, drecv, rsend, rrecv, wg, wu, wd,
                 loc_sem, xs_sem, xr_sem, ws_sem, wr_sem, vs_sem, vr_sem, ss_sem, sr_sem, ks_sem, kr_sem, os_sem, or_sem,
                 ds_sem, dr_sem, rs_sem, rr_sem):
    cps, tps, seqs, n, hid, hd, qh, cap = dims
    experts = cps * tps
    group = experts
    chips = tps // 2
    hslots = tps // 2
    piece = n * hslots
    pieces = 2 * cps
    lanes = 2 * hd
    qrows = qh * piece
    kdim = qh * hd
    c = lax.axis_index('cp')
    t = lax.axis_index('tp')
    me = c * tps + t
    xc = t // 2
    core = t % 2

    unit = hid // (3 * cps)

    def slot(dx, other):
        return (xc + dx) % chips, (core if not other else 1 - core)

    def flat(sl):
        return sl[0] * 2 + sl[1]

    right, left, sib = slot(1, False), slot(chips - 1, False), slot(0, True)
    own, opposite = (xc, core), slot(2, False)

    def rcopy(src, dst, ssem, rsem, cc, tt):
        return pltpu.make_async_remote_copy(src_ref=src, dst_ref=dst, send_sem=ssem, recv_sem=rsem,
                                            device_id={'cp': cc, 'tp': tt}, device_id_type=MESH)

    def load(src, dst, i):
        cp = pltpu.make_async_copy(src, dst, loc_sem.at[i])
        cp.start()
        return cp

    ld_x = [load(x_hbm.at[s], xf.at[s, xc, core], s) for s in range(seqs)]
    ld_wo = load(wo_hbm, wof.at[xc, core], 2)
    ld_qkv = [load(wv_hbm, wqkv.at[pl.ds(0, hd)], 3), load(wk_hbm, wqkv.at[pl.ds(hd, hd)], 4)]
    for i in range(qh):
        ld_qkv.append(load(wq_hbm.at[pl.ds(i * hd, hd)], wqkv.at[pl.ds(lanes * (i + 1) + hd, hd)], 5 + i))
    ld_exp = [load(wg_hbm, wg, 5 + qh), load(wu_hbm, wu, 6 + qh), load(wd_hbm, wd, 7 + qh)]

    barrier = pltpu.get_barrier_semaphore()

    def sig(i, _):
        g = (me + i) % group
        pl.semaphore_signal(barrier, inc=1, device_id={'cp': g // tps, 'tp': g % tps}, device_id_type=MESH)
        return 0

    lax.fori_loop(1, group, sig, 0)
    pl.semaphore_wait(barrier, group - 1)

    def gather(get, ss, rs):
        l2, r2, o2 = slot(chips - 1, True), slot(1, True), slot(2, True)
        sends = [
            (own, 'lo', right), (own, 'hi', right), (own, 'hi', left), (own, 'lo', left),
            (left, 'lo', right), (right, 'hi', left),
            (own, 'all', sib), (left, 'all', sib), (right, 'all', sib), (opposite, 'lo', sib), (opposite, 'hi', sib),
        ]
        gets = [
            (left, 'lo'), (left, 'hi'), (right, 'hi'), (right, 'lo'),
            (opposite, 'lo'), (opposite, 'hi'),
            (sib, 'all'), (l2, 'all'), (r2, 'all'), (o2, 'lo'), (o2, 'hi'),
        ]

        def copy(sl, part, kind, dst):
            return rcopy(get(sl, part), get(sl, part), ss.at[kind], rs.at[kind], c, flat(dst))

        def start(*kinds):
            for k in kinds:
                copy(*sends[k][:2], k, sends[k][2]).start()

        def got(*kinds):
            for k in kinds:
                copy(*gets[k], k, sib).wait_recv()

        def sent(*kinds):
            for k in kinds:
                copy(*sends[k][:2], k, sends[k][2]).wait_send()

        return start, got, sent

    def rows_of(rows):
        return {'lo': pl.ds(0, rows // 2), 'hi': pl.ds(rows // 2, rows // 2), 'all': pl.ds(0, rows)}

    xparts, wparts = rows_of(n), rows_of(kdim)
    xg = [gather(lambda sl, part, s=s: xf.at[s, sl[0], sl[1], xparts[part]], xs_sem.at[s], xr_sem.at[s]) for s in range(seqs)]

    cols_a = pl.ds(0, hid - cps * unit)

    def cols_b(r):
        return pl.ds(pl.multiple_of(hid - cps * unit + r * unit, unit), unit)

    wa = gather(lambda sl, part: wof.at[sl[0], sl[1], wparts[part], cols_a], ws_sem.at[0], wr_sem.at[0])

    def wb(q, mine):
        sl = own if mine else (left, right, opposite)[q]
        ref = wof.at[sl[0], sl[1], :, cols_b(c)]
        dst = (right, left, opposite)[q]
        return rcopy(ref, ref, ws_sem.at[1, q], wr_sem.at[1, q], c, flat(dst))


    remote = (left, right, opposite)

    def spread(q, r, src):
        sl = remote[q]
        ref = wof.at[sl[0], sl[1], :, cols_b(src)]
        return rcopy(ref, ref, vs_sem.at[q, r], vr_sem.at[q, src], r, t)

    def share(k, mine):
        cr = core if mine else 1 - core
        if k == 0:
            ref = wof.at[xc, cr]
        elif k < 5:
            q, part = ((0, 'all'), (1, 'all'), (2, 'lo'), (2, 'hi'))[k - 1]
            ref = wof.at[remote[q][0], cr, wparts[part], cols_a]
        else:
            q, i = (k - 5) % 3, (k - 5) // 3
            ref = wof.at[remote[q][0], cr, :, cols_b((c + i) % cps)]
        return rcopy(ref, ref, ss_sem.at[k], sr_sem.at[k], c, flat(sib))

    shares = 5 + 3 * cps

    ld_x[0].wait()
    xg[0][0](0, 2, 1, 3, 6)
    ld_x[1].wait()
    xg[1][0](0, 2)

    ecol = lax.broadcasted_iota(jnp.int32, (experts, n), 0)
    later = (lax.broadcasted_iota(jnp.int32, (n, n), 0) < lax.broadcasted_iota(jnp.int32, (n, n), 1)).astype(F32).astype(BF16)
    srow = lax.broadcasted_iota(jnp.int32, (experts * cap, n), 0)
    eye = lax.broadcasted_iota(jnp.int32, (n, n), 0) == lax.broadcasted_iota(jnp.int32, (n, n), 1)
    for s in range(seqs):
        first = jnp.zeros((experts, 1), F32)
        both = None
        for k in range(2):
            idk = ids_ref[s, k:k + 1, :]
            hits = (ecol == idk).astype(F32)
            before = mm(hits.astype(BF16), later) + first
            rank = jnp.sum(hits * before, axis=0, keepdims=True).astype(jnp.int32)
            first = first + jnp.sum(hits, axis=1, keepdims=True)
            dest = idk * cap + rank
            pick = (srow == dest).astype(F32)
            both = pick if both is None else both + pick
            onehot_t[s, k * n:(k + 1) * n, :] = pick.T.astype(BF16)
            gcol[s, k] = jnp.broadcast_to(jnp.sum(jnp.where(eye, gates_ref[s, k:k + 1, :], 0.0), axis=1, keepdims=True), (n, 128))
        onehot[s] = both.astype(BF16)
    for i in range(qh):
        wqkv[lanes * (i + 1):lanes * (i + 1) + hd, :] = jnp.zeros((hd, hid), BF16)

    def kv_piece(half):
        return c if half == 0 else pieces - 1 - c

    def kv_copy(s, half, r, src):
        ref = kv.at[s, src if half == 0 else pieces - 1 - src]
        return rcopy(ref, ref, ks_sem.at[s, half, r], kr_sem.at[s, half, src], r, t)

    def project(s):
        for half in range(2):
            rows = xf[s, half * (chips // 2):(half + 1) * (chips // 2)].reshape(piece, hid)
            out = mm_nt(rows, wqkv[...])
            kv[s, kv_piece(half)] = out[:, :lanes].astype(BF16)
            for i in range(qh):
                qs[s, half, i * piece:(i + 1) * piece, :] = out[:, lanes * (i + 1):lanes * (i + 2)].astype(BF16)
            for i in range(1, cps):
                r = (c + i) % cps
                if half == 0:
                    kv_copy(s, half, r, c).start()
                else:
                    @pl.when(r < c)
                    def _():
                        kv_copy(s, half, r, c).start()

    with scope('xrelay0'):
        start, got, _ = xg[0]
        got(0)
        start(4)
        got(2)
        start(5)
        xg[1][0](1, 3, 6)
        got(1)
        start(7)
        got(3)
        start(8)
    with scope('xrelay1'):
        xg[1][1](0)
        xg[1][0](4)
        xg[1][1](2)
        xg[1][0](5)
    with scope('xfinish0'):
        start, got, _ = xg[0]
        got(4)
        start(9)
        got(5)
        start(10)
        for cp in ld_qkv:
            cp.wait()
        ld_wo.wait()
        for q in range(3):
            wb(q, True).start()
        wa[0](0, 2, 1, 3)
        share(0, True).start()
        got(6, 7, 8, 9, 10)
    with scope('qkv0'):
        project(0)
    with scope('xfinish1'):
        start, got, _ = xg[1]
        got(1)
        start(7)
        got(3)
        start(8)
        got(4)
        start(9)
        got(5)
        start(10)
        got(6, 7, 8, 9, 10)
    with scope('qkv1'):
        project(1)

    scale = hd ** -0.5 * math.log2(math.e)
    causal = lax.broadcasted_iota(jnp.int32, (piece, piece), 1) <= lax.broadcasted_iota(jnp.int32, (piece, piece), 0)
    lane_lo = lax.broadcasted_iota(jnp.int32, (n, lanes), 1) < hd
    mid = piece // 2

    def attend(s, half):
        blocks = c + 1 if half == 0 else pieces - c
        for i in range(qh):
            rs = slice(i * piece, (i + 1) * piece)
            mx[rs] = jnp.full((piece, mid), -jnp.inf, F32)

        def scores(j, diag):
            for i in range(qh):
                rs = slice(i * piece, (i + 1) * piece)
                sc = mm_nt(qs[s, half, rs, :], kv[s, j])
                if diag:
                    sc = jnp.where(causal, sc, -jnp.inf)
                sbuf[j, rs, :] = sc
                mx[rs] = jnp.maximum(mx[rs], jnp.maximum(sc[:, :mid], sc[:, mid:]))

        def one(j, _):
            scores(j, False)
            return 0

        lax.fori_loop(0, blocks - 1, one, 0)
        scores(blocks - 1, True)
        for i in range(qh):
            rs = slice(i * piece, (i + 1) * piece)
            mx[rs] = jnp.broadcast_to(jnp.max(mx[rs], axis=1, keepdims=True), (piece, mid))
            lsum[rs] = jnp.zeros((piece, mid), F32)
            acc[rs] = jnp.zeros((piece, lanes), F32)

        def two(j, _):
            for i in range(qh):
                rs = slice(i * piece, (i + 1) * piece)
                top = mx[rs]
                pa = jnp.exp2((sbuf[j, rs, :mid] - top) * scale)
                pb = jnp.exp2((sbuf[j, rs, mid:] - top) * scale)
                lsum[rs] += pa + pb
                acc[rs] += mm(jnp.concatenate([pa, pb], axis=1).astype(BF16), kv[s, j])
            return 0

        lax.fori_loop(0, blocks, two, 0)
        for u in range(hslots):
            heads = []
            for i in range(qh):
                rs = slice(i * piece + u * n, i * piece + (u + 1) * n)
                heads.append(acc[rs] / jnp.sum(lsum[rs], axis=1, keepdims=True))
            for b in range(0, qh - 1, 2):
                both = jnp.where(lane_lo, heads[b], pltpu.roll(heads[b + 1], hd, 1))
                osend[s, half * hslots + u, b // 2 * n:(b // 2 + 1) * n, :] = both.astype(BF16)
            last = heads[qh - 1]
            both = jnp.where(lane_lo[:n // 2], last[:n // 2], pltpu.roll(last[n // 2:], hd, 1))
            osend[s, half * hslots + u, qh // 2 * n:, :] = both.astype(BF16)
        for u in range(hslots):
            dst = half * hslots + u

            @pl.when(dst != t)
            def _():
                rcopy(osend.at[s, dst], orecv.at[s, t], os_sem.at[s, dst], or_sem.at[s, t], c, dst).start()

            @pl.when(dst == t)
            def _():
                orecv[s, t] = osend[s, dst]

    def kv_wait(s, half):
        for i in range(1, cps):
            r = (c + i) % cps
            if half == 0:
                @pl.when(r < c)
                def _():
                    kv_copy(s, 0, c, r).wait_recv()
            else:
                @pl.when(r > c)
                def _():
                    kv_copy(s, 0, c, r).wait_recv()
                    kv_copy(s, 1, c, r).wait_recv()

    def exchange(src, dst, ss, rs):
        far = (2, 1, chips - 1, 0)
        for r in range(cps):
            for a, dx in enumerate(far):
                dc = far[(r + a) % cps]
                dxe = jnp.where(core == 0, dx, (chips - dx) % chips)
                cc = (c + dc) % cps
                for dk in range(2):
                    if (dx, dc, dk) != (0, 0, 0):
                        tt = flat(slot(dxe, dk == 1))
                        g = cc * tps + tt
                        rcopy(src.at[g], dst.at[me], ss, rs, cc, tt).start()
        dst[me] = src[me]

    def arrived(dst, rs):
        part = dst.at[pl.ds(0, group - 1)]
        rcopy(part, part, rs, rs, c, t).wait_recv()

    def left_all(src, ss):
        part = src.at[pl.ds(0, group - 1)]
        rcopy(part, part, ss, ss, c, t).wait_send()

    def o_wait(s):
        for i in range(1, tps):
            src = (t + i) % tps
            rcopy(orecv.at[s, src], orecv.at[s, src], os_sem.at[s, src], or_sem.at[s, src], c, src).wait_recv()

    def unpack(s, u):
        full = [orecv[s, u, b * n:(b + 1) * n, :] for b in range(qh // 2)]
        last = orecv[s, u, qh // 2 * n:, :]
        return full + [jnp.concatenate([last[:, :hd], last[:, hd:]], axis=0)]

    def out_part(s, dxs):
        heads, weights = [], []
        for dx in dxs:
            xq = (xc + dx) % chips
            for cr in range(2):
                heads += unpack(s, xq * 2 + cr)
            weights.append(wof[xq].reshape(2 * kdim, hid))
        return mm(jnp.concatenate(heads, axis=1), jnp.concatenate(weights, axis=0))

    def dispatch(s, added):
        mid_rows = (xf[s, xc, core].astype(F32) + added).astype(BF16)
        hbuf[s] = mid_rows
        dsend[s] = mm(onehot[s], mid_rows).reshape(group, cap, hid).astype(BF16)
        exchange(dsend.at[s], drecv.at[s], ds_sem.at[s], dr_sem.at[s])

    with scope('wb1'):
        for q in range(3):
            wb(q, False).wait_recv()
            for i in range(1, cps):
                spread(q, (c + i) % cps, c).start()
            share(5 + q, True).start()
    with scope('kvwait00'):
        kv_wait(0, 0)
    with scope('attend00'):
        attend(0, 0)
    with scope('kvwait01'):
        kv_wait(0, 1)
    with scope('attend01'):
        attend(0, 1)
    with scope('wa2'):
        wa[1](0)
        wa[0](4)
        wa[1](2)
        wa[0](5)
        wa[1](1, 3)
        share(1, True).start()
        share(2, True).start()
    with scope('kvwait10'):
        kv_wait(1, 0)
    with scope('attend10'):
        attend(1, 0)
    with scope('kvwait11'):
        kv_wait(1, 1)
    with scope('attend11'):
        attend(1, 1)
    def y_shares(q):
        for i in range(1, cps):
            spread(q, (c + i) % cps, (c + i) % cps).wait_recv()
            share(5 + 3 * i + q, True).start()

    with scope('wy01'):
        y_shares(0)
        y_shares(1)
    with scope('wa3'):
        wa[1](4)
        share(3, True).start()
        wa[1](5)
        share(4, True).start()
        y_shares(2)
    with scope('wshare0'):
        for k in (0, 1, 2) + tuple(5 + 3 * i + q for i in range(cps) for q in range(2)):
            share(k, False).wait_recv()
        o_wait(0)
    with scope('part0'):
        abuf[...] = out_part(0, (0, 1, chips - 1))
    with scope('wshare1'):
        for k in (3, 4) + tuple(5 + 3 * i + 2 for i in range(cps)):
            share(k, False).wait_recv()
    with scope('out0'):
        dispatch(0, abuf[...] + out_part(0, (2,)))
    with scope('owait1'):
        o_wait(1)
    with scope('out1'):
        dispatch(1, mm(jnp.concatenate(sum([unpack(1, u) for u in range(tps)], []), axis=1), wof[...].reshape(tps * kdim, hid)))

    for cp in ld_exp:
        cp.wait()
    for s in range(seqs):
        with scope(f'dwait{s}'):
            arrived(drecv.at[s], dr_sem.at[s])
        rows = drecv[s].astype(F32).reshape(group * cap, hid).astype(BF16)
        act = (jax.nn.silu(mm(rows, wg[...])) * mm(rows, wu[...])).astype(BF16)
        rsend[s] = mm(act, wd[...]).reshape(group, cap, hid).astype(BF16)
        exchange(rsend.at[s], rrecv.at[s], rs_sem.at[s], rr_sem.at[s])

    for s in range(seqs):
        with scope(f'rwait{s}'):
            arrived(rrecv.at[s], rr_sem.at[s])
        z = mm(onehot_t[s], rrecv[s].astype(F32).reshape(group * cap, hid).astype(BF16))
        g0 = gcol[s, 0][:, :1]
        g1 = gcol[s, 1][:, :1]
        y_ref[s] = (hbuf[s].astype(F32) + (g0 * z[:n] + g1 * z[n:])).astype(BF16)

    for s in range(seqs):
        xg[s][2](*range(11))
        for half in range(2):
            for i in range(1, cps):
                r = (c + i) % cps
                if half == 0:
                    kv_copy(s, half, r, c).wait_send()
                else:
                    @pl.when(r < c)
                    def _():
                        kv_copy(s, half, r, c).wait_send()
        for i in range(1, tps):
            dst = (t + i) % tps
            rcopy(osend.at[s, dst], orecv.at[s, t], os_sem.at[s, dst], or_sem.at[s, t], c, dst).wait_send()
        left_all(dsend.at[s], ds_sem.at[s])
        left_all(rsend.at[s], rs_sem.at[s])
    wa[2](*range(6))
    for q in range(3):
        wb(q, True).wait_send()
    for q in range(3):
        for i in range(1, cps):
            spread(q, (c + i) % cps, c).wait_send()
    for k in range(shares):
        share(k, True).wait_send()


def solution(mesh):
    cps = mesh.shape['cp']
    tps = mesh.shape['tp']
    experts = cps * tps
    row_spec = P(None, ('data', 'cp', 'tp'), None)
    head_spec = P(None, 'tp', None)
    out_spec = P('tp', None, None)
    expert_spec = P(('cp', 'tp'), None, None)

    def device_step(act_in, route_ids, route_gates, w_query, w_key, w_value, w_out, w_gate, w_up, w_down):
        seqs, n, hid = act_in.shape
        qh, hd = w_query.shape[1], w_query.shape[2]
        ff = w_gate.shape[2]
        cap = (4 * n) // experts
        kdim = qh * hd
        lanes = 2 * hd
        hslots = tps // 2
        piece = n * hslots
        wq = jnp.transpose(w_query, (1, 2, 0)).reshape(kdim, hid)
        wk = jnp.transpose(w_key, (1, 2, 0)).reshape(hd, hid)
        wv = jnp.transpose(w_value, (1, 2, 0)).reshape(hd, hid)
        ids = jnp.transpose(route_ids, (0, 2, 1))
        gates = jnp.transpose(route_gates, (0, 2, 1))
        dims = (cps, tps, seqs, n, hid, hd, qh, cap)
        orows = n * (qh // 2) + n // 2
        vm = pl.BlockSpec(memory_space=pltpu.VMEM)
        anym = pl.BlockSpec(memory_space=pl.ANY)
        dma = pltpu.SemaphoreType.DMA
        scratch = [
            pltpu.VMEM((seqs, tps // 2, 2, n, hid), BF16),
            pltpu.VMEM((lanes * (qh + 1), hid), BF16),
            pltpu.VMEM((seqs, 2 * cps, piece, lanes), BF16),
            pltpu.VMEM((seqs, 2, qh * piece, lanes), BF16),
            pltpu.VMEM((2 * cps, qh * piece, piece), F32),
            pltpu.VMEM((qh * piece, piece // 2), F32),
            pltpu.VMEM((qh * piece, piece // 2), F32),
            pltpu.VMEM((qh * piece, lanes), F32),
            pltpu.VMEM((seqs, tps, orows, lanes), BF16),
            pltpu.VMEM((seqs, tps, orows, lanes), BF16),
            pltpu.VMEM((tps // 2, 2, kdim, hid), BF16),
            pltpu.VMEM((seqs, experts * cap, n), BF16),
            pltpu.VMEM((seqs, 2 * n, experts * cap), BF16),
            pltpu.VMEM((seqs, 2, n, 128), F32),
            pltpu.VMEM((n, hid), F32),
            pltpu.VMEM((seqs, n, hid), BF16),
            pltpu.VMEM((seqs, experts, cap, hid), BF16),
            pltpu.VMEM((seqs, experts, cap, hid), BF16),
            pltpu.VMEM((seqs, experts, cap, hid), BF16),
            pltpu.VMEM((seqs, experts, cap, hid), BF16),
            pltpu.VMEM((hid, ff), BF16),
            pltpu.VMEM((hid, ff), BF16),
            pltpu.VMEM((ff, hid), BF16),
            dma((8 + qh,)),
            dma((seqs, 11)), dma((seqs, 11)),
            dma((2, 6)), dma((2, 6)),
            dma((3, cps)), dma((3, cps)),
            dma((5 + 3 * cps,)), dma((5 + 3 * cps,)),
            dma((seqs, 2, cps)), dma((seqs, 2, cps)),
            dma((seqs, tps)), dma((seqs, tps)),
            dma((seqs,)), dma((seqs,)),
            dma((seqs,)), dma((seqs,)),
        ]
        return pl.pallas_call(
            functools.partial(layer_kernel, dims),
            out_shape=pltpu.VMEM((seqs, n, hid), BF16),
            in_specs=[anym, vm, vm, anym, anym, anym, anym, anym, anym, anym],
            out_specs=vm,
            scratch_shapes=scratch,
            compiler_params=pltpu.CompilerParams(collective_id=0, has_side_effects=True, vmem_limit_bytes=58 * 1024 * 1024),
            name='layer',
        )(act_in, ids, gates, wq, wk, wv, w_out.reshape(kdim, hid), w_gate[0], w_up[0], w_down[0])

    return jax.shard_map(device_step, mesh=mesh, in_specs=(row_spec, row_spec, row_spec, head_spec, head_spec, head_spec, out_spec, expert_spec, expert_spec, expert_spec), out_specs=row_spec, check_vma=False)
```

```python
import functools
import math

import jax
import jax.numpy as jnp
from jax import lax
from jax.experimental import pallas as pl
from jax.experimental.pallas import tpu as pltpu
from jax.sharding import PartitionSpec as P

MESH = pl.DeviceIdType.MESH
scope = jax.named_scope
F32 = jnp.float32
BF16 = jnp.bfloat16
NT = (((1,), (1,)), ((), ()))


def mm(a, b):
    return jnp.dot(a, b, preferred_element_type=F32)


def mm_nt(a, b):
    return lax.dot_general(a, b, NT, preferred_element_type=F32)


def layer_kernel(dims, x_hbm, ids_ref, gates_ref, wq_hbm, wk_hbm, wv_hbm, wo_hbm, wg_hbm, wu_hbm, wd_hbm, y_ref,
                 xf, wqkv, kv, qs, sbuf, mx, lsum, acc, osend, orecv, wof, onehot, onehot_t, gcol, abuf, hbuf,
                 dsend, drecv, rsend, rrecv, wg, wu, wd,
                 loc_sem, xs_sem, xr_sem, ws_sem, wr_sem, vs_sem, vr_sem, ss_sem, sr_sem, ks_sem, kr_sem, os_sem, or_sem,
                 ds_sem, dr_sem, rs_sem, rr_sem):
    cps, tps, seqs, n, hid, hd, qh, cap = dims
    experts = cps * tps
    group = experts
    chips = tps // 2
    hslots = tps // 2
    piece = n * hslots
    pieces = 2 * cps
    lanes = 2 * hd
    qrows = qh * piece
    kdim = qh * hd
    c = lax.axis_index('cp')
    t = lax.axis_index('tp')
    me = c * tps + t
    xc = t // 2
    core = t % 2

    unit = hid // (3 * cps)

    def slot(dx, other):
        return (xc + dx) % chips, (core if not other else 1 - core)

    def flat(sl):
        return sl[0] * 2 + sl[1]

    right, left, sib = slot(1, False), slot(chips - 1, False), slot(0, True)
    own, opposite = (xc, core), slot(2, False)

    def rcopy(src, dst, ssem, rsem, cc, tt):
        return pltpu.make_async_remote_copy(src_ref=src, dst_ref=dst, send_sem=ssem, recv_sem=rsem,
                                            device_id={'cp': cc, 'tp': tt}, device_id_type=MESH)

    def load(src, dst, i):
        cp = pltpu.make_async_copy(src, dst, loc_sem.at[i])
        cp.start()
        return cp

    ld_x = [load(x_hbm.at[s], xf.at[s, xc, core], s) for s in range(seqs)]
    ld_wo = load(wo_hbm, wof.at[xc, core], 2)
    ld_qkv = [load(wv_hbm, wqkv.at[pl.ds(0, hd)], 3), load(wk_hbm, wqkv.at[pl.ds(hd, hd)], 4)]
    for i in range(qh):
        ld_qkv.append(load(wq_hbm.at[pl.ds(i * hd, hd)], wqkv.at[pl.ds(lanes * (i + 1) + hd, hd)], 5 + i))
    ld_exp = [load(wg_hbm, wg, 5 + qh), load(wu_hbm, wu, 6 + qh), load(wd_hbm, wd, 7 + qh)]

    barrier = pltpu.get_barrier_semaphore()

    def sig(i, _):
        g = (me + i) % group
        pl.semaphore_signal(barrier, inc=1, device_id={'cp': g // tps, 'tp': g % tps}, device_id_type=MESH)
        return 0

    lax.fori_loop(1, group, sig, 0)
    pl.semaphore_wait(barrier, group - 1)

    def gather(get, ss, rs):
        l2, r2, o2 = slot(chips - 1, True), slot(1, True), slot(2, True)
        sends = [
            (own, 'lo', right), (own, 'hi', right), (own, 'hi', left), (own, 'lo', left),
            (left, 'lo', right), (right, 'hi', left),
            (own, 'all', sib), (left, 'all', sib), (right, 'all', sib), (opposite, 'lo', sib), (opposite, 'hi', sib),
        ]
        gets = [
            (left, 'lo'), (left, 'hi'), (right, 'hi'), (right, 'lo'),
            (opposite, 'lo'), (opposite, 'hi'),
            (sib, 'all'), (l2, 'all'), (r2, 'all'), (o2, 'lo'), (o2, 'hi'),
        ]

        def copy(sl, part, kind, dst):
            return rcopy(get(sl, part), get(sl, part), ss.at[kind], rs.at[kind], c, flat(dst))

        def start(*kinds):
            for k in kinds:
                copy(*sends[k][:2], k, sends[k][2]).start()

        def got(*kinds):
            for k in kinds:
                copy(*gets[k], k, sib).wait_recv()

        def sent(*kinds):
            for k in kinds:
                copy(*sends[k][:2], k, sends[k][2]).wait_send()

        return start, got, sent

    def rows_of(rows):
        return {'lo': pl.ds(0, rows // 2), 'hi': pl.ds(rows // 2, rows // 2), 'all': pl.ds(0, rows)}

    xparts, wparts = rows_of(n), rows_of(kdim)
    xg = [gather(lambda sl, part, s=s: xf.at[s, sl[0], sl[1], xparts[part]], xs_sem.at[s], xr_sem.at[s]) for s in range(seqs)]

    cols_a = pl.ds(0, hid - cps * unit)

    def cols_b(r):
        return pl.ds(pl.multiple_of(hid - cps * unit + r * unit, unit), unit)

    wa = gather(lambda sl, part: wof.at[sl[0], sl[1], wparts[part], cols_a], ws_sem.at[0], wr_sem.at[0])

    def wb(q, mine):
        sl = own if mine else (left, right, opposite)[q]
        ref = wof.at[sl[0], sl[1], :, cols_b(c)]
        dst = (right, left, opposite)[q]
        return rcopy(ref, ref, ws_sem.at[1, q], wr_sem.at[1, q], c, flat(dst))


    remote = (left, right, opposite)

    def spread(q, r, src):
        sl = remote[q]
        ref = wof.at[sl[0], sl[1], :, cols_b(src)]
        return rcopy(ref, ref, vs_sem.at[q, r], vr_sem.at[q, src], r, t)

    def share(k, mine):
        cr = core if mine else 1 - core
        if k == 0:
            ref = wof.at[xc, cr]
        elif k < 5:
            q, part = ((0, 'all'), (1, 'all'), (2, 'lo'), (2, 'hi'))[k - 1]
            ref = wof.at[remote[q][0], cr, wparts[part], cols_a]
        else:
            q, i = (k - 5) % 3, (k - 5) // 3
            ref = wof.at[remote[q][0], cr, :, cols_b((c + i) % cps)]
        return rcopy(ref, ref, ss_sem.at[k], sr_sem.at[k], c, flat(sib))

    shares = 5 + 3 * cps

    ld_x[0].wait()
    xg[0][0](0, 2, 1, 3, 6)
    ld_x[1].wait()
    xg[1][0](0, 2)

    ecol = lax.broadcasted_iota(jnp.int32, (experts, n), 0)
    later = (lax.broadcasted_iota(jnp.int32, (n, n), 0) < lax.broadcasted_iota(jnp.int32, (n, n), 1)).astype(F32).astype(BF16)
    srow = lax.broadcasted_iota(jnp.int32, (experts * cap, n), 0)
    eye = lax.broadcasted_iota(jnp.int32, (n, n), 0) == lax.broadcasted_iota(jnp.int32, (n, n), 1)
    for s in range(seqs):
        first = jnp.zeros((experts, 1), F32)
        both = None
        for k in range(2):
            idk = ids_ref[s, k:k + 1, :]
            hits = (ecol == idk).astype(F32)
            before = mm(hits.astype(BF16), later) + first
            rank = jnp.sum(hits * before, axis=0, keepdims=True).astype(jnp.int32)
            first = first + jnp.sum(hits, axis=1, keepdims=True)
            dest = idk * cap + rank
            pick = (srow == dest).astype(F32)
            both = pick if both is None else both + pick
            onehot_t[s, k * n:(k + 1) * n, :] = pick.T.astype(BF16)
            gcol[s, k] = jnp.broadcast_to(jnp.sum(jnp.where(eye, gates_ref[s, k:k + 1, :], 0.0), axis=1, keepdims=True), (n, 128))
        onehot[s] = both.astype(BF16)
    for i in range(qh):
        wqkv[lanes * (i + 1):lanes * (i + 1) + hd, :] = jnp.zeros((hd, hid), BF16)

    def kv_piece(half):
        return c if half == 0 else pieces - 1 - c

    def kv_copy(s, half, r, src):
        ref = kv.at[s, src if half == 0 else pieces - 1 - src]
        return rcopy(ref, ref, ks_sem.at[s, half, r], kr_sem.at[s, half, src], r, t)

    def project(s):
        for half in range(2):
            rows = xf[s, half * (chips // 2):(half + 1) * (chips // 2)].reshape(piece, hid)
            out = mm_nt(rows, wqkv[...])
            kv[s, kv_piece(half)] = out[:, :lanes].astype(BF16)
            for i in range(qh):
                qs[s, half, i * piece:(i + 1) * piece, :] = out[:, lanes * (i + 1):lanes * (i + 2)].astype(BF16)
            for i in range(1, cps):
                r = (c + i) % cps
                if half == 0:
                    kv_copy(s, half, r, c).start()
                else:
                    @pl.when(r < c)
                    def _():
                        kv_copy(s, half, r, c).start()

    with scope('xrelay0'):
        start, got, _ = xg[0]
        got(0)
        start(4)
        got(2)
        start(5)
        xg[1][0](1, 3, 6)
        got(1)
        start(7)
        got(3)
        start(8)
    with scope('xrelay1'):
        xg[1][1](0)
        xg[1][0](4)
        xg[1][1](2)
        xg[1][0](5)
    with scope('xfinish0'):
        start, got, _ = xg[0]
        got(4)
        start(9)
        got(5)
        start(10)
        for cp in ld_qkv:
            cp.wait()
        ld_wo.wait()
        for q in range(3):
            wb(q, True).start()
        wa[0](0, 2, 1, 3)
        share(0, True).start()
        got(6, 7, 8, 9, 10)
    with scope('qkv0'):
        project(0)
    with scope('xfinish1'):
        start, got, _ = xg[1]
        got(1)
        start(7)
        got(3)
        start(8)
        got(4)
        start(9)
        got(5)
        start(10)
        got(6, 7, 8, 9, 10)
    with scope('qkv1'):
        project(1)

    scale = hd ** -0.5 * math.log2(math.e)
    causal = lax.broadcasted_iota(jnp.int32, (piece, piece), 1) <= lax.broadcasted_iota(jnp.int32, (piece, piece), 0)
    lane_lo = lax.broadcasted_iota(jnp.int32, (n, lanes), 1) < hd
    mid = piece // 2

    def attend(s, half):
        blocks = c + 1 if half == 0 else pieces - c
        for i in range(qh):
            rs = slice(i * piece, (i + 1) * piece)
            mx[rs] = jnp.full((piece, mid), -jnp.inf, F32)

        def scores(j, diag):
            for i in range(qh):
                rs = slice(i * piece, (i + 1) * piece)
                sc = mm_nt(qs[s, half, rs, :], kv[s, j])
                if diag:
                    sc = jnp.where(causal, sc, -jnp.inf)
                sbuf[j, rs, :] = sc
                mx[rs] = jnp.maximum(mx[rs], jnp.maximum(sc[:, :mid], sc[:, mid:]))

        def one(j, _):
            scores(j, False)
            return 0

        lax.fori_loop(0, blocks - 1, one, 0)
        scores(blocks - 1, True)
        for i in range(qh):
            rs = slice(i * piece, (i + 1) * piece)
            mx[rs] = jnp.broadcast_to(jnp.max(mx[rs], axis=1, keepdims=True), (piece, mid))
            lsum[rs] = jnp.zeros((piece, mid), F32)
            acc[rs] = jnp.zeros((piece, lanes), F32)

        def two(j, _):
            for i in range(qh):
                rs = slice(i * piece, (i + 1) * piece)
                top = mx[rs]
                pa = jnp.exp2((sbuf[j, rs, :mid] - top) * scale)
                pb = jnp.exp2((sbuf[j, rs, mid:] - top) * scale)
                lsum[rs] += pa + pb
                acc[rs] += mm(jnp.concatenate([pa, pb], axis=1).astype(BF16), kv[s, j])
            return 0

        lax.fori_loop(0, blocks, two, 0)
        for u in range(hslots):
            heads = []
            for i in range(qh):
                rs = slice(i * piece + u * n, i * piece + (u + 1) * n)
                heads.append(acc[rs] / jnp.sum(lsum[rs], axis=1, keepdims=True))
            for b in range(0, qh - 1, 2):
                both = jnp.where(lane_lo, heads[b], pltpu.roll(heads[b + 1], hd, 1))
                osend[s, half * hslots + u, b // 2 * n:(b // 2 + 1) * n, :] = both.astype(BF16)
            last = heads[qh - 1]
            both = jnp.where(lane_lo[:n // 2], last[:n // 2], pltpu.roll(last[n // 2:], hd, 1))
            osend[s, half * hslots + u, qh // 2 * n:, :] = both.astype(BF16)
        for u in range(hslots):
            dst = half * hslots + u

            @pl.when(dst != t)
            def _():
                rcopy(osend.at[s, dst], orecv.at[s, t], os_sem.at[s, dst], or_sem.at[s, t], c, dst).start()

            @pl.when(dst == t)
            def _():
                orecv[s, t] = osend[s, dst]

    def kv_wait(s, half):
        for i in range(1, cps):
            r = (c + i) % cps
            if half == 0:
                @pl.when(r < c)
                def _():
                    kv_copy(s, 0, c, r).wait_recv()
            else:
                @pl.when(r > c)
                def _():
                    kv_copy(s, 0, c, r).wait_recv()
                    kv_copy(s, 1, c, r).wait_recv()

    def exchange(src, dst, ss, rs):
        far = (2, 1, chips - 1, 0)
        for r in range(cps):
            for a, dx in enumerate(far):
                dc = far[(r + a) % cps]
                dxe = jnp.where(core == 0, dx, (chips - dx) % chips)
                cc = (c + jnp.where(core == 0, dc, (cps - dc) % cps)) % cps
                for dk in range(2):
                    if (dx, dc, dk) != (0, 0, 0):
                        tt = flat(slot(dxe, dk == 1))
                        g = cc * tps + tt
                        rcopy(src.at[g], dst.at[me], ss, rs, cc, tt).start()
        dst[me] = src[me]

    def arrived(dst, rs):
        part = dst.at[pl.ds(0, group - 1)]
        rcopy(part, part, rs, rs, c, t).wait_recv()

    def left_all(src, ss):
        part = src.at[pl.ds(0, group - 1)]
        rcopy(part, part, ss, ss, c, t).wait_send()

    def o_wait(s):
        for i in range(1, tps):
            src = (t + i) % tps
            rcopy(orecv.at[s, src], orecv.at[s, src], os_sem.at[s, src], or_sem.at[s, src], c, src).wait_recv()

    def unpack(s, u):
        full = [orecv[s, u, b * n:(b + 1) * n, :] for b in range(qh // 2)]
        last = orecv[s, u, qh // 2 * n:, :]
        return full + [jnp.concatenate([last[:, :hd], last[:, hd:]], axis=0)]

    def out_part(s, dxs):
        heads, weights = [], []
        for dx in dxs:
            xq = (xc + dx) % chips
            for cr in range(2):
                heads += unpack(s, xq * 2 + cr)
            weights.append(wof[xq].reshape(2 * kdim, hid))
        return mm(jnp.concatenate(heads, axis=1), jnp.concatenate(weights, axis=0))

    def dispatch(s, added):
        mid_rows = (xf[s, xc, core].astype(F32) + added).astype(BF16)
        hbuf[s] = mid_rows
        dsend[s] = mm(onehot[s], mid_rows).reshape(group, cap, hid).astype(BF16)
        exchange(dsend.at[s], drecv.at[s], ds_sem.at[s], dr_sem.at[s])

    with scope('wb1'):
        for q in range(3):
            wb(q, False).wait_recv()
            for i in range(1, cps):
                spread(q, (c + i) % cps, c).start()
            share(5 + q, True).start()
    with scope('kvwait00'):
        kv_wait(0, 0)
    with scope('attend00'):
        attend(0, 0)
    with scope('kvwait01'):
        kv_wait(0, 1)
    with scope('attend01'):
        attend(0, 1)
    with scope('wa2'):
        wa[1](0)
        wa[0](4)
        wa[1](2)
        wa[0](5)
        wa[1](1, 3)
        share(1, True).start()
        share(2, True).start()
    with scope('kvwait10'):
        kv_wait(1, 0)
    with scope('attend10'):
        attend(1, 0)
    with scope('kvwait11'):
        kv_wait(1, 1)
    with scope('attend11'):
        attend(1, 1)
    def y_shares(q):
        for i in range(1, cps):
            spread(q, (c + i) % cps, (c + i) % cps).wait_recv()
            share(5 + 3 * i + q, True).start()

    with scope('wy01'):
        y_shares(0)
        y_shares(1)
    with scope('wa3'):
        wa[1](4)
        share(3, True).start()
        wa[1](5)
        share(4, True).start()
        y_shares(2)
    with scope('wshare0'):
        for k in (0, 1, 2) + tuple(5 + 3 * i + q for i in range(cps) for q in range(2)):
            share(k, False).wait_recv()
        o_wait(0)
    with scope('part0'):
        abuf[...] = out_part(0, (0, 1, chips - 1))
    with scope('wshare1'):
        for k in (3, 4) + tuple(5 + 3 * i + 2 for i in range(cps)):
            share(k, False).wait_recv()
    with scope('out0'):
        dispatch(0, abuf[...] + out_part(0, (2,)))
    with scope('owait1'):
        o_wait(1)
    with scope('out1'):
        dispatch(1, mm(jnp.concatenate(sum([unpack(1, u) for u in range(tps)], []), axis=1), wof[...].reshape(tps * kdim, hid)))

    for cp in ld_exp:
        cp.wait()
    for s in range(seqs):
        with scope(f'dwait{s}'):
            arrived(drecv.at[s], dr_sem.at[s])
        rows = drecv[s].astype(F32).reshape(group * cap, hid).astype(BF16)
        act = (jax.nn.silu(mm(rows, wg[...])) * mm(rows, wu[...])).astype(BF16)
        rsend[s] = mm(act, wd[...]).reshape(group, cap, hid).astype(BF16)
        exchange(rsend.at[s], rrecv.at[s], rs_sem.at[s], rr_sem.at[s])

    for s in range(seqs):
        with scope(f'rwait{s}'):
            arrived(rrecv.at[s], rr_sem.at[s])
        z = mm(onehot_t[s], rrecv[s].astype(F32).reshape(group * cap, hid).astype(BF16))
        g0 = gcol[s, 0][:, :1]
        g1 = gcol[s, 1][:, :1]
        y_ref[s] = (hbuf[s].astype(F32) + (g0 * z[:n] + g1 * z[n:])).astype(BF16)

    for s in range(seqs):
        xg[s][2](*range(11))
        for half in range(2):
            for i in range(1, cps):
                r = (c + i) % cps
                if half == 0:
                    kv_copy(s, half, r, c).wait_send()
                else:
                    @pl.when(r < c)
                    def _():
                        kv_copy(s, half, r, c).wait_send()
        for i in range(1, tps):
            dst = (t + i) % tps
            rcopy(osend.at[s, dst], orecv.at[s, t], os_sem.at[s, dst], or_sem.at[s, t], c, dst).wait_send()
        left_all(dsend.at[s], ds_sem.at[s])
        left_all(rsend.at[s], rs_sem.at[s])
    wa[2](*range(6))
    for q in range(3):
        wb(q, True).wait_send()
    for q in range(3):
        for i in range(1, cps):
            spread(q, (c + i) % cps, c).wait_send()
    for k in range(shares):
        share(k, True).wait_send()


def solution(mesh):
    cps = mesh.shape['cp']
    tps = mesh.shape['tp']
    experts = cps * tps
    row_spec = P(None, ('data', 'cp', 'tp'), None)
    head_spec = P(None, 'tp', None)
    out_spec = P('tp', None, None)
    expert_spec = P(('cp', 'tp'), None, None)

    def device_step(act_in, route_ids, route_gates, w_query, w_key, w_value, w_out, w_gate, w_up, w_down):
        seqs, n, hid = act_in.shape
        qh, hd = w_query.shape[1], w_query.shape[2]
        ff = w_gate.shape[2]
        cap = (4 * n) // experts
        kdim = qh * hd
        lanes = 2 * hd
        hslots = tps // 2
        piece = n * hslots
        wq = jnp.transpose(w_query, (1, 2, 0)).reshape(kdim, hid)
        wk = jnp.transpose(w_key, (1, 2, 0)).reshape(hd, hid)
        wv = jnp.transpose(w_value, (1, 2, 0)).reshape(hd, hid)
        ids = jnp.transpose(route_ids, (0, 2, 1))
        gates = jnp.transpose(route_gates, (0, 2, 1))
        dims = (cps, tps, seqs, n, hid, hd, qh, cap)
        orows = n * (qh // 2) + n // 2
        vm = pl.BlockSpec(memory_space=pltpu.VMEM)
        anym = pl.BlockSpec(memory_space=pl.ANY)
        dma = pltpu.SemaphoreType.DMA
        scratch = [
            pltpu.VMEM((seqs, tps // 2, 2, n, hid), BF16),
            pltpu.VMEM((lanes * (qh + 1), hid), BF16),
            pltpu.VMEM((seqs, 2 * cps, piece, lanes), BF16),
            pltpu.VMEM((seqs, 2, qh * piece, lanes), BF16),
            pltpu.VMEM((2 * cps, qh * piece, piece), F32),
            pltpu.VMEM((qh * piece, piece // 2), F32),
            pltpu.VMEM((qh * piece, piece // 2), F32),
            pltpu.VMEM((qh * piece, lanes), F32),
            pltpu.VMEM((seqs, tps, orows, lanes), BF16),
            pltpu.VMEM((seqs, tps, orows, lanes), BF16),
            pltpu.VMEM((tps // 2, 2, kdim, hid), BF16),
            pltpu.VMEM((seqs, experts * cap, n), BF16),
            pltpu.VMEM((seqs, 2 * n, experts * cap), BF16),
            pltpu.VMEM((seqs, 2, n, 128), F32),
            pltpu.VMEM((n, hid), F32),
            pltpu.VMEM((seqs, n, hid), BF16),
            pltpu.VMEM((seqs, experts, cap, hid), BF16),
            pltpu.VMEM((seqs, experts, cap, hid), BF16),
            pltpu.VMEM((seqs, experts, cap, hid), BF16),
            pltpu.VMEM((seqs, experts, cap, hid), BF16),
            pltpu.VMEM((hid, ff), BF16),
            pltpu.VMEM((hid, ff), BF16),
            pltpu.VMEM((ff, hid), BF16),
            dma((8 + qh,)),
            dma((seqs, 11)), dma((seqs, 11)),
            dma((2, 6)), dma((2, 6)),
            dma((3, cps)), dma((3, cps)),
            dma((5 + 3 * cps,)), dma((5 + 3 * cps,)),
            dma((seqs, 2, cps)), dma((seqs, 2, cps)),
            dma((seqs, tps)), dma((seqs, tps)),
            dma((seqs,)), dma((seqs,)),
            dma((seqs,)), dma((seqs,)),
        ]
        return pl.pallas_call(
            functools.partial(layer_kernel, dims),
            out_shape=pltpu.VMEM((seqs, n, hid), BF16),
            in_specs=[anym, vm, vm, anym, anym, anym, anym, anym, anym, anym],
            out_specs=vm,
            scratch_shapes=scratch,
            compiler_params=pltpu.CompilerParams(collective_id=0, has_side_effects=True, vmem_limit_bytes=58 * 1024 * 1024),
            name='layer',
        )(act_in, ids, gates, wq, wk, wv, w_out.reshape(kdim, hid), w_gate[0], w_up[0], w_down[0])

    return jax.shard_map(device_step, mesh=mesh, in_specs=(row_spec, row_spec, row_spec, head_spec, head_spec, head_spec, out_spec, expert_spec, expert_spec, expert_spec), out_specs=row_spec, check_vma=False)
```
